128 devices in a mesh: rows: 128 (over z, y, x, core).
Axes of the slice: x: 4, y: 4, z: 4, core: 2. Of those that a mesh axis runs over, the one named last changes fastest.
Arguments:
- wave_fn: float32 [640, 4, 4, 640], P('rows')
- left_env: bfloat16 [32, 640, 640], P(None, 'rows')
- op_pair: bfloat16 [32, 16, 16], replicated
- right_env: bfloat16 [32, 640, 640], replicated
Outputs:
- output 1: float32 [7, 640, 4, 4, 640], P(None, 'rows')
- output 2: float32 [6], replicated
- output 3: float32 [6], replicated
All inputs are finite; a program needn't handle non-finite values.
Results may differ from the reference program's by a relative error of at most 0.011815.
Values are sent between devices in bfloat16 or wider.
A program may use at most 1 GiB of HBM per device.

```python
import jax
import jax.numpy as jnp
from jax import lax

BOND_DIM = 640
PHYS_DIM = 4
NUM_TERMS = 32
NUM_STEPS = 6


def sym_noise(rng_key, num_mats, mat_size):
    raw_draw = jax.random.normal(rng_key, (num_mats, mat_size, mat_size), jnp.float32)
    return (raw_draw + jnp.swapaxes(raw_draw, 1, 2)) * (0.5 ** 0.5) * mat_size ** -0.5


def setup_inputs(seed: int = 0) -> dict:
    key_list = jax.random.split(jax.random.key(seed), 7)
    pair_dim = PHYS_DIM * PHYS_DIM
    shift_left = jax.random.uniform(key_list[0], (NUM_TERMS, 1, 1), jnp.float32, 0.3, 0.9)
    shift_pair = jax.random.uniform(key_list[1], (NUM_TERMS, 1, 1), jnp.float32, 0.3, 0.9)
    shift_right = jax.random.uniform(key_list[2], (NUM_TERMS, 1, 1), jnp.float32, 0.3, 0.9)
    left_env = sym_noise(key_list[3], NUM_TERMS, BOND_DIM) + shift_left * jnp.eye(BOND_DIM, dtype=jnp.float32)
    op_pair = (sym_noise(key_list[4], NUM_TERMS, pair_dim) + shift_pair * jnp.eye(pair_dim, dtype=jnp.float32)) * NUM_TERMS ** -0.5
    right_env = sym_noise(key_list[5], NUM_TERMS, BOND_DIM) + shift_right * jnp.eye(BOND_DIM, dtype=jnp.float32)
    wave_fn = jax.random.normal(key_list[6], (BOND_DIM, PHYS_DIM, PHYS_DIM, BOND_DIM), jnp.float32)
    return {"wave_fn": wave_fn, "left_env": left_env.astype(jnp.bfloat16), "op_pair": op_pair.astype(jnp.bfloat16), "right_env": right_env.astype(jnp.bfloat16)}


def matvec(vec_in, left_env, op_pair, right_env):
    pair_dim = PHYS_DIM * PHYS_DIM
    flat_in = vec_in.astype(jnp.bfloat16).reshape(BOND_DIM, pair_dim * BOND_DIM)

    def add_term(acc_sum, term_ops):
        left_k, pair_k, right_k = term_ops
        left_out = jnp.dot(left_k, flat_in, preferred_element_type=jnp.float32).astype(jnp.bfloat16)
        left_out = left_out.reshape(BOND_DIM, pair_dim, BOND_DIM)
        mid_out = jnp.einsum("qr,arc->aqc", pair_k.astype(jnp.float32), left_out.astype(jnp.float32)).astype(jnp.bfloat16)
        part_out = jnp.dot(mid_out.reshape(BOND_DIM * pair_dim, BOND_DIM), right_k.T, preferred_element_type=jnp.float32)
        return acc_sum + part_out, None

    start_sum = jnp.zeros((BOND_DIM * pair_dim, BOND_DIM), jnp.float32)
    sigma_all = lax.scan(add_term, start_sum, (left_env, op_pair, right_env))[0]
    return sigma_all.reshape(BOND_DIM, PHYS_DIM, PHYS_DIM, BOND_DIM)


def reference(wave_fn, left_env, op_pair, right_env):
    vec_count = BOND_DIM * BOND_DIM * PHYS_DIM * PHYS_DIM
    first_vec = wave_fn / jnp.sqrt(jnp.sum(wave_fn * wave_fn) / vec_count)

    def lanczos_step(carry_in, unused):
        prev_vec, cur_vec, beta_prev = carry_in
        sigma_all = matvec(cur_vec, left_env, op_pair, right_env)
        alpha_val = jnp.sum(sigma_all * cur_vec) / vec_count
        resid_vec = sigma_all - alpha_val * cur_vec - beta_prev * prev_vec
        beta_val = jnp.sqrt(jnp.sum(resid_vec * resid_vec) / vec_count)
        next_vec = resid_vec / beta_val
        return (cur_vec, next_vec, beta_val), (next_vec, alpha_val, beta_val)

    start_carry = (jnp.zeros_like(first_vec), first_vec, jnp.zeros((), jnp.float32))
    later_vecs, alphas, betas = lax.scan(lanczos_step, start_carry, None, length=NUM_STEPS)[1]
    return jnp.concatenate([first_vec[None], later_vecs], axis=0), alphas, betas
```

```python
import functools

import jax
import jax.numpy as jnp
from jax import lax
from jax.experimental import pallas as pl
from jax.experimental.pallas import tpu as pltpu
from jax.sharding import PartitionSpec as P

NUM_STEPS = 6
MESH = pl.DeviceIdType.MESH
F32 = jnp.float32
BF16 = jnp.bfloat16

GA, GC = 16, 8
ROWS, COLS = 40, 80
BOND, PAIR, TERMS = 640, 16, 32
LANES = 128
VEC = BOND * BOND * PAIR


def remote(src, dst, send, recv, dev):
    return pltpu.make_async_remote_copy(src_ref=src, dst_ref=dst, send_sem=send, recv_sem=recv, device_id=(dev,), device_id_type=MESH)


def lane_roll(val, shift):
    shift = shift % LANES
    return val if shift == 0 else pltpu.roll(val, shift, axis=val.ndim - 1)


def lane_iota(val):
    return lax.broadcasted_iota(jnp.int32, val.shape, val.ndim - 1)


def take_piece(tiles, idx):
    tile, off = divmod(COLS * idx, LANES)
    out = lane_roll(tiles(tile), -off)
    lane = lane_iota(out)
    if off + COLS > LANES:
        out = jnp.where(lane < LANES - off, out, lane_roll(tiles(tile + 1), -off))
    return jnp.where(lane < COLS, out, jnp.zeros_like(out))


def dense_tile(pieces, tile):
    out = None
    for idx in range(8):
        shift = COLS * idx - LANES * tile
        if shift <= -COLS or shift >= LANES:
            continue
        moved = lane_roll(pieces(idx), shift)
        out = moved if out is None else jnp.where(lane_iota(moved) >= shift, moved, out)
    return out


def kernel(psi, lw, wbig, right, vecs, alphas, betas, lall, lh, rtmp, rt, ug, xs, ys, part, rd, ssum, ra, rb, fl, fr, fin,
           sig, vt, piece_buf, out_recv, outv, ar1, ar2, psi_s, psi_r, l_s, l_r, lf_s, lf_r, out_s, out_r, g_s, g_r, d_s, d_r,
           ring_s, ring_r, a1_s, a1_r, a2_s, a2_r, loc):
    me = lax.axis_index("rows")
    core = lax.rem(me, 2)
    x = lax.rem(me // 2, 4)
    y = lax.rem(me // 8, 4)
    z = me // 32
    i = me // 8
    j = lax.rem(me, 8)

    def in_row(dj):
        jj = lax.rem(j + dj, 8)
        return jj, i * 8 + jj

    def in_col(di):
        ii = lax.rem(i + di, PAIR)
        return ii, ii * 8 + j

    barrier = pltpu.get_barrier_semaphore()
    for dj in range(1, 8):
        pl.semaphore_signal(barrier, inc=1, device_id=(in_row(dj)[1],), device_id_type=MESH)
    for di in range(1, PAIR):
        pl.semaphore_signal(barrier, inc=1, device_id=(in_col(di)[1],), device_id_type=MESH)
    pl.semaphore_wait(barrier, 22)

    partner = me + 1 - 2 * core
    xdev = lambda xx: i * 8 + lax.rem(xx + 4, 4) * 2 + core

    cp_r = pltpu.make_async_copy(right.at[:, pl.ds(pl.multiple_of(j * COLS, COLS), COLS), :], rtmp.at[:, pl.ds(0, COLS), :], loc.at[0])
    cp_r.start()
    cp_l = pltpu.make_async_copy(lw, lall.at[j], loc.at[1])
    cp_l.start()

    for jj in range(8):
        piece_buf[jj] = take_piece(lambda t: psi[:, LANES * t:LANES * t + LANES], jj)
    my_rows = pl.ds(pl.multiple_of(j * COLS, COLS), COLS)
    vt[0, my_rows, :] = piece_buf[j]
    psi_copies = []
    for dj in range(1, 8):
        jj, dev = in_row(dj)
        cp = remote(piece_buf.at[jj], vt.at[0, my_rows], psi_s.at[jj], psi_r.at[j], dev)
        cp.start()
        psi_copies.append(cp)
    l_copies = []
    for dx in range(1, 4):
        xx = lax.rem(x + dx, 4)
        cp = remote(lw, lall.at[j], l_s.at[xx], l_r.at[x], i * 8 + xx * 2 + core)
        cp.start()
        l_copies.append(cp)
    cp = remote(lw, lall.at[j], lf_s.at[x], lf_r.at[x], partner)
    cp.start()
    l_copies.append(cp)

    row_lane = lax.broadcasted_iota(jnp.int32, (1, LANES), 1)

    def total(val):
        return jnp.sum(jnp.sum(val, axis=0, keepdims=True), axis=1, keepdims=True)

    def pack_row(n, s, e, c):
        zero = jnp.zeros((1, LANES), F32)
        return jnp.where(row_lane == 0, n, jnp.where(row_lane == 1, s, jnp.where(row_lane == 2, e, jnp.where(row_lane == 3, c, zero))))

    def merge(mat):
        lane = lax.broadcasted_iota(jnp.int32, mat.shape, 2)
        col = lambda idx: jnp.sum(jnp.where(lane == idx, mat, 0.0), axis=2, keepdims=True)
        n, s, e, c = col(0), col(1), col(2), col(3)
        mean = jnp.where(n > 0, s / jnp.where(n > 0, n, 1.0), 0.0)
        n_all, s_all, c_all = (jnp.sum(val, axis=0, keepdims=True) for val in (n, s, c))
        mean_all = jnp.where(n_all > 0, s_all / jnp.where(n_all > 0, n_all, 1.0), 0.0)
        diff = mean - mean_all
        e_all = jnp.sum(e + diff * n * diff, axis=0, keepdims=True)
        return tuple(val.reshape(1, 1) for val in (n_all, s_all, e_all, c_all))

    def all_reduce(n, s, e, c):
        ar1[j] = pack_row(n, s, e, c)
        copies = []
        for dj in range(1, 8):
            jj, dev = in_row(dj)
            cp = remote(ar1.at[j], ar1.at[j], a1_s.at[jj], a1_r.at[j], dev)
            cp.start()
            copies.append(cp)
        for dj in range(1, 8):
            jj, dev = in_row(dj)
            remote(ar1.at[jj], ar1.at[jj], a1_s.at[jj], a1_r.at[jj], dev).wait_recv()
        n, s, e, c = merge(ar1[...])
        ar2[i] = pack_row(n, s, e, c)
        for di in range(1, PAIR):
            ii, dev = in_col(di)
            cp = remote(ar2.at[i], ar2.at[i], a2_s.at[ii], a2_r.at[i], dev)
            cp.start()
            copies.append(cp)
        for di in range(1, PAIR):
            ii, dev = in_col(di)
            remote(ar2.at[ii], ar2.at[ii], a2_s.at[ii], a2_r.at[ii], dev).wait_recv()
        for cp in copies:
            cp.wait_send()
        return merge(ar2[...])

    psi_val = psi[...]
    n_psi = total(psi_val * psi_val)
    zero11 = jnp.zeros((1, 1), F32)
    n_psi = all_reduce(n_psi, zero11, zero11, zero11)[0]
    inv_norm = 1.0 / jnp.sqrt(n_psi / VEC)

    for dj in range(1, 8):
        jj, dev = in_row(dj)
        rows = pl.ds(pl.multiple_of(jj * COLS, COLS), COLS)
        remote(piece_buf.at[jj], vt.at[0, rows], psi_s.at[jj], psi_r.at[jj], dev).wait_recv()
    for cp in psi_copies:
        cp.wait_send()
    vt[0] = vt[0] * inv_norm
    vt[2] = jnp.zeros((BOND, LANES), F32)
    fin[...] = jnp.zeros((LANES, BOND), F32)

    cp_r.wait()
    def turn_right(k, carry):
        rtmp[k, pl.ds(COLS, 48), :] = jnp.zeros((48, BOND), BF16)
        for b in range(5):
            rt[pl.ds(LANES * b, LANES), pl.ds(pl.multiple_of(k * LANES, LANES), LANES)] = rtmp[k, :, pl.ds(LANES * b, LANES)].T
        return carry

    lax.fori_loop(0, TERMS, turn_right, 0)

    cp_l.wait()
    fwd = []
    for dx in range(1, 4):
        xx = lax.rem(x + dx, 4)
        src = xx * 2 + core
        remote(lw, lall.at[src], l_s.at[xx], l_r.at[xx], i * 8 + src).wait_recv()
        cp = remote(lall.at[src], lall.at[src], lf_s.at[xx], lf_r.at[xx], partner)
        cp.start()
        fwd.append(cp)
    for xx in range(4):
        src = xx * 2 + 1 - core
        remote(lw, lall.at[src], lf_s.at[xx], lf_r.at[xx], partner).wait_recv()
    for cp in l_copies + fwd:
        cp.wait_send()
    for t in range(8):
        block = lall[t]
        lane = lane_iota(block)
        for h in range(2):
            keep = (lane < 512) | (((lane // 8) % 2) == h)
            lh[h, pl.ds(160 * t, 160), :] = jnp.where(keep, block, jnp.zeros_like(block))

    def ring_ids(half, phase):
        base = half * 8 + phase * 4
        return base, base + 1, base + 2, base + 3

    def gather_phase(up, down, own, blocks, halves, ids):
        to_up, to_dn, fw_up, fw_dn = ids
        from_dn, from_up, far = blocks
        sends = [remote(own(None), own(None), g_s.at[to_up], g_r.at[to_up], up), remote(own(None), own(None), g_s.at[to_dn], g_r.at[to_dn], down)]
        for cp in sends:
            cp.start()

        def forward():
            remote(from_dn(None), from_dn(None), g_s.at[to_up], g_r.at[to_up], up).wait_recv()
            one = remote(from_dn(halves[0]), from_dn(halves[0]), g_s.at[fw_up], g_r.at[fw_up], up)
            one.start()
            remote(from_up(None), from_up(None), g_s.at[to_dn], g_r.at[to_dn], down).wait_recv()
            two = remote(from_up(halves[1]), from_up(halves[1]), g_s.at[fw_dn], g_r.at[fw_dn], down)
            two.start()
            sends.extend([one, two])

        def finish():
            remote(far(halves[0]), far(halves[0]), g_s.at[fw_up], g_r.at[fw_up], up).wait_recv()
            remote(far(halves[1]), far(halves[1]), g_s.at[fw_dn], g_r.at[fw_dn], down).wait_recv()

        return sends, forward, finish

    def wrap4(val):
        return lax.rem(val + 4, 4)

    y_up, y_dn = (z * 4 + wrap4(y + 1)) * 8 + j, (z * 4 + wrap4(y - 1)) * 8 + j
    z_up, z_dn = (wrap4(z + 1) * 4 + y) * 8 + j, (wrap4(z - 1) * 4 + y) * 8 + j
    PARTS = (((0, 12), (0, 6), (6, 6)), ((12, 13), (12, 6), (18, 7)))

    def gather():
        def one(zz, yy, whole):
            def ref(part):
                lo, cnt = part or whole
                return ug.at[zz, yy, pl.ds(lo, cnt)]
            return ref

        def z_bundle(zz, whole):
            def ref(part):
                lo, cnt = part or whole
                return ug.at[zz, :, pl.ds(lo, cnt)]
            return ref

        def y_bundle(yy, whole):
            def ref(part):
                lo, cnt = part or whole
                return ug.at[:, yy, pl.ds(lo, cnt)]
            return ref

        wa, wb = PARTS[0][0], PARTS[1][0]
        ha, hb = PARTS[0][1:], PARTS[1][1:]
        a1 = gather_phase(y_up, y_dn, one(z, y, wa), (one(z, wrap4(y - 1), wa), one(z, wrap4(y + 1), wa), one(z, wrap4(y + 2), wa)), ha, ring_ids(0, 0))
        b1 = gather_phase(z_up, z_dn, one(z, y, wb), (one(wrap4(z - 1), y, wb), one(wrap4(z + 1), y, wb), one(wrap4(z + 2), y, wb)), hb, ring_ids(1, 0))
        a1[1]()
        b1[1]()
        a1[2]()
        a2 = gather_phase(z_up, z_dn, z_bundle(z, wa), (z_bundle(wrap4(z - 1), wa), z_bundle(wrap4(z + 1), wa), z_bundle(wrap4(z + 2), wa)), ha, ring_ids(0, 1))
        b1[2]()
        b2 = gather_phase(y_up, y_dn, y_bundle(y, wb), (y_bundle(wrap4(y - 1), wb), y_bundle(wrap4(y + 1), wb), y_bundle(wrap4(y + 2), wb)), hb, ring_ids(1, 1))
        a2[1]()
        b2[1]()
        a2[2]()
        b2[2]()
        for ph in (a1, b1, a2, b2):
            for cp in ph[0]:
                cp.wait_send()

    def out_start(buf):
        copies = []
        for dj in range(1, 8):
            jj, dev = in_row(dj)
            rows = pl.ds(pl.multiple_of(jj * COLS, COLS), COLS)
            cp = remote(vt.at[buf, rows], out_recv.at[j], out_s.at[jj], out_r.at[j], dev)
            cp.start()
            copies.append(cp)
        out_recv[j] = vt[buf, my_rows, :]
        return copies

    def out_finish(copies, buf, step):
        for dj in range(1, 8):
            jj, dev = in_row(dj)
            rows = pl.ds(pl.multiple_of(jj * COLS, COLS), COLS)
            remote(vt.at[buf, rows], out_recv.at[jj], out_s.at[jj], out_r.at[jj], dev).wait_recv()
        for tile in range(5):
            outv[:, pl.ds(LANES * tile, LANES)] = dense_tile(lambda idx: out_recv[idx], tile)
        cp = pltpu.make_async_copy(outv, vecs.at[step], loc.at[2])
        cp.start()
        for other in copies:
            other.wait_send()
        return cp

    def step_body(step, beta):
        cur = lax.rem(step, 3)
        prev = lax.rem(step + 2, 3)
        nxt = lax.rem(step + 1, 3)

        strided = [vt[cur, pl.ds(r, ROWS, stride=PAIR), :] for r in range(PAIR)]
        for lt in range(5):
            half = [dense_tile(lambda idx, h=h: strided[8 * h + idx], lt) for h in range(2)]
            for h in range(2):
                for tt in range(2):
                    ug[z, y, lt * 5 + 2 * h + tt] = half[h][PAIR * tt:PAIR * tt + PAIR].astype(BF16)
            ug[z, y, lt * 5 + 4] = jnp.concatenate([half[0][32:ROWS], half[1][32:ROWS]], axis=0).astype(BF16)
        gather()
        out_copies = out_start(cur)
        v_cur = vt[cur]
        n_loc = total(v_cur * v_cur)
        c_loc = total(v_cur * vt[prev])

        def left_half(h, carry):
            def tiles(tr, lt):
                return ug[:, :, lt * 5 + tr].reshape(256, LANES)

            for rp in range(4):
                cols = []
                for rr in range(2):
                    idx = 2 * rp + rr
                    tail = take_piece(lambda t: tiles(4, t), idx)
                    main = [take_piece(lambda t, tt=tt: ug[:, :, t * 5 + 2 * h + tt].reshape(256, LANES), idx) for tt in range(2)]
                    cols.append(jnp.concatenate([main[0], main[1], tail], axis=0))
                rhs = jnp.concatenate(cols, axis=1)
                for mc in range(2):
                    res = jnp.dot(lh[h, pl.ds(BOND * mc, BOND), :], rhs, preferred_element_type=F32).astype(BF16)
                    for rr in range(2):
                        xs[h * 8 + 2 * rp + rr, pl.ds(BOND * mc, BOND), :] = res[:, LANES * rr:LANES * rr + LANES]
            return carry

        lax.fori_loop(0, 2, left_half, 0)

        def pair_rows(ap, carry):
            for h in range(2):
                rhs = jnp.concatenate([xs[:, pl.ds(pl.multiple_of(ap * 64 + 32 * aa + PAIR * h, PAIR), PAIR), :].reshape(256, LANES) for aa in range(2)], axis=1)
                res = jnp.dot(wbig[h], rhs, preferred_element_type=F32).astype(BF16)
                for aa in range(2):
                    for k in range(PAIR):
                        ys[pl.ds(pl.multiple_of(ap * 32 + PAIR * aa, PAIR), PAIR), pl.ds((PAIR * h + k) * LANES, LANES)] = res[PAIR * k:PAIR * k + PAIR, LANES * aa:LANES * aa + LANES]
            return carry

        lax.fori_loop(0, ROWS // 2, pair_rows, 0)

        for mc in range(2):
            res = lax.dot_general(rt[pl.ds(320 * mc, 320), :], ys[...], (((1,), (1,)), ((), ())), preferred_element_type=F32)
            for xx in range(2):
                for cc in range(2):
                    lo = (2 * xx + cc) * COLS
                    part[2 * mc + xx, cc] = res[lo:lo + COLS]

        cp_d = remote(part.at[:, 1 - core], rd, d_s, d_r, partner)
        cp_d.start()
        cp_o = out_finish(out_copies, cur, step)
        cp_d.wait()
        for xx in range(4):
            ssum[xx] = part[xx, core] + rd[xx]
        xo, xu, xd = wrap4(x + 2), wrap4(x + 1), wrap4(x - 1)
        up, dn = xdev(x + 1), xdev(x - 1)
        lo, hi = pl.ds(0, ROWS), pl.ds(ROWS, ROWS)
        c0 = remote(ssum.at[xo, lo], ra, ring_s.at[0], ring_r.at[0], up)
        c1 = remote(ssum.at[xo, hi], rb, ring_s.at[1], ring_r.at[1], dn)
        c2 = remote(ssum.at[xu, hi], fl.at[hi], ring_s.at[2], ring_r.at[2], up)
        c3 = remote(ssum.at[xd, lo], fr.at[lo], ring_s.at[3], ring_r.at[3], dn)
        for cp in (c0, c1, c2, c3):
            cp.start()
        c0.wait_recv()
        ssum[xu, lo] = ssum[xu, lo] + ra[...]
        c4 = remote(ssum.at[xu, lo], fl.at[lo], ring_s.at[4], ring_r.at[4], up)
        c4.start()
        c1.wait_recv()
        ssum[xd, hi] = ssum[xd, hi] + rb[...]
        c5 = remote(ssum.at[xd, hi], fr.at[hi], ring_s.at[5], ring_r.at[5], dn)
        c5.start()
        cp_o.wait()
        c2.wait_recv()
        c3.wait_recv()
        c4.wait_recv()
        c5.wait_recv()
        fin[pl.ds(0, COLS), :] = ssum[x] + fl[...] + fr[...]
        for cp in (c0, c1, c2, c3, c4, c5):
            cp.wait_send()
        for b in range(5):
            sig[pl.ds(LANES * b, LANES), :] = fin[:, pl.ds(LANES * b, LANES)].T

        t_val = sig[...] - beta * vt[prev]
        s_loc = total(t_val * vt[cur])
        own = jnp.where(n_loc > 0, s_loc / jnp.where(n_loc > 0, n_loc, 1.0), 0.0)
        sig[...] = t_val
        w_val = t_val - own * vt[cur]
        e_loc = total(w_val * w_val)
        n, s, e, c = all_reduce(n_loc, s_loc, e_loc, c_loc)
        alpha = (s + beta * c) / VEC
        diff = alpha - jnp.where(n > 0, s / jnp.where(n > 0, n, 1.0), 0.0)
        beta_new = jnp.sqrt((e + diff * n * diff) / VEC)
        alphas[pl.ds(step, 1), :] = jnp.broadcast_to(alpha, (1, LANES))
        betas[pl.ds(step, 1), :] = jnp.broadcast_to(beta_new, (1, LANES))
        inv = 1.0 / beta_new
        vt[nxt] = (sig[...] - alpha * vt[cur]) * inv
        return beta_new

    lax.fori_loop(0, NUM_STEPS, step_body, zero11)
    copies = out_start(NUM_STEPS % 3)
    out_finish(copies, NUM_STEPS % 3, NUM_STEPS).wait()


def run_kernel(psi, lw, wbig, right):
    vmem, anys = pl.BlockSpec(memory_space=pltpu.VMEM), pl.BlockSpec(memory_space=pl.ANY)
    dma = pltpu.SemaphoreType.DMA
    vm = pltpu.VMEM
    scratch = [
        vm((8, 160, 768), BF16), vm((2, 1280, 768), BF16), vm((TERMS, LANES, BOND), BF16), vm((BOND, 4096), BF16),
        vm((4, 4, 25, PAIR, LANES), BF16), vm((PAIR, 1280, LANES), BF16), vm((BOND, 4096), BF16), vm((4, 2, COLS, BOND), F32),
        vm((4, COLS, BOND), F32), vm((4, COLS, BOND), F32), vm((ROWS, BOND), F32), vm((ROWS, BOND), F32), vm((COLS, BOND), F32), vm((COLS, BOND), F32),
        vm((LANES, BOND), F32), vm((BOND, LANES), F32), vm((3, BOND, LANES), F32), vm((8, COLS, LANES), F32), vm((8, COLS, LANES), F32), vm((COLS, BOND), F32),
        vm((8, 1, LANES), F32), vm((PAIR, 1, LANES), F32),
        dma((8,)), dma((8,)), dma((4,)), dma((4,)), dma((4,)), dma((4,)), dma((8,)), dma((8,)), dma((PAIR,)), dma((PAIR,)), dma, dma,
        dma((6,)), dma((6,)), dma((8,)), dma((8,)), dma((PAIR,)), dma((PAIR,)), dma((3,)),
    ]
    return pl.pallas_call(
        kernel,
        out_shape=(jax.ShapeDtypeStruct((NUM_STEPS + 1, COLS, BOND), F32), jax.ShapeDtypeStruct((8, LANES), F32), jax.ShapeDtypeStruct((8, LANES), F32)),
        in_specs=[vmem, anys, vmem, anys],
        out_specs=(anys, vmem, vmem),
        scratch_shapes=scratch,
        compiler_params=pltpu.CompilerParams(collective_id=0, has_side_effects=True, vmem_limit_bytes=64 * 1024 * 1024 - 65536),
        name="lanczos",
    )(psi, lw, wbig, right)


def solution(mesh):
    def local_run(wave_rows, left_rows, op_pair, right_env):
        psi = wave_rows.reshape(COLS, BOND)
        left = jnp.transpose(left_rows, (1, 0, 2)).reshape(160, PAIR, ROWS)
        main = jnp.transpose(left[:, :, :32].reshape(160, PAIR, 2, PAIR), (0, 2, 1, 3)).reshape(160, 512)
        tail = jnp.broadcast_to(left[:, :, None, 32:], (160, PAIR, 2, 8)).reshape(160, 256)
        lw = jnp.concatenate([main, tail], axis=1)
        eye = jnp.eye(PAIR, dtype=bool)[None, :, None, None, :]
        wbig = jnp.where(eye, op_pair.reshape(2, PAIR, PAIR, PAIR)[..., None], jnp.zeros((), BF16)).reshape(2, 256, 256)
        vecs, alphas, betas = run_kernel(psi, lw, wbig, right_env)
        return vecs.reshape(7, 5, 4, 4, BOND), alphas[:6, 0], betas[:6, 0]

    rows = "rows"
    return jax.shard_map(local_run, mesh=mesh, in_specs=(P(rows), P(None, rows), P(), P()), out_specs=(P(None, rows), P(), P()), check_vma=False)
```

```python
import functools

import jax
import jax.numpy as jnp
from jax import lax
from jax.experimental import pallas as pl
from jax.experimental.pallas import tpu as pltpu
from jax.sharding import PartitionSpec as P

NUM_STEPS = 6
MESH = pl.DeviceIdType.MESH
F32 = jnp.float32
BF16 = jnp.bfloat16

ROWS, COLS = 40, 80
BOND, PAIR, TERMS = 640, 16, 32
LANES = 128
VEC = BOND * BOND * PAIR


def remote(src, dst, send, recv, dev):
    return pltpu.make_async_remote_copy(src_ref=src, dst_ref=dst, send_sem=send, recv_sem=recv, device_id=(dev,), device_id_type=MESH)


def lane_roll(val, shift):
    shift = shift % LANES
    return val if shift == 0 else pltpu.roll(val, shift, axis=val.ndim - 1)


def lane_iota(val):
    return lax.broadcasted_iota(jnp.int32, val.shape, val.ndim - 1)


def take_piece(tiles, idx):
    tile, off = divmod(COLS * idx, LANES)
    out = lane_roll(tiles(tile), -off)
    lane = lane_iota(out)
    if off + COLS > LANES:
        out = jnp.where(lane < LANES - off, out, lane_roll(tiles(tile + 1), -off))
    return jnp.where(lane < COLS, out, jnp.zeros_like(out))


def dense_tile(pieces, tile):
    out = None
    for idx in range(8):
        shift = COLS * idx - LANES * tile
        if shift <= -COLS or shift >= LANES:
            continue
        moved = lane_roll(pieces(idx), shift)
        out = moved if out is None else jnp.where(lane_iota(moved) >= shift, moved, out)
    return out


def kernel(psi, left, pair, right, vecs, alphas, betas, lall, lh, wbig, rtmp, rt, ug, xs, ys, part, rd, ssum, ra, rb, fl, fr, fin,
           sig, vt, piece_buf, out_recv, outv, ar1, ar2, psi_s, psi_r, l_s, l_r, out_s, out_r, g_s, g_r, d_s, d_r,
           ring_s, ring_r, a1_s, a1_r, a2_s, a2_r, loc):
    me = lax.axis_index("rows")
    core = lax.rem(me, 2)
    x = lax.rem(me // 2, 4)
    y = lax.rem(me // 8, 4)
    z = me // 32
    i = me // 8
    j = lax.rem(me, 8)
    lo, hi = pl.ds(0, ROWS), pl.ds(ROWS, ROWS)

    def wrap4(val):
        return lax.rem(val + 4, 4)

    def in_row(dj):
        jj = lax.rem(j + dj, 8)
        return jj, i * 8 + jj

    def in_col(di):
        ii = lax.rem(i + di, PAIR)
        return ii, ii * 8 + j

    def rows_of(jj):
        return pl.ds(pl.multiple_of(jj * COLS, COLS), COLS)

    barrier = pltpu.get_barrier_semaphore()
    for dj in range(1, 8):
        pl.semaphore_signal(barrier, inc=1, device_id=(in_row(dj)[1],), device_id_type=MESH)
    for di in range(1, PAIR):
        pl.semaphore_signal(barrier, inc=1, device_id=(in_col(di)[1],), device_id_type=MESH)
    pl.semaphore_wait(barrier, 22)

    partner = me + 1 - 2 * core
    x_up, x_dn = i * 8 + wrap4(x + 1) * 2 + core, i * 8 + wrap4(x - 1) * 2 + core
    my_rows = rows_of(j)

    cp_r = pltpu.make_async_copy(right.at[:, my_rows, :], rtmp.at[:, pl.ds(0, COLS), :], loc.at[0])
    cp_r.start()
    cp_l = pltpu.make_async_copy(left, lall.at[x, core], loc.at[1])
    cp_l.start()

    row_lane = lax.broadcasted_iota(jnp.int32, (1, LANES), 1)

    def total(val):
        return jnp.sum(jnp.sum(val, axis=0, keepdims=True), axis=1, keepdims=True)

    def ratio(num, den):
        good = den > 0
        return jnp.where(good, num / jnp.where(good, den, 1.0), 0.0)

    def pack_row(stats):
        row = jnp.zeros((1, LANES), F32)
        for idx, val in enumerate(stats):
            row = jnp.where(row_lane == idx, val, row)
        return row

    def merge(mat):
        lane = lax.broadcasted_iota(jnp.int32, mat.shape, 2)
        n, s, e, c = (jnp.sum(jnp.where(lane == idx, mat, 0.0), axis=2, keepdims=True) for idx in range(4))
        n_all, s_all, c_all = (jnp.sum(val, axis=0, keepdims=True) for val in (n, s, c))
        diff = ratio(s, n) - ratio(s_all, n_all)
        e_all = jnp.sum(e + diff * n * diff, axis=0, keepdims=True)
        return tuple(val.reshape(1, 1) for val in (n_all, s_all, e_all, c_all))

    def all_reduce(stats, first=None, second=None):
        ar1[j] = pack_row(stats)
        copies = []
        for dj in range(1, 8):
            jj, dev = in_row(dj)
            cp = remote(ar1.at[j], ar1.at[j], a1_s.at[jj], a1_r.at[j], dev)
            cp.start()
            copies.append(cp)
        if first:
            first()
        for dj in range(1, 8):
            jj, dev = in_row(dj)
            remote(ar1.at[jj], ar1.at[jj], a1_s.at[jj], a1_r.at[jj], dev).wait_recv()
        ar2[i] = pack_row(merge(ar1[...]))
        for di in range(1, PAIR):
            ii, dev = in_col(di)
            cp = remote(ar2.at[i], ar2.at[i], a2_s.at[ii], a2_r.at[i], dev)
            cp.start()
            copies.append(cp)
        if second:
            second()
        for di in range(1, PAIR):
            ii, dev = in_col(di)
            remote(ar2.at[ii], ar2.at[ii], a2_s.at[ii], a2_r.at[ii], dev).wait_recv()
        for cp in copies:
            cp.wait_send()
        return merge(ar2[...])

    def l_copy(src, rows, idx, dev):
        ref = lall.at[src[0], src[1], rows]
        return remote(ref, ref, l_s.at[idx], l_r.at[idx], dev)

    every, low, high = pl.ds(0, 160), pl.ds(0, COLS), pl.ds(COLS, COLS)

    def psi_sends():
        for jj in range(8):
            piece_buf[jj] = take_piece(lambda t: psi[:, LANES * t:LANES * t + LANES], jj)
        vt[0, my_rows, :] = piece_buf[j]
        for dj in range(1, 8):
            jj, dev = in_row(dj)
            remote(piece_buf.at[jj], vt.at[0, my_rows], psi_s.at[jj], psi_r.at[j], dev).start()
        cp_l.wait()
        l_copy((x, core), every, 0, x_up).start()
        l_copy((x, core), every, 1, x_dn).start()
        l_copy((x, core), every, 4, partner).start()
        spread = jnp.where(lax.broadcasted_iota(jnp.int32, (PAIR, 256), 1) // PAIR == lax.broadcasted_iota(jnp.int32, (PAIR, 256), 0), 1.0, 0.0).astype(BF16)
        same = lax.broadcasted_iota(jnp.int32, (256, 256), 1) % PAIR == lax.broadcasted_iota(jnp.int32, (256, 256), 0) // PAIR
        for h in range(2):
            wide = jnp.dot(pair[pl.ds(256 * h, 256), :], spread, preferred_element_type=F32)
            wbig[h] = jnp.where(same, wide, 0.0).astype(BF16)
        vt[2] = jnp.zeros((BOND, LANES), F32)
        fin[...] = jnp.zeros((LANES, BOND), F32)

    def turn_right():
        cp_r.wait()

        def body(k, carry):
            rtmp[k, pl.ds(COLS, 48), :] = jnp.zeros((48, BOND), BF16)
            for b in range(5):
                rt[pl.ds(LANES * b, LANES), pl.ds(pl.multiple_of(k * LANES, LANES), LANES)] = rtmp[k, :, pl.ds(LANES * b, LANES)].T
            return carry

        lax.fori_loop(0, TERMS, body, 0)

    psi_val = psi[...]
    n_psi = all_reduce([total(psi_val * psi_val)], psi_sends, turn_right)[0]
    inv_norm = 1.0 / jnp.sqrt(n_psi / VEC)

    for dj in range(1, 8):
        jj, dev = in_row(dj)
        cp = remote(piece_buf.at[jj], vt.at[0, rows_of(jj)], psi_s.at[jj], psi_r.at[jj], dev)
        cp.wait_recv()
        cp.wait_send()
    vt[0] = vt[0] * inv_norm
    outv[...] = psi_val * inv_norm
    cp_v = pltpu.make_async_copy(outv, vecs.at[0], loc.at[2])
    cp_v.start()

    lower, upper, far = (wrap4(x - 1), core), (wrap4(x + 1), core), (wrap4(x + 2), core)

    def left_forward():
        l_copy(lower, every, 0, x_up).wait_recv()
        l_copy(lower, low, 2, x_up).start()
        l_copy(upper, every, 1, x_dn).wait_recv()
        l_copy(upper, high, 3, x_dn).start()
        l_copy(lower, every, 5, partner).start()
        l_copy(upper, every, 6, partner).start()

    def left_finish():
        l_copy(far, low, 2, x_up).wait_recv()
        l_copy(far, high, 3, x_dn).wait_recv()
        l_copy(far, every, 7, partner).start()
        for idx, dx in ((4, 0), (5, 3), (6, 1), (7, 2)):
            l_copy((wrap4(x + dx), 1 - core), every, idx, partner).wait_recv()
        for idx, rows in enumerate((every, every, low, high, every, every, every, every)):
            l_copy((x, core), rows, idx, partner).wait_send()
        for h in range(2):
            src = lax.broadcasted_iota(jnp.int32, (BOND, 768), 0)
            col = lax.broadcasted_iota(jnp.int32, (BOND, 768), 1)
            group = (col % 256) // PAIR
            main = ROWS * group + PAIR * (col // 256) + col % PAIR
            tail = jnp.where((col // 8) % 2 == h, ROWS * group + 32 + col % 8, -1)
            order = jnp.where(src == jnp.where(col < 512, main, tail), 1.0, 0.0).astype(BF16)

            def body(t, carry):
                rows = pl.ds(pl.multiple_of(t * 160, 160), 160)
                lh[h, rows, :] = jnp.dot(lall[t // 2, t % 2], order, preferred_element_type=F32).astype(BF16)
                return carry

            lax.fori_loop(0, 8, body, 0)

    def flow(base, firsts, seconds, ref, parts):
        done = []
        offs = (0, -1, 1, 2)

        def send(blk, prt, idx, dev):
            here = ref(blk, parts[prt])
            cp = remote(here, here, g_s.at[base + idx], g_r.at[base + idx], dev)
            cp.start()
            done.append(cp)

        def wait(blk, prt, idx):
            here = ref(blk, parts[prt])
            remote(here, here, g_s.at[base + idx], g_r.at[base + idx], partner).wait_recv()

        def second(b, prt):
            for way in ((0, 1) if prt == 0 else (1, 0)):
                send((offs[b], 0), prt, 6 * b + 6 + 2 * way + prt, seconds[way])

        def second_forward(b):
            wait((offs[b], -1), 0, 6 * b + 6)
            send((offs[b], -1), 0, 6 * b + 10, seconds[0])
            wait((offs[b], 1), 1, 6 * b + 9)
            send((offs[b], 1), 1, 6 * b + 11, seconds[1])

        for prt, way in ((0, 0), (1, 1), (1, 0), (0, 1)):
            send((0, 0), prt, 2 * way + prt, firsts[way])
        yield
        second(0, 0)
        second(0, 1)
        yield
        wait((-1, 0), 0, 0)
        send((-1, 0), 0, 4, firsts[0])
        second(1, 0)
        yield
        wait((1, 0), 1, 3)
        send((1, 0), 1, 5, firsts[1])
        second(2, 1)
        yield
        wait((-1, 0), 1, 1)
        second(1, 1)
        wait((1, 0), 0, 2)
        second(2, 0)
        yield
        second_forward(0)
        yield
        wait((2, 0), 0, 4)
        second(3, 0)
        wait((2, 0), 1, 5)
        second(3, 1)
        yield
        for b in range(1, 4):
            second_forward(b)
            yield
        for b in range(4):
            for off, prt, idx in ((-1, 1, 7), (1, 0, 8), (2, 0, 10), (2, 1, 11)):
                wait((offs[b], off), prt, 6 * b + idx)
        for cp in done:
            cp.wait_send()
        yield

    def device(zz, yy):
        return (wrap4(zz) * 4 + wrap4(yy)) * 8 + j

    y_ways, z_ways = (device(z, y + 1), device(z, y - 1)), (device(z + 1, y), device(z - 1, y))

    def gather(busy):
        def y_first(blk, prt):
            return ug.at[wrap4(z + blk[1]), wrap4(y + blk[0]), pl.ds(*prt)]

        def z_first(blk, prt):
            return ug.at[wrap4(z + blk[0]), wrap4(y + blk[1]), pl.ds(*prt)]

        both = [flow(0, y_ways, z_ways, y_first, ((0, 6), (6, 6))), flow(30, z_ways, y_ways, z_first, ((12, 6), (18, 7)))]
        for idx, unused in enumerate(zip(*both)):
            if idx == 1:
                busy()

    def out_copy(slot, jj, dev):
        return remote(sig.at[rows_of(jj)], out_recv.at[slot], out_s.at[jj], out_r.at[slot], dev)

    def out_start():
        for dj in range(1, 8):
            jj, dev = in_row(dj)
            out_copy(j, jj, dev).start()
        out_recv[j] = sig[my_rows, :]

    def out_finish(step):
        for dj in range(1, 8):
            jj, dev = in_row(dj)
            out_copy(jj, jj, dev).wait_recv()
            out_copy(j, jj, dev).wait_send()
        cp_v.wait()
        alpha, inv = fin[pl.ds(COLS, 1), pl.ds(0, 1)], fin[pl.ds(COLS + 8, 1), pl.ds(0, 1)]
        for tile in range(5):
            lanes = pl.ds(LANES * tile, LANES)
            outv[:, lanes] = (dense_tile(lambda idx: out_recv[idx], tile) - alpha * outv[:, lanes]) * inv
        pltpu.make_async_copy(outv, vecs.at[step], loc.at[2]).start()

    def step_body(step, beta):
        cur = lax.rem(step, 3)
        prev = lax.rem(step + 2, 3)
        nxt = lax.rem(step + 1, 3)

        with jax.named_scope("pack"):
            strided = [vt[cur, pl.ds(r, ROWS, stride=PAIR), :] for r in range(PAIR)]
            for lt in range(5):
                half = [dense_tile(lambda idx, h=h: strided[8 * h + idx], lt) for h in range(2)]
                for h in range(2):
                    for tt in range(2):
                        ug[z, y, lt * 5 + 2 * h + tt] = half[h][PAIR * tt:PAIR * tt + PAIR].astype(BF16)
                ug[z, y, lt * 5 + 4] = jnp.concatenate([half[0][32:ROWS], half[1][32:ROWS]], axis=0).astype(BF16)

        def busy():
            @pl.when(step == 0)
            def _():
                left_forward()

            @pl.when(step > 0)
            def _():
                out_finish(step)

        with jax.named_scope("gather"):
            gather(busy)

        @pl.when(step == 0)
        def _():
            with jax.named_scope("leftfin"):
                left_finish()

        def left_half(h, carry):
            for rp in range(4):
                cols = []
                for rr in range(2):
                    idx = 2 * rp + rr
                    rows = [take_piece(lambda t, tr=tr: ug[:, :, t * 5 + tr].reshape(256, LANES), idx) for tr in (2 * h, 2 * h + 1, 4)]
                    cols.append(jnp.concatenate(rows, axis=0))
                rhs = jnp.concatenate(cols, axis=1)
                for mc in range(2):
                    rows = pl.ds(BOND * mc, BOND)
                    res = jnp.dot(lh[h, rows, :], rhs, preferred_element_type=F32).astype(BF16)
                    for rr in range(2):
                        xs[h * 8 + 2 * rp + rr, rows, :] = res[:, LANES * rr:LANES * rr + LANES]
            return carry

        with jax.named_scope("lstage"):
            lax.fori_loop(0, 2, left_half, 0)

        def some_rows(ap, carry):
            for pr in range(4):
                for h in range(2):
                    starts = [pl.multiple_of((ap * 8 + 2 * pr + aa) * 32 + PAIR * h, PAIR) for aa in range(2)]
                    rhs = jnp.concatenate([xs[:, pl.ds(start, PAIR), :].reshape(256, LANES) for start in starts], axis=1)
                    res = jnp.dot(wbig[h], rhs, preferred_element_type=F32).astype(BF16)
                    for aa in range(2):
                        rows = pl.ds(pl.multiple_of((ap * 8 + 2 * pr + aa) * PAIR, PAIR), PAIR)
                        for k in range(PAIR):
                            ys[rows, pl.ds((PAIR * h + k) * LANES, LANES)] = res[PAIR * k:PAIR * k + PAIR, LANES * aa:LANES * aa + LANES]
            return carry

        with jax.named_scope("wstage"):
            lax.fori_loop(0, 5, some_rows, 0)

        spots = [wrap4(x + dx) for dx in (2, 1, 3, 0)]

        def sigma(first, cols):
            lhs = jnp.concatenate([rt[pl.ds(pl.multiple_of(spot * 160, 160), 160), :] for spot in spots[first:first + 2]], axis=0)
            res = lax.dot_general(lhs, ys[cols, :], (((1,), (1,)), ((), ())), preferred_element_type=F32)
            for idx in range(4):
                part[first + idx // 2, idx % 2, :, cols] = res[idx * COLS:idx * COLS + COLS]

        def swap(first):
            return remote(part.at[pl.ds(first, 2), 1 - core], rd.at[pl.ds(first, 2)], d_s.at[first // 2], d_r.at[first // 2], partner)

        def add_pair(first):
            swap(first).wait()
            for slot in (first, first + 1):
                ssum[slot] = part[slot, core] + rd[slot]

        def ring(slot, rows, dst, idx, dev):
            return remote(ssum.at[slot, rows], dst, ring_s.at[idx], ring_r.at[idx], dev)

        copies = [ring(0, lo, ra, 0, x_up), ring(0, hi, rb, 1, x_dn), ring(1, hi, fl.at[hi], 2, x_up), ring(2, lo, fr.at[lo], 3, x_dn),
                  ring(1, lo, fl.at[lo], 4, x_up), ring(2, hi, fr.at[hi], 5, x_dn)]
        with jax.named_scope("rstage"):
            sigma(0, pl.ds(0, BOND))
            swap(0).start()
            sigma(2, pl.ds(0, 384))
        with jax.named_scope("ring0"):
            add_pair(0)
            for cp in copies[:3]:
                cp.start()
        with jax.named_scope("rstage2"):
            sigma(2, pl.ds(384, 256))
            swap(2).start()
        with jax.named_scope("xring"):
            add_pair(2)
            copies[3].start()
            copies[0].wait_recv()
            ssum[1, lo] = ssum[1, lo] + ra[...]
            copies[4].start()
            copies[1].wait_recv()
            ssum[2, hi] = ssum[2, hi] + rb[...]
            copies[5].start()
            v_cur = vt[cur]
            n_loc = total(v_cur * v_cur)
            c_loc = total(v_cur * vt[prev])
            for cp in copies[2:]:
                cp.wait_recv()
            fin[pl.ds(0, COLS), :] = ssum[3] + fl[...] + fr[...]
            for cp in copies:
                cp.wait_send()
        with jax.named_scope("turn"):
            for b in range(5):
                rows = pl.ds(LANES * b, LANES)
                sig[rows, :] = jnp.where(row_lane < COLS, fin[:, rows].T, 0.0)

        with jax.named_scope("vec1"):
            t_val = sig[...] - beta * vt[prev]
            s_loc = total(t_val * vt[cur])
            sig[...] = t_val
            w_val = t_val - ratio(s_loc, n_loc) * vt[cur]
            e_loc = total(w_val * w_val)
        with jax.named_scope("allred"):
            n, s, e, c = all_reduce([n_loc, s_loc, e_loc, c_loc], out_start)
        with jax.named_scope("vec2"):
            alpha = (s + beta * c) / VEC
            diff = alpha - ratio(s, n)
            beta_new = jnp.sqrt((e + diff * n * diff) / VEC)
            inv = 1.0 / beta_new
            vt[nxt] = (sig[...] - alpha * vt[cur]) * inv
            fin[pl.ds(COLS, 1), :] = jnp.broadcast_to(alpha, (1, BOND))
            fin[pl.ds(COLS + 8, 1), :] = jnp.broadcast_to(inv, (1, BOND))
            alphas[step] = alpha[0, 0]
            betas[step] = beta_new[0, 0]
        return beta_new

    lax.fori_loop(0, NUM_STEPS, step_body, jnp.zeros((1, 1), F32))
    out_finish(NUM_STEPS)
    cp_v.wait()


def run_kernel(psi, left, pair, right):
    vmem, anys, smem = (pl.BlockSpec(memory_space=space) for space in (pltpu.VMEM, pl.ANY, pltpu.SMEM))
    dma = pltpu.SemaphoreType.DMA
    vm = pltpu.VMEM
    block = (COLS, BOND)
    scratch = [
        vm((4, 2, 160, BOND), BF16), vm((2, 1280, 768), BF16), vm((2, 256, 256), BF16), vm((TERMS, LANES, BOND), BF16), vm((BOND, 4096), BF16),
        vm((4, 4, 25, PAIR, LANES), BF16), vm((PAIR, 1280, LANES), BF16), vm((BOND, 4096), BF16), vm((4, 2) + block, F32),
        vm((4,) + block, F32), vm((4,) + block, F32), vm((ROWS, BOND), F32), vm((ROWS, BOND), F32), vm(block, F32), vm(block, F32),
        vm((LANES, BOND), F32), vm((BOND, LANES), F32), vm((3, BOND, LANES), F32), vm((8, COLS, LANES), F32), vm((8, COLS, LANES), F32), vm(block, F32),
        vm((8, 1, LANES), F32), vm((PAIR, 1, LANES), F32),
    ] + [dma((num,)) for num in (8, 8, 8, 8, 8, 8, 60, 60, 2, 2, 6, 6, 8, 8, PAIR, PAIR, 3)]
    scal = jax.ShapeDtypeStruct((NUM_STEPS,), F32)
    return pl.pallas_call(
        kernel,
        out_shape=(jax.ShapeDtypeStruct((NUM_STEPS + 1,) + block, F32), scal, scal),
        in_specs=[vmem, anys, vmem, anys],
        out_specs=(anys, smem, smem),
        scratch_shapes=scratch,
        compiler_params=pltpu.CompilerParams(collective_id=0, has_side_effects=True, vmem_limit_bytes=67043328),
        name="lanczos",
    )(psi, left, pair, right)


def solution(mesh):
    def local_run(wave_rows, left_rows, op_pair, right_env):
        psi = wave_rows.reshape(COLS, BOND)
        left = jnp.transpose(left_rows, (1, 0, 2)).reshape(160, BOND)
        vecs, alphas, betas = run_kernel(psi, left, op_pair.reshape(512, PAIR), right_env)
        return vecs.reshape(7, 5, 4, 4, BOND), alphas, betas

    rows = "rows"
    return jax.shard_map(local_run, mesh=mesh, in_specs=(P(rows), P(None, rows), P(), P()), out_specs=(P(None, rows), P(), P()), check_vma=False)
```

```python
import functools

import jax
import jax.numpy as jnp
from jax import lax
from jax.experimental import pallas as pl
from jax.experimental.pallas import tpu as pltpu
from jax.sharding import PartitionSpec as P

NUM_STEPS = 6
MESH = pl.DeviceIdType.MESH
F32 = jnp.float32
BF16 = jnp.bfloat16

ROWS, COLS = 40, 80
BOND, PAIR, TERMS = 640, 16, 32
LANES = 128
VEC = BOND * BOND * PAIR


def remote(src, dst, send, recv, dev):
    return pltpu.make_async_remote_copy(src_ref=src, dst_ref=dst, send_sem=send, recv_sem=recv, device_id=(dev,), device_id_type=MESH)


def lane_roll(val, shift):
    shift = shift % LANES
    return val if shift == 0 else pltpu.roll(val, shift, axis=val.ndim - 1)


def lane_iota(val):
    return lax.broadcasted_iota(jnp.int32, val.shape, val.ndim - 1)


def take_piece(tiles, idx):
    tile, off = divmod(COLS * idx, LANES)
    out = lane_roll(tiles(tile), -off)
    lane = lane_iota(out)
    if off + COLS > LANES:
        out = jnp.where(lane < LANES - off, out, lane_roll(tiles(tile + 1), -off))
    return jnp.where(lane < COLS, out, jnp.zeros_like(out))


def dense_tile(pieces, tile):
    out = None
    for idx in range(8):
        shift = COLS * idx - LANES * tile
        if shift <= -COLS or shift >= LANES:
            continue
        moved = lane_roll(pieces(idx), shift)
        out = moved if out is None else jnp.where(lane_iota(moved) >= shift, moved, out)
    return out


def kernel(psi, left, pair, right, vecs, alphas, betas, lall, lh, wbig, rtmp, rt, ug, xs, ys, part, rd, ssum, ra, rb, fl, fr, fin,
           sig, vt, piece_buf, out_recv, outv, stat, psi_s, psi_r, l_s, l_r, out_s, out_r, g_s, g_r, d_s, d_r,
           ring_s, ring_r, a_s, a_r, loc):
    me = lax.axis_index("rows")
    core = lax.rem(me, 2)
    x = lax.rem(me // 2, 4)
    y = lax.rem(me // 8, 4)
    z = me // 32
    i = me // 8
    j = lax.rem(me, 8)
    lo, hi = pl.ds(0, ROWS), pl.ds(ROWS, ROWS)

    def wrap4(val):
        return lax.rem(val + 4, 4)

    def in_row(dj):
        jj = lax.rem(j + dj, 8)
        return jj, i * 8 + jj

    def rows_of(jj):
        return pl.ds(pl.multiple_of(jj * COLS, COLS), COLS)

    barrier = pltpu.get_barrier_semaphore()

    def greet(d, carry):
        pl.semaphore_signal(barrier, inc=1, device_id=(lax.rem(me + d, LANES),), device_id_type=MESH)
        return carry

    lax.fori_loop(1, LANES, greet, 0)
    pl.semaphore_wait(barrier, LANES - 1)

    partner = me + 1 - 2 * core
    x_up, x_dn = i * 8 + wrap4(x + 1) * 2 + core, i * 8 + wrap4(x - 1) * 2 + core
    my_rows = rows_of(j)

    cp_r = pltpu.make_async_copy(right.at[:, my_rows, :], rtmp.at[:, pl.ds(0, COLS), :], loc.at[0])
    cp_r.start()
    cp_l = pltpu.make_async_copy(left, lall.at[x, core], loc.at[1])
    cp_l.start()

    row_lane = lax.broadcasted_iota(jnp.int32, (1, LANES), 1)

    def total(val):
        return jnp.sum(jnp.sum(val, axis=0, keepdims=True), axis=1, keepdims=True)

    def ratio(num, den):
        good = den > 0
        return jnp.where(good, num / jnp.where(good, den, 1.0), 0.0)

    def all_reduce(stats, hook):
        row = jnp.zeros((1, LANES), F32)
        for idx, val in enumerate(stats):
            row = jnp.where(row_lane == idx, val, row)
        stat[me, pl.ds(0, 1), :] = row
        stat[me, pl.ds(1, 1), :] = jnp.broadcast_to(ratio(stats[1], stats[0]), (1, LANES))

        def give(d, carry):
            dev = lax.rem(me + d, LANES)
            remote(stat.at[me], stat.at[me], a_s, a_r, dev).start()
            return carry

        lax.fori_loop(1, LANES, give, 0, unroll=True)
        hook()
        most = stat.at[pl.ds(0, LANES - 1)]
        remote(most, most, a_s, a_r, partner).wait()
        rows = stat[:, pl.ds(0, 1), :]
        sums = jnp.sum(rows, axis=0)
        n, s, e, c = (jnp.sum(jnp.where(row_lane == idx, sums, 0.0), axis=1, keepdims=True) for idx in range(4))
        diff = stat[:, pl.ds(1, 1), :] - ratio(s, n)[None]
        moved = jnp.sum(diff * rows * diff, axis=0)
        return n, s, e + jnp.sum(jnp.where(row_lane == 0, moved, 0.0), axis=1, keepdims=True), c

    def l_copy(src, rows, idx, dev):
        ref = lall.at[src[0], src[1], rows]
        return remote(ref, ref, l_s.at[idx], l_r.at[idx], dev)

    every, low, high = pl.ds(0, 160), pl.ds(0, COLS), pl.ds(COLS, COLS)

    def psi_sends():
        for jj in range(8):
            piece_buf[jj] = take_piece(lambda t: psi[:, LANES * t:LANES * t + LANES], jj)
        vt[0, my_rows, :] = piece_buf[j]
        for dj in range(1, 8):
            jj, dev = in_row(dj)
            remote(piece_buf.at[jj], vt.at[0, my_rows], psi_s.at[jj], psi_r.at[j], dev).start()
        cp_l.wait()
        l_copy((x, core), every, 0, x_up).start()
        l_copy((x, core), every, 1, x_dn).start()
        l_copy((x, core), every, 4, partner).start()
        spread = jnp.where(lax.broadcasted_iota(jnp.int32, (PAIR, 256), 1) // PAIR == lax.broadcasted_iota(jnp.int32, (PAIR, 256), 0), 1.0, 0.0).astype(BF16)
        same = lax.broadcasted_iota(jnp.int32, (256, 256), 1) % PAIR == lax.broadcasted_iota(jnp.int32, (256, 256), 0) // PAIR
        for h in range(2):
            wide = jnp.dot(pair[pl.ds(256 * h, 256), :], spread, preferred_element_type=F32)
            wbig[h] = jnp.where(same, wide, 0.0).astype(BF16)
        vt[2] = jnp.zeros((BOND, LANES), F32)
        fin[...] = jnp.zeros((LANES, BOND), F32)

    def turn_right():
        cp_r.wait()

        def body(k, carry):
            rtmp[k, pl.ds(COLS, 48), :] = jnp.zeros((48, BOND), BF16)
            for b in range(5):
                rt[pl.ds(LANES * b, LANES), pl.ds(pl.multiple_of(k * LANES, LANES), LANES)] = rtmp[k, :, pl.ds(LANES * b, LANES)].T
            return carry

        lax.fori_loop(0, TERMS, body, 0)

    lower, upper, far = (wrap4(x - 1), core), (wrap4(x + 1), core), (wrap4(x + 2), core)

    def left_forward():
        l_copy(lower, every, 0, x_up).wait_recv()
        l_copy(lower, low, 2, x_up).start()
        l_copy(upper, every, 1, x_dn).wait_recv()
        l_copy(upper, high, 3, x_dn).start()
        l_copy(lower, every, 5, partner).start()
        l_copy(upper, every, 6, partner).start()

    def start_up():
        psi_sends()
        turn_right()
        left_forward()

    psi_val = psi[...]
    zero = jnp.zeros((1, 1), F32)
    n_psi = all_reduce([total(psi_val * psi_val), zero], start_up)[0]
    inv_norm = 1.0 / jnp.sqrt(n_psi / VEC)

    for dj in range(1, 8):
        jj, dev = in_row(dj)
        cp = remote(piece_buf.at[jj], vt.at[0, rows_of(jj)], psi_s.at[jj], psi_r.at[jj], dev)
        cp.wait_recv()
        cp.wait_send()
    vt[0] = vt[0] * inv_norm
    outv[...] = psi_val * inv_norm
    cp_v = pltpu.make_async_copy(outv, vecs.at[0], loc.at[2])
    cp_v.start()

    def left_finish():
        l_copy(far, low, 2, x_up).wait_recv()
        l_copy(far, high, 3, x_dn).wait_recv()
        l_copy(far, every, 7, partner).start()
        for idx, dx in ((4, 0), (5, 3), (6, 1), (7, 2)):
            l_copy((wrap4(x + dx), 1 - core), every, idx, partner).wait_recv()
        for idx, rows in enumerate((every, every, low, high, every, every, every, every)):
            l_copy((x, core), rows, idx, partner).wait_send()
        for h in range(2):
            src = lax.broadcasted_iota(jnp.int32, (BOND, 768), 0)
            col = lax.broadcasted_iota(jnp.int32, (BOND, 768), 1)
            group = (col % 256) // PAIR
            main = ROWS * group + PAIR * (col // 256) + col % PAIR
            tail = jnp.where((col // 8) % 2 == h, ROWS * group + 32 + col % 8, -1)
            order = jnp.where(src == jnp.where(col < 512, main, tail), 1.0, 0.0).astype(BF16)

            def body(t, carry):
                rows = pl.ds(pl.multiple_of(t * 160, 160), 160)
                lh[h, rows, :] = jnp.dot(lall[t // 2, t % 2], order, preferred_element_type=F32).astype(BF16)
                return carry

            lax.fori_loop(0, 8, body, 0)

    def flow(base, firsts, seconds, ref, parts):
        done = []
        offs = (0, -1, 1, 2)

        def send(blk, prt, idx, dev):
            here = ref(blk, parts[prt])
            cp = remote(here, here, g_s.at[base + idx], g_r.at[base + idx], dev)
            cp.start()
            done.append(cp)

        def wait(blk, prt, idx):
            here = ref(blk, parts[prt])
            remote(here, here, g_s.at[base + idx], g_r.at[base + idx], partner).wait_recv()

        def second(b, prt):
            for way in ((0, 1) if prt == 0 else (1, 0)):
                send((offs[b], 0), prt, 6 * b + 6 + 2 * way + prt, seconds[way])

        def second_forward(b):
            wait((offs[b], -1), 0, 6 * b + 6)
            send((offs[b], -1), 0, 6 * b + 10, seconds[0])
            wait((offs[b], 1), 1, 6 * b + 9)
            send((offs[b], 1), 1, 6 * b + 11, seconds[1])

        for prt, way in ((0, 0), (1, 1), (1, 0), (0, 1)):
            send((0, 0), prt, 2 * way + prt, firsts[way])
        for prt in range(2):
            send((0, 0), prt, 4 + prt, firsts[2])
        yield
        second(0, 0)
        second(0, 1)
        yield
        wait((-1, 0), 0, 0)
        second(1, 0)
        yield
        wait((1, 0), 1, 3)
        second(2, 1)
        yield
        wait((-1, 0), 1, 1)
        second(1, 1)
        wait((1, 0), 0, 2)
        second(2, 0)
        yield
        second_forward(0)
        yield
        wait((2, 0), 0, 4)
        second(3, 0)
        wait((2, 0), 1, 5)
        second(3, 1)
        yield
        for b in range(1, 4):
            second_forward(b)
            yield
        for b in range(4):
            for off, prt, idx in ((-1, 1, 7), (1, 0, 8), (2, 0, 10), (2, 1, 11)):
                wait((offs[b], off), prt, 6 * b + idx)
        for cp in done:
            cp.wait_send()
        yield

    def device(zz, yy):
        return (wrap4(zz) * 4 + wrap4(yy)) * 8 + j

    y_ways, z_ways = (device(z, y + 1), device(z, y - 1), device(z, y + 2)), (device(z + 1, y), device(z - 1, y), device(z + 2, y))

    def gather(busy):
        def y_first(blk, prt):
            return ug.at[wrap4(z + blk[1]), wrap4(y + blk[0]), pl.ds(*prt)]

        def z_first(blk, prt):
            return ug.at[wrap4(z + blk[0]), wrap4(y + blk[1]), pl.ds(*prt)]

        both = [flow(0, y_ways, z_ways, y_first, ((0, 6), (6, 6))), flow(30, z_ways, y_ways, z_first, ((12, 6), (18, 7)))]
        for idx, unused in enumerate(zip(*both)):
            if idx in busy:
                busy[idx]()

    def out_copy(slot, jj, dev):
        return remote(sig.at[rows_of(jj)], out_recv.at[slot], out_s.at[jj], out_r.at[slot], dev)

    def out_start():
        for dj in range(1, 8):
            jj, dev = in_row(dj)
            out_copy(j, jj, dev).start()
        out_recv[j] = sig[my_rows, :]

    def out_finish(step):
        for dj in range(1, 8):
            jj, dev = in_row(dj)
            out_copy(jj, jj, dev).wait_recv()
            out_copy(j, jj, dev).wait_send()
        cp_v.wait()
        alpha, inv = fin[pl.ds(COLS, 1), pl.ds(0, 1)], fin[pl.ds(COLS + 8, 1), pl.ds(0, 1)]
        for tile in range(5):
            lanes = pl.ds(LANES * tile, LANES)
            outv[:, lanes] = (dense_tile(lambda idx: out_recv[idx], tile) - alpha * outv[:, lanes]) * inv
        pltpu.make_async_copy(outv, vecs.at[step], loc.at[2]).start()

    def step_body(step, beta):
        cur = lax.rem(step, 3)
        prev = lax.rem(step + 2, 3)
        nxt = lax.rem(step + 1, 3)

        with jax.named_scope("pack"):
            strided = [vt[cur, pl.ds(r, ROWS, stride=PAIR), :] for r in range(PAIR)]
            for lt in range(5):
                half = [dense_tile(lambda idx, h=h: strided[8 * h + idx], lt) for h in range(2)]
                for h in range(2):
                    for tt in range(2):
                        ug[z, y, lt * 5 + 2 * h + tt] = half[h][PAIR * tt:PAIR * tt + PAIR].astype(BF16)
                ug[z, y, lt * 5 + 4] = jnp.concatenate([half[0][32:ROWS], half[1][32:ROWS]], axis=0).astype(BF16)

        def first_step():
            @pl.when(step == 0)
            def _():
                left_finish()

        def later_step():
            @pl.when(step > 0)
            def _():
                out_finish(step)

        with jax.named_scope("gather"):
            gather({1: first_step, 6: later_step})

        def left_half(h, carry):
            for rp in range(4):
                cols = []
                for rr in range(2):
                    idx = 2 * rp + rr
                    rows = [take_piece(lambda t, tr=tr: ug[:, :, t * 5 + tr].reshape(256, LANES), idx) for tr in (2 * h, 2 * h + 1, 4)]
                    cols.append(jnp.concatenate(rows, axis=0))
                rhs = jnp.concatenate(cols, axis=1)
                for mc in range(2):
                    rows = pl.ds(BOND * mc, BOND)
                    res = jnp.dot(lh[h, rows, :], rhs, preferred_element_type=F32).astype(BF16)
                    for rr in range(2):
                        xs[h * 8 + 2 * rp + rr, rows, :] = res[:, LANES * rr:LANES * rr + LANES]
            return carry

        with jax.named_scope("lstage"):
            lax.fori_loop(0, 2, left_half, 0)

        def some_rows(ap, carry):
            for pr in range(4):
                for h in range(2):
                    starts = [pl.multiple_of((ap * 8 + 2 * pr + aa) * 32 + PAIR * h, PAIR) for aa in range(2)]
                    rhs = jnp.concatenate([xs[:, pl.ds(start, PAIR), :].reshape(256, LANES) for start in starts], axis=1)
                    res = jnp.dot(wbig[h], rhs, preferred_element_type=F32).astype(BF16)
                    for aa in range(2):
                        rows = pl.ds(pl.multiple_of((ap * 8 + 2 * pr + aa) * PAIR, PAIR), PAIR)
                        for k in range(PAIR):
                            ys[rows, pl.ds((PAIR * h + k) * LANES, LANES)] = res[PAIR * k:PAIR * k + PAIR, LANES * aa:LANES * aa + LANES]
            return carry

        xo, xu, xd = wrap4(x + 2), wrap4(x + 1), wrap4(x - 1)

        def sigma(cols):
            for half in range(2):
                res = lax.dot_general(rt[pl.ds(320 * half, 320), :], ys[cols, :], (((1,), (1,)), ((), ())), preferred_element_type=F32)
                for idx in range(4):
                    part[2 * half + idx // 2, idx % 2, :, cols] = res[idx * COLS:idx * COLS + COLS]

        class Chunk:
            def __init__(self, num, start, width):
                cols = self.cols = pl.ds(start, width)
                self.rows = start // LANES, (start + width) // LANES
                self.swap = remote(part.at[:, 1 - core, :, cols], rd.at[:, :, cols], d_s.at[num], d_r.at[num], partner)
                plan = ((xo, lo, ra, lo, x_up), (xo, hi, rb, lo, x_dn), (xu, hi, fl, hi, x_up), (xd, lo, fr, lo, x_dn), (xu, lo, fl, lo, x_up), (xd, hi, fr, hi, x_dn))
                self.copies = [remote(ssum.at[chip, rows, cols], dst.at[to, cols], ring_s.at[6 * num + idx], ring_r.at[6 * num + idx], dev)
                               for idx, (chip, rows, dst, to, dev) in enumerate(plan)]

            def make_y(self):
                lax.fori_loop(*self.rows, some_rows, 0)

            def make(self):
                sigma(self.cols)
                self.swap.start()

            def add(self):
                self.swap.wait()
                for chip in range(4):
                    ssum[chip, :, self.cols] = part[chip, core, :, self.cols] + rd[chip, :, self.cols]
                for cp in self.copies[:4]:
                    cp.start()

            def pass_on(self):
                self.copies[0].wait_recv()
                ssum[xu, lo, self.cols] = ssum[xu, lo, self.cols] + ra[:, self.cols]
                self.copies[4].start()
                self.copies[1].wait_recv()
                ssum[xd, hi, self.cols] = ssum[xd, hi, self.cols] + rb[:, self.cols]
                self.copies[5].start()

            def finish(self):
                for cp in self.copies[2:]:
                    cp.wait_recv()
                fin[pl.ds(0, COLS), self.cols] = ssum[x, :, self.cols] + fl[:, self.cols] + fr[:, self.cols]
                for cp in self.copies:
                    cp.wait_send()

        one, two, three = (Chunk(*spec) for spec in ((0, 0, 256), (1, 256, 256), (2, 512, LANES)))
        with jax.named_scope("w0"):
            one.make_y()
        with jax.named_scope("r0"):
            one.make()
        with jax.named_scope("w1"):
            two.make_y()
        with jax.named_scope("add0"):
            one.add()
        with jax.named_scope("r1"):
            two.make()
        with jax.named_scope("w2"):
            three.make_y()
        with jax.named_scope("add1"):
            two.add()
        with jax.named_scope("r2"):
            three.make()
        with jax.named_scope("pass0"):
            one.pass_on()
        with jax.named_scope("add2"):
            three.add()
        with jax.named_scope("pass1"):
            two.pass_on()
            three.pass_on()
        with jax.named_scope("xfin"):
            v_cur = vt[cur]
            n_loc = total(v_cur * v_cur)
            c_loc = total(v_cur * vt[prev])
            one.finish()
            two.finish()
            three.finish()
        with jax.named_scope("turn"):
            for b in range(5):
                rows = pl.ds(LANES * b, LANES)
                sig[rows, :] = jnp.where(row_lane < COLS, fin[:, rows].T, 0.0)

        with jax.named_scope("vec1"):
            t_val = sig[...] - beta * vt[prev]
            s_loc = total(t_val * vt[cur])
            sig[...] = t_val
            w_val = t_val - ratio(s_loc, n_loc) * vt[cur]
            e_loc = total(w_val * w_val)
        with jax.named_scope("allred"):
            def last_start():
                pl.when(step == NUM_STEPS - 1)(out_start)

            n, s, e, c = all_reduce([n_loc, s_loc, e_loc, c_loc], last_start)
            pl.when(step < NUM_STEPS - 1)(out_start)
        with jax.named_scope("vec2"):
            alpha = (s + beta * c) / VEC
            diff = alpha - ratio(s, n)
            beta_new = jnp.sqrt((e + diff * n * diff) / VEC)
            inv = 1.0 / beta_new
            vt[nxt] = (sig[...] - alpha * vt[cur]) * inv
            fin[pl.ds(COLS, 1), :] = jnp.broadcast_to(alpha, (1, BOND))
            fin[pl.ds(COLS + 8, 1), :] = jnp.broadcast_to(inv, (1, BOND))
            alphas[step] = alpha[0, 0]
            betas[step] = beta_new[0, 0]
        return beta_new

    lax.fori_loop(0, NUM_STEPS, step_body, jnp.zeros((1, 1), F32))
    out_finish(NUM_STEPS)
    cp_v.wait()


def run_kernel(psi, left, pair, right):
    vmem, anys, smem = (pl.BlockSpec(memory_space=space) for space in (pltpu.VMEM, pl.ANY, pltpu.SMEM))
    dma = pltpu.SemaphoreType.DMA
    vm = pltpu.VMEM
    block = (COLS, BOND)
    scratch = [
        vm((4, 2, 160, BOND), BF16), vm((2, 1280, 768), BF16), vm((2, 256, 256), BF16), vm((TERMS, LANES, BOND), BF16), vm((BOND, 4096), BF16),
        vm((4, 4, 25, PAIR, LANES), BF16), vm((PAIR, 1280, LANES), BF16), vm((BOND, 4096), BF16), vm((4, 2) + block, F32),
        vm((4,) + block, F32), vm((4,) + block, F32), vm((ROWS, BOND), F32), vm((ROWS, BOND), F32), vm(block, F32), vm(block, F32),
        vm((LANES, BOND), F32), vm((BOND, LANES), F32), vm((3, BOND, LANES), F32), vm((8, COLS, LANES), F32), vm((8, COLS, LANES), F32), vm(block, F32),
        vm((LANES, 2, LANES), F32),
    ] + [dma((num,)) for num in (8, 8, 8, 8, 8, 8, 60, 60, 3, 3, 18, 18)] + [dma, dma, dma((3,))]
    scal = jax.ShapeDtypeStruct((NUM_STEPS,), F32)
    return pl.pallas_call(
        kernel,
        out_shape=(jax.ShapeDtypeStruct((NUM_STEPS + 1,) + block, F32), scal, scal),
        in_specs=[vmem, anys, vmem, anys],
        out_specs=(anys, smem, smem),
        scratch_shapes=scratch,
        compiler_params=pltpu.CompilerParams(collective_id=0, has_side_effects=True, vmem_limit_bytes=67043328),
        name="lanczos",
    )(psi, left, pair, right)


def solution(mesh):
    def local_run(wave_rows, left_rows, op_pair, right_env):
        psi = wave_rows.reshape(COLS, BOND)
        left = jnp.transpose(left_rows, (1, 0, 2)).reshape(160, BOND)
        vecs, alphas, betas = run_kernel(psi, left, op_pair.reshape(512, PAIR), right_env)
        return vecs.reshape(7, 5, 4, 4, BOND), alphas, betas

    rows = "rows"
    return jax.shard_map(local_run, mesh=mesh, in_specs=(P(rows), P(None, rows), P(), P()), out_specs=(P(None, rows), P(), P()), check_vma=False)
```

```python
import itertools

import jax
import jax.numpy as jnp
from jax import lax
from jax.experimental import pallas as pl
from jax.experimental.pallas import tpu as pltpu
from jax.sharding import PartitionSpec as P

NUM_STEPS = 6
MESH = pl.DeviceIdType.MESH
F32 = jnp.float32
BF16 = jnp.bfloat16

ROWS, COLS = 40, 80
BOND, PAIR, TERMS = 640, 16, 32
LANES = 128
VEC = BOND * BOND * PAIR
PARTS = ((((0, 2), (2, 5)), ((7, 2), (9, 6))), (((15, 1), (16, 4)), ((20, 1), (21, 4))))
ORDER = "001000P1001010101Q10L1L1L1L1LLLL01"
GSEM = 30
FARTHEST = sorted(itertools.product(range(4), range(4), range(4), range(2)), key=lambda off: -sum(min(d, 4 - d) for d in off))[:-1]


def remote(src, dst, send, recv, dev):
    return pltpu.make_async_remote_copy(src_ref=src, dst_ref=dst, send_sem=send, recv_sem=recv, device_id=(dev,), device_id_type=MESH)


def tile_of(lane_tile, row_tile):
    return 15 + 2 * lane_tile + row_tile - 2 if row_tile in (2, 3) else 3 * lane_tile + min(row_tile, 2)


def lane_roll(val, shift):
    shift = shift % LANES
    return val if shift == 0 else pltpu.roll(val, shift, axis=val.ndim - 1)


def lane_iota(val):
    return lax.broadcasted_iota(jnp.int32, val.shape, val.ndim - 1)


def take_piece(tiles, idx):
    tile, off = divmod(COLS * idx, LANES)
    out = lane_roll(tiles(tile), -off)
    lane = lane_iota(out)
    if off + COLS > LANES:
        out = jnp.where(lane < LANES - off, out, lane_roll(tiles(tile + 1), -off))
    return jnp.where(lane < COLS, out, jnp.zeros_like(out))


def dense_tile(pieces, tile):
    out = None
    for idx in range(8):
        shift = COLS * idx - LANES * tile
        if shift <= -COLS or shift >= LANES:
            continue
        moved = lane_roll(pieces(idx), shift)
        out = moved if out is None else jnp.where(lane_iota(moved) >= shift, moved, out)
    return out


def kernel(psi, left, pair, right, vecs, alphas, betas, lall, lh, wbig, rtmp, rt, ug, xs, ys, part, rd, ssum, ra, rb, fl, fr, fin,
           sig, vt, piece_buf, out_recv, outv, stat, psi_s, psi_r, l_s, l_r, out_s, out_r, g_s, g_r, d_s, d_r,
           ring_s, ring_r, a_s, a_r, loc):
    me = lax.axis_index("rows")
    core = lax.rem(me, 2)
    x = lax.rem(me // 2, 4)
    y = lax.rem(me // 8, 4)
    z = me // 32
    i = me // 8
    j = lax.rem(me, 8)
    lo, hi = pl.ds(0, ROWS), pl.ds(ROWS, ROWS)

    def wrap4(val):
        return lax.rem(val + 4, 4)

    def in_row(dj):
        jj = lax.rem(j + dj, 8)
        return jj, i * 8 + jj

    def rows_of(jj):
        return pl.ds(pl.multiple_of(jj * COLS, COLS), COLS)

    barrier = pltpu.get_barrier_semaphore()

    def greet(d, carry):
        pl.semaphore_signal(barrier, inc=1, device_id=(lax.rem(me + d, LANES),), device_id_type=MESH)
        return carry

    lax.fori_loop(1, LANES, greet, 0)
    pl.semaphore_wait(barrier, LANES - 1)

    partner = me + 1 - 2 * core
    places = ([wrap4(z + d) * 32 for d in range(4)], [wrap4(y + d) * 8 for d in range(4)], [wrap4(x + d) * 2 for d in range(4)], (core, 1 - core))
    x_far = i * 8 + wrap4(x + 2) * 2 + core
    x_up, x_dn = i * 8 + wrap4(x + 1) * 2 + core, i * 8 + wrap4(x - 1) * 2 + core
    my_rows = rows_of(j)

    cp_r = pltpu.make_async_copy(right.at[:, my_rows, :], rtmp.at[:, pl.ds(0, COLS), :], loc.at[0])
    cp_r.start()
    cp_l = pltpu.make_async_copy(left, lall.at[x, core], loc.at[1])
    cp_l.start()

    row_lane = lax.broadcasted_iota(jnp.int32, (1, LANES), 1)

    def total(val):
        return jnp.sum(jnp.sum(val, axis=0, keepdims=True), axis=1, keepdims=True)

    def ratio(num, den):
        good = den > 0
        return jnp.where(good, num / jnp.where(good, den, 1.0), 0.0)

    def all_reduce(stats, hook):
        row = jnp.zeros((1, LANES), F32)
        for idx, val in enumerate(stats):
            row = jnp.where(row_lane == idx, val, row)
        stat[me, pl.ds(0, 1), :] = row
        stat[me, pl.ds(1, 1), :] = jnp.broadcast_to(ratio(stats[1], stats[0]), (1, LANES))

        for off in FARTHEST:
            dev = sum(spot[step] for spot, step in zip(places, off))
            remote(stat.at[me], stat.at[me], a_s, a_r, dev).start()
        hook()
        most = stat.at[pl.ds(0, LANES - 1)]
        remote(most, most, a_s, a_r, partner).wait()
        rows = stat[:, pl.ds(0, 1), :]
        sums = jnp.sum(rows, axis=0)
        n, s, e, c = (jnp.sum(jnp.where(row_lane == idx, sums, 0.0), axis=1, keepdims=True) for idx in range(4))
        diff = stat[:, pl.ds(1, 1), :] - ratio(s, n)[None]
        moved = jnp.sum(diff * rows * diff, axis=0)
        return n, s, e + jnp.sum(jnp.where(row_lane == 0, moved, 0.0), axis=1, keepdims=True), c

    def l_copy(src, rows, idx, dev):
        ref = lall.at[src[0], src[1], rows]
        return remote(ref, ref, l_s.at[idx], l_r.at[idx], dev)

    every = pl.ds(0, 160)

    def psi_sends():
        for jj in range(8):
            piece_buf[jj] = take_piece(lambda t: psi[:, LANES * t:LANES * t + LANES], jj)
        vt[0, my_rows, :] = piece_buf[j]
        for dj in range(1, 8):
            jj, dev = in_row(dj)
            remote(piece_buf.at[jj], vt.at[0, my_rows], psi_s.at[jj], psi_r.at[j], dev).start()
        cp_l.wait()
        l_copy((x, core), every, 0, x_up).start()
        l_copy((x, core), every, 1, x_dn).start()
        l_copy((x, core), every, 2, x_far).start()
        l_copy((x, core), every, 4, partner).start()
        spread = jnp.where(lax.broadcasted_iota(jnp.int32, (PAIR, 256), 1) // PAIR == lax.broadcasted_iota(jnp.int32, (PAIR, 256), 0), 1.0, 0.0).astype(BF16)
        same = lax.broadcasted_iota(jnp.int32, (256, 256), 1) % PAIR == lax.broadcasted_iota(jnp.int32, (256, 256), 0) // PAIR
        for h in range(2):
            wide = jnp.dot(pair[pl.ds(256 * h, 256), :], spread, preferred_element_type=F32)
            wbig[h] = jnp.where(same, wide, 0.0).astype(BF16)
        vt[2] = jnp.zeros((BOND, LANES), F32)
        fin[...] = jnp.zeros((LANES, BOND), F32)

    def turn_right():
        cp_r.wait()

        def body(k, carry):
            rtmp[k, pl.ds(COLS, 48), :] = jnp.zeros((48, BOND), BF16)
            for b in range(5):
                rt[pl.ds(LANES * b, LANES), pl.ds(pl.multiple_of(k * LANES, LANES), LANES)] = rtmp[k, :, pl.ds(LANES * b, LANES)].T
            return carry

        lax.fori_loop(0, TERMS, body, 0)

    lower, upper, far = (wrap4(x - 1), core), (wrap4(x + 1), core), (wrap4(x + 2), core)

    def left_forward():
        for idx, (block, way) in enumerate(((lower, x_up), (upper, x_dn), (far, x_far))):
            l_copy(block, every, idx, way).wait_recv()
            l_copy(block, every, 5 + idx, partner).start()

    def start_up():
        psi_sends()
        turn_right()

    psi_val = psi[...]
    zero = jnp.zeros((1, 1), F32)
    n_psi = all_reduce([total(psi_val * psi_val), zero], start_up)[0]
    inv_norm = 1.0 / jnp.sqrt(n_psi / VEC)

    for dj in range(1, 8):
        jj, dev = in_row(dj)
        cp = remote(piece_buf.at[jj], vt.at[0, rows_of(jj)], psi_s.at[jj], psi_r.at[jj], dev)
        cp.wait_recv()
        cp.wait_send()
    vt[0] = vt[0] * inv_norm
    outv[...] = psi_val * inv_norm
    cp_v = pltpu.make_async_copy(outv, vecs.at[0], loc.at[2])
    cp_v.start()

    def left_finish():
        for idx, dx in ((4, 0), (5, 3), (6, 1), (7, 2)):
            l_copy((wrap4(x + dx), 1 - core), every, idx, partner).wait_recv()
        for idx in (0, 1, 2, 4, 5, 6, 7):
            l_copy((x, core), every, idx, partner).wait_send()
        for h in range(2):
            src = lax.broadcasted_iota(jnp.int32, (BOND, 768), 0)
            col = lax.broadcasted_iota(jnp.int32, (BOND, 768), 1)
            group = (col % 256) // PAIR
            main = ROWS * group + PAIR * (col // 256) + col % PAIR
            tail = jnp.where((col // 8) % 2 == h, ROWS * group + 32 + col % 8, -1)
            order = jnp.where(src == jnp.where(col < 512, main, tail), 1.0, 0.0).astype(BF16)

            def body(t, carry):
                rows = pl.ds(pl.multiple_of(t * 160, 160), 160)
                lh[h, rows, :] = jnp.dot(lall[t // 2, t % 2], order, preferred_element_type=F32).astype(BF16)
                return carry

            lax.fori_loop(0, 8, body, 0)

    def flow(base, firsts, seconds, ref, parts):
        done = []
        offs = (0, -1, 1, 2)

        def send(blk, prt, idx, dev):
            here = ref(blk, parts[prt])
            cp = remote(here, here, g_s.at[base + idx], g_r.at[base + idx], dev)
            cp.start()
            done.append(cp)

        def wait(blk, prt, idx):
            here = ref(blk, parts[prt])
            remote(here, here, g_s.at[base + idx], g_r.at[base + idx], partner).wait_recv()

        def second(b, prt):
            for way in ((0, 1) if prt == 0 else (1, 0)):
                send((offs[b], 0), prt, 6 * b + 6 + 2 * way + prt, seconds[way])

        def second_forward(b):
            wait((offs[b], -1), 0, 6 * b + 6)
            send((offs[b], -1), 0, 6 * b + 10, seconds[0])
            wait((offs[b], 1), 1, 6 * b + 9)
            send((offs[b], 1), 1, 6 * b + 11, seconds[1])

        for prt, way in ((0, 0), (1, 1), (1, 0), (0, 1)):
            send((0, 0), prt, 2 * way + prt, firsts[way])
        for prt in range(2):
            send((0, 0), prt, 4 + prt, firsts[2])
        yield
        second(0, 0)
        second(0, 1)
        yield
        wait((-1, 0), 0, 0)
        second(1, 0)
        yield
        wait((1, 0), 1, 3)
        second(2, 1)
        yield
        wait((-1, 0), 1, 1)
        second(1, 1)
        wait((1, 0), 0, 2)
        second(2, 0)
        yield
        second_forward(0)
        yield
        wait((2, 0), 0, 4)
        second(3, 0)
        wait((2, 0), 1, 5)
        second(3, 1)
        yield
        for b in range(1, 4):
            second_forward(b)
            yield
        for b in range(4):
            for off, prt, idx in ((-1, 1, 7), (1, 0, 8), (2, 0, 10), (2, 1, 11)):
                wait((offs[b], off), prt, 6 * b + idx)
        yield
        for cp in done:
            cp.wait_send()
        yield

    def device(zz, yy):
        return (wrap4(zz) * 4 + wrap4(yy)) * 8 + j

    y_ways, z_ways = (device(z, y + 1), device(z, y - 1), device(z, y + 2)), (device(z + 1, y), device(z - 1, y), device(z + 2, y))

    def y_first(blk, prt):
        return ug.at[wrap4(z + blk[1]), wrap4(y + blk[0]), pl.ds(*prt)]

    def z_first(blk, prt):
        return ug.at[wrap4(z + blk[0]), wrap4(y + blk[1]), pl.ds(*prt)]

    def gather(hooks):
        flows = [[flow(GSEM * (2 * h + idx), *ways, ref, PARTS[h][idx]) for idx, (ways, ref) in enumerate((((y_ways, z_ways), y_first), ((z_ways, y_ways), z_first)))]
                 for h in range(2)]
        for mark in ORDER:
            if mark in hooks:
                hooks[mark]()
            else:
                for one in flows[int(mark)]:
                    next(one)

    def out_copy(slot, jj, dev):
        return remote(sig.at[rows_of(jj)], out_recv.at[slot], out_s.at[jj], out_r.at[slot], dev)

    def out_start():
        for dj in range(1, 8):
            jj, dev = in_row(dj)
            out_copy(j, jj, dev).start()
        out_recv[j] = sig[my_rows, :]

    def out_finish(step):
        for dj in range(1, 8):
            jj, dev = in_row(dj)
            out_copy(jj, jj, dev).wait_recv()
            out_copy(j, jj, dev).wait_send()
        cp_v.wait()
        alpha, inv = fin[pl.ds(COLS, 1), pl.ds(0, 1)], fin[pl.ds(COLS + 8, 1), pl.ds(0, 1)]
        for tile in range(5):
            lanes = pl.ds(LANES * tile, LANES)
            outv[:, lanes] = (dense_tile(lambda idx: out_recv[idx], tile) - alpha * outv[:, lanes]) * inv
        pltpu.make_async_copy(outv, vecs.at[step], loc.at[2]).start()

    def step_body(step, beta):
        cur = lax.rem(step, 3)
        prev = lax.rem(step + 2, 3)
        nxt = lax.rem(step + 1, 3)

        with jax.named_scope("pack"):
            strided = [vt[cur, pl.ds(r, ROWS, stride=PAIR), :] for r in range(PAIR)]
            for lt in range(5):
                half = [dense_tile(lambda idx, h=h: strided[8 * h + idx], lt) for h in range(2)]
                for h in range(2):
                    for tt in range(2):
                        ug[z, y, tile_of(lt, 2 * h + tt)] = half[h][PAIR * tt:PAIR * tt + PAIR].astype(BF16)
                ug[z, y, tile_of(lt, 4)] = jnp.concatenate([half[0][32:ROWS], half[1][32:ROWS]], axis=0).astype(BF16)

        def early():
            pl.when(step == 0)(left_forward)

        def late():
            pl.when(step == 0)(left_finish)

            @pl.when(step > 0)
            def _():
                out_finish(step)

        pieces = iter(range(8))

        def left_piece():
            pos = next(pieces)
            h = pos // 4
            cols = []
            for r in (2 * pos, 2 * pos + 1):
                rows = [take_piece(lambda t, tr=tr: ug[:, :, tile_of(t, tr)].reshape(256, LANES), r % 8) for tr in (2 * h, 2 * h + 1, 4)]
                cols.append(jnp.concatenate(rows, axis=0))
            rhs = jnp.concatenate(cols, axis=1)
            for mc in range(2):
                rows = pl.ds(BOND * mc, BOND)
                res = jnp.dot(lh[h, rows, :], rhs, preferred_element_type=F32).astype(BF16)
                for rr in range(2):
                    xs[2 * pos + rr, rows, :] = res[:, LANES * rr:LANES * rr + LANES]

        def named(name, call):
            def run():
                with jax.named_scope(name):
                    call()
            return run

        with jax.named_scope("gather"):
            gather({"P": early, "Q": named("late", late), "L": named("left", left_piece)})

        def some_rows(ap, carry):
            for pr in range(4):
                for h in range(2):
                    starts = [pl.multiple_of((ap * 8 + 2 * pr + aa) * 32 + PAIR * h, PAIR) for aa in range(2)]
                    rhs = jnp.concatenate([xs[:, pl.ds(start, PAIR), :].reshape(256, LANES) for start in starts], axis=1)
                    res = jnp.dot(wbig[h], rhs, preferred_element_type=F32).astype(BF16)
                    for aa in range(2):
                        rows = pl.ds(pl.multiple_of((ap * 8 + 2 * pr + aa) * PAIR, PAIR), PAIR)
                        for k in range(PAIR):
                            ys[rows, pl.ds((PAIR * h + k) * LANES, LANES)] = res[PAIR * k:PAIR * k + PAIR, LANES * aa:LANES * aa + LANES]
            return carry

        xo, xu, xd = wrap4(x + 2), wrap4(x + 1), wrap4(x - 1)

        def sigma(cols):
            for half in range(2):
                res = lax.dot_general(rt[pl.ds(320 * half, 320), :], ys[cols, :], (((1,), (1,)), ((), ())), preferred_element_type=F32)
                for idx in range(4):
                    part[2 * half + idx // 2, idx % 2, :, cols] = res[idx * COLS:idx * COLS + COLS]

        class Chunk:
            def __init__(self, num, start, width):
                cols = self.cols = pl.ds(start, width)
                self.rows = start // LANES, (start + width) // LANES
                self.swap = remote(part.at[:, 1 - core, :, cols], rd.at[:, :, cols], d_s.at[num], d_r.at[num], partner)
                plan = ((xo, lo, ra, lo, x_up), (xo, hi, rb, lo, x_dn), (xu, hi, fl, hi, x_up), (xd, lo, fr, lo, x_dn), (xu, lo, fl, lo, x_up), (xd, hi, fr, hi, x_dn))
                self.copies = [remote(ssum.at[chip, rows, cols], dst.at[to, cols], ring_s.at[6 * num + idx], ring_r.at[6 * num + idx], dev)
                               for idx, (chip, rows, dst, to, dev) in enumerate(plan)]

            def make_y(self):
                lax.fori_loop(*self.rows, some_rows, 0)

            def make(self):
                sigma(self.cols)
                self.swap.start()

            def add(self):
                self.swap.wait()
                for chip in range(4):
                    ssum[chip, :, self.cols] = part[chip, core, :, self.cols] + rd[chip, :, self.cols]
                for cp in self.copies[:4]:
                    cp.start()

            def pass_on(self):
                self.copies[0].wait_recv()
                ssum[xu, lo, self.cols] = ssum[xu, lo, self.cols] + ra[:, self.cols]
                self.copies[4].start()
                self.copies[1].wait_recv()
                ssum[xd, hi, self.cols] = ssum[xd, hi, self.cols] + rb[:, self.cols]
                self.copies[5].start()

            def finish(self):
                for cp in self.copies[2:]:
                    cp.wait_recv()
                fin[pl.ds(0, COLS), self.cols] = ssum[x, :, self.cols] + fl[:, self.cols] + fr[:, self.cols]
                for cp in self.copies:
                    cp.wait_send()

        one, two, three = (Chunk(*spec) for spec in ((0, 0, 256), (1, 256, 256), (2, 512, LANES)))
        with jax.named_scope("w0"):
            one.make_y()
        with jax.named_scope("r0"):
            one.make()
        with jax.named_scope("w1"):
            two.make_y()
        with jax.named_scope("add0"):
            one.add()
        with jax.named_scope("r1"):
            two.make()
        with jax.named_scope("w2"):
            three.make_y()
        with jax.named_scope("add1"):
            two.add()
        with jax.named_scope("r2"):
            three.make()
        with jax.named_scope("pass0"):
            one.pass_on()
        with jax.named_scope("add2"):
            three.add()
        with jax.named_scope("pass1"):
            two.pass_on()
            three.pass_on()
        with jax.named_scope("xfin"):
            v_cur = vt[cur]
            n_loc = total(v_cur * v_cur)
            c_loc = total(v_cur * vt[prev])
            one.finish()
            two.finish()
            three.finish()
        with jax.named_scope("turn"):
            for b in range(5):
                rows = pl.ds(LANES * b, LANES)
                sig[rows, :] = jnp.where(row_lane < COLS, fin[:, rows].T, 0.0)

        with jax.named_scope("vec1"):
            t_val = sig[...] - beta * vt[prev]
            s_loc = total(t_val * vt[cur])
            sig[...] = t_val
            w_val = t_val - ratio(s_loc, n_loc) * vt[cur]
            e_loc = total(w_val * w_val)
        with jax.named_scope("allred"):
            def last_start():
                pl.when(step == NUM_STEPS - 1)(out_start)

            n, s, e, c = all_reduce([n_loc, s_loc, e_loc, c_loc], last_start)
            pl.when(step < NUM_STEPS - 1)(out_start)
        with jax.named_scope("vec2"):
            alpha = (s + beta * c) / VEC
            diff = alpha - ratio(s, n)
            beta_new = jnp.sqrt((e + diff * n * diff) / VEC)
            inv = 1.0 / beta_new
            vt[nxt] = (sig[...] - alpha * vt[cur]) * inv
            fin[pl.ds(COLS, 1), :] = jnp.broadcast_to(alpha, (1, BOND))
            fin[pl.ds(COLS + 8, 1), :] = jnp.broadcast_to(inv, (1, BOND))
            alphas[step] = alpha[0, 0]
            betas[step] = beta_new[0, 0]
        return beta_new

    lax.fori_loop(0, NUM_STEPS, step_body, jnp.zeros((1, 1), F32))
    out_finish(NUM_STEPS)
    cp_v.wait()


def run_kernel(psi, left, pair, right):
    vmem, anys, smem = (pl.BlockSpec(memory_space=space) for space in (pltpu.VMEM, pl.ANY, pltpu.SMEM))
    dma = pltpu.SemaphoreType.DMA
    vm = pltpu.VMEM
    block = (COLS, BOND)
    scratch = [
        vm((4, 2, 160, BOND), BF16), vm((2, 1280, 768), BF16), vm((2, 256, 256), BF16), vm((TERMS, LANES, BOND), BF16), vm((BOND, 4096), BF16),
        vm((4, 4, 25, PAIR, LANES), BF16), vm((PAIR, 1280, LANES), BF16), vm((BOND, 4096), BF16), vm((4, 2) + block, F32),
        vm((4,) + block, F32), vm((4,) + block, F32), vm((ROWS, BOND), F32), vm((ROWS, BOND), F32), vm(block, F32), vm(block, F32),
        vm((LANES, BOND), F32), vm((BOND, LANES), F32), vm((3, BOND, LANES), F32), vm((8, COLS, LANES), F32), vm((8, COLS, LANES), F32), vm(block, F32),
        vm((LANES, 2, LANES), F32),
    ] + [dma((num,)) for num in (8, 8, 8, 8, 8, 8, 4 * GSEM, 4 * GSEM, 3, 3, 18, 18)] + [dma, dma, dma((3,))]
    scal = jax.ShapeDtypeStruct((NUM_STEPS,), F32)
    return pl.pallas_call(
        kernel,
        out_shape=(jax.ShapeDtypeStruct((NUM_STEPS + 1,) + block, F32), scal, scal),
        in_specs=[vmem, anys, vmem, anys],
        out_specs=(anys, smem, smem),
        scratch_shapes=scratch,
        compiler_params=pltpu.CompilerParams(collective_id=0, has_side_effects=True, vmem_limit_bytes=67043328),
        name="lanczos",
    )(psi, left, pair, right)


def solution(mesh):
    def local_run(wave_rows, left_rows, op_pair, right_env):
        psi = wave_rows.reshape(COLS, BOND)
        left = jnp.transpose(left_rows, (1, 0, 2)).reshape(160, BOND)
        vecs, alphas, betas = run_kernel(psi, left, op_pair.reshape(512, PAIR), right_env)
        return vecs.reshape(7, 5, 4, 4, BOND), alphas, betas

    rows = "rows"
    return jax.shard_map(local_run, mesh=mesh, in_specs=(P(rows), P(None, rows), P(), P()), out_specs=(P(None, rows), P(), P()), check_vma=False)
```

```python
import itertools

import jax
import jax.numpy as jnp
import numpy as np
from jax import lax
from jax.experimental import pallas as pl
from jax.experimental.pallas import tpu as pltpu
from jax.sharding import PartitionSpec as P

NUM_STEPS = 6
MESH = pl.DeviceIdType.MESH
F32 = jnp.float32
BF16 = jnp.bfloat16

ROWS, COLS = 40, 80
BOND, PAIR, TERMS = 640, 16, 32
LANES = 128
VEC = BOND * BOND * PAIR
PARTS = ((((0, 4), (4, 3)), ((7, 4), (11, 4))), (((15, 2), (17, 3)), ((20, 3), (23, 2))))
ORDER = "001000P1111001Q10011010L1L01"
GSEM = 30
FARTHEST = sorted(itertools.product(range(4), range(4), range(4), range(2)), key=lambda off: -sum(min(d, 4 - d) for d in off))[:-1]


def left_order():
    col = np.arange(1024)
    group, tail = (col % 256) // PAIR, col >= 512
    src = np.where(tail, ROWS * group + 32 + col % 8, ROWS * group + PAIR * (col // 256) + col % PAIR)
    used = ~tail | ((col // 8) % 2 == (col >= 768))
    return jnp.asarray((np.arange(BOND)[:, None] == src) & used, BF16)


def remote(src, dst, send, recv, dev):
    return pltpu.make_async_remote_copy(src_ref=src, dst_ref=dst, send_sem=send, recv_sem=recv, device_id=(dev,), device_id_type=MESH)


def tile_of(lane_tile, row_tile):
    return 15 + 2 * lane_tile + row_tile - 2 if row_tile in (2, 3) else 3 * lane_tile + min(row_tile, 2)


def lane_roll(val, shift):
    shift = shift % LANES
    return val if shift == 0 else pltpu.roll(val, shift, axis=val.ndim - 1)


def lane_iota(val):
    return lax.broadcasted_iota(jnp.int32, val.shape, val.ndim - 1)


def take_piece(tiles, idx):
    tile, off = divmod(COLS * idx, LANES)
    out = lane_roll(tiles(tile), -off)
    lane = lane_iota(out)
    if off + COLS > LANES:
        out = jnp.where(lane < LANES - off, out, lane_roll(tiles(tile + 1), -off))
    return jnp.where(lane < COLS, out, jnp.zeros_like(out))


def dense_tile(pieces, tile):
    out = None
    for idx in range(8):
        shift = COLS * idx - LANES * tile
        if shift <= -COLS or shift >= LANES:
            continue
        moved = lane_roll(pieces(idx), shift)
        out = moved if out is None else jnp.where(lane_iota(moved) >= shift, moved, out)
    return out


def kernel(psi, left, pair, order, right, vecs, alphas, betas, lall, lh, wbig, rtmp, rt, ug, xs, ys, part, rd, ssum, ra, rb, fl, fr, fin,
           sig, vt, piece_buf, out_recv, outv, stat, psi_s, psi_r, l_s, l_r, out_s, out_r, g_s, g_r, d_s, d_r,
           ring_s, ring_r, a_s, a_r, loc):
    me = lax.axis_index("rows")
    core = lax.rem(me, 2)
    x = lax.rem(me // 2, 4)
    y = lax.rem(me // 8, 4)
    z = me // 32
    i = me // 8
    j = lax.rem(me, 8)
    lo, hi = pl.ds(0, ROWS), pl.ds(ROWS, ROWS)

    def wrap4(val):
        return lax.rem(val + 4, 4)

    def in_row(dj):
        jj = lax.rem(j + dj, 8)
        return jj, i * 8 + jj

    def rows_of(jj):
        return pl.ds(pl.multiple_of(jj * COLS, COLS), COLS)

    barrier = pltpu.get_barrier_semaphore()

    def greet(d, carry):
        pl.semaphore_signal(barrier, inc=1, device_id=(lax.rem(me + d, LANES),), device_id_type=MESH)
        return carry

    lax.fori_loop(1, LANES, greet, 0)
    pl.semaphore_wait(barrier, LANES - 1)

    partner = me + 1 - 2 * core
    places = ([wrap4(z + d) * 32 for d in range(4)], [wrap4(y + d) * 8 for d in range(4)], [wrap4(x + d) * 2 for d in range(4)], (core, 1 - core))
    x_far = i * 8 + wrap4(x + 2) * 2 + core
    x_up, x_dn = i * 8 + wrap4(x + 1) * 2 + core, i * 8 + wrap4(x - 1) * 2 + core
    my_rows = rows_of(j)

    cp_r = pltpu.make_async_copy(right.at[:, my_rows, :], rtmp.at[:, pl.ds(0, COLS), :], loc.at[0])
    cp_r.start()
    cp_l = pltpu.make_async_copy(left, lall.at[x, core], loc.at[1])
    cp_l.start()

    row_lane = lax.broadcasted_iota(jnp.int32, (1, LANES), 1)

    def total(val):
        return jnp.sum(jnp.sum(val, axis=0, keepdims=True), axis=1, keepdims=True)

    def ratio(num, den):
        good = den > 0
        return jnp.where(good, num / jnp.where(good, den, 1.0), 0.0)

    def all_reduce(stats, hook):
        row = jnp.zeros((1, LANES), F32)
        for idx, val in enumerate(stats):
            row = jnp.where(row_lane == idx, val, row)
        stat[me, pl.ds(0, 1), :] = row
        stat[me, pl.ds(1, 1), :] = jnp.broadcast_to(ratio(stats[1], stats[0]), (1, LANES))

        for off in FARTHEST:
            dev = sum(spot[step] for spot, step in zip(places, off))
            remote(stat.at[me], stat.at[me], a_s, a_r, dev).start()
        hook()
        most = stat.at[pl.ds(0, LANES - 1)]
        with jax.named_scope("arwait"):
            remote(most, most, a_s, a_r, partner).wait()
        rows = stat[:, pl.ds(0, 1), :]
        sums = jnp.sum(rows, axis=0)
        n, s, e, c = (jnp.sum(jnp.where(row_lane == idx, sums, 0.0), axis=1, keepdims=True) for idx in range(4))
        diff = stat[:, pl.ds(1, 1), :] - ratio(s, n)[None]
        moved = jnp.sum(diff * rows * diff, axis=0)
        return n, s, e + jnp.sum(jnp.where(row_lane == 0, moved, 0.0), axis=1, keepdims=True), c

    def l_copy(src, rows, idx, dev):
        ref = lall.at[src[0], src[1], rows]
        return remote(ref, ref, l_s.at[idx], l_r.at[idx], dev)

    every = pl.ds(0, 160)

    def psi_sends():
        for jj in range(8):
            piece_buf[jj] = take_piece(lambda t: psi[:, LANES * t:LANES * t + LANES], jj)
        vt[0, my_rows, :] = piece_buf[j]
        for dj in range(1, 8):
            jj, dev = in_row(dj)
            remote(piece_buf.at[jj], vt.at[0, my_rows], psi_s.at[jj], psi_r.at[j], dev).start()
        cp_l.wait()
        l_copy((x, core), every, 0, x_up).start()
        l_copy((x, core), every, 1, x_dn).start()
        l_copy((x, core), every, 2, x_far).start()
        l_copy((x, core), every, 4, partner).start()
        spread = jnp.where(lax.broadcasted_iota(jnp.int32, (PAIR, 256), 1) // PAIR == lax.broadcasted_iota(jnp.int32, (PAIR, 256), 0), 1.0, 0.0).astype(BF16)
        same = lax.broadcasted_iota(jnp.int32, (256, 256), 1) % PAIR == lax.broadcasted_iota(jnp.int32, (256, 256), 0) // PAIR
        for h in range(2):
            wide = jnp.dot(pair[pl.ds(256 * h, 256), :], spread, preferred_element_type=F32)
            wbig[h] = jnp.where(same, wide, 0.0).astype(BF16)
        vt[2] = jnp.zeros((BOND, LANES), F32)
        fin[...] = jnp.zeros((LANES, BOND), F32)

    def turn_right():
        cp_r.wait()

        def body(k, carry):
            rtmp[k, pl.ds(COLS, 48), :] = jnp.zeros((48, BOND), BF16)
            for b in range(5):
                rt[pl.ds(LANES * b, LANES), pl.ds(pl.multiple_of(k * LANES, LANES), LANES)] = rtmp[k, :, pl.ds(LANES * b, LANES)].T
            return carry

        lax.fori_loop(0, TERMS, body, 0)

    lower, upper, far = (wrap4(x - 1), core), (wrap4(x + 1), core), (wrap4(x + 2), core)

    def left_forward():
        for idx, (block, way) in enumerate(((lower, x_up), (upper, x_dn), (far, x_far))):
            l_copy(block, every, idx, way).wait_recv()
            l_copy(block, every, 5 + idx, partner).start()

    def start_up():
        with jax.named_scope("psi"):
            psi_sends()
        with jax.named_scope("turnr"):
            turn_right()

    psi_val = psi[...]
    zero = jnp.zeros((1, 1), F32)
    n_psi = all_reduce([total(psi_val * psi_val), zero], start_up)[0]
    inv_norm = 1.0 / jnp.sqrt(n_psi / VEC)

    for dj in range(1, 8):
        jj, dev = in_row(dj)
        cp = remote(piece_buf.at[jj], vt.at[0, rows_of(jj)], psi_s.at[jj], psi_r.at[jj], dev)
        cp.wait_recv()
        cp.wait_send()
    vt[0] = vt[0] * inv_norm
    outv[...] = psi_val * inv_norm
    cp_v = pltpu.make_async_copy(outv, vecs.at[0], loc.at[2])
    cp_v.start()

    def left_finish():
        for idx, dx in ((4, 0), (5, 3), (6, 1), (7, 2)):
            l_copy((wrap4(x + dx), 1 - core), every, idx, partner).wait_recv()
        for idx in (0, 1, 2, 4, 5, 6, 7):
            l_copy((x, core), every, idx, partner).wait_send()
        def body(t, carry):
            rows = pl.ds(pl.multiple_of(t * 160, 160), 160)
            res = jnp.dot(lall[t // 2, t % 2], order[...], preferred_element_type=F32).astype(BF16)
            for h in range(2):
                lh[h, rows, :] = jnp.concatenate([res[:, :512], res[:, 512 + 256 * h:768 + 256 * h]], axis=1)
            return carry

        lax.fori_loop(0, 8, body, 0)

    def flow(base, firsts, seconds, ref, parts):
        done = []
        offs = (0, -1, 1, 2)

        def send(blk, prt, idx, dev):
            here = ref(blk, parts[prt])
            cp = remote(here, here, g_s.at[base + idx], g_r.at[base + idx], dev)
            cp.start()
            done.append(cp)

        def wait(blk, prt, idx):
            here = ref(blk, parts[prt])
            remote(here, here, g_s.at[base + idx], g_r.at[base + idx], partner).wait_recv()

        def second(b, prt):
            for way in ((0, 1) if prt == 0 else (1, 0)):
                send((offs[b], 0), prt, 6 * b + 6 + 2 * way + prt, seconds[way])

        def second_forward(b):
            wait((offs[b], -1), 0, 6 * b + 6)
            send((offs[b], -1), 0, 6 * b + 10, seconds[0])
            wait((offs[b], 1), 1, 6 * b + 9)
            send((offs[b], 1), 1, 6 * b + 11, seconds[1])

        for prt, way in ((0, 0), (1, 1), (1, 0), (0, 1)):
            send((0, 0), prt, 2 * way + prt, firsts[way])
        for prt in range(2):
            send((0, 0), prt, 4 + prt, firsts[2])
        yield
        second(0, 0)
        second(0, 1)
        yield
        wait((-1, 0), 0, 0)
        second(1, 0)
        yield
        wait((1, 0), 1, 3)
        second(2, 1)
        yield
        wait((-1, 0), 1, 1)
        second(1, 1)
        wait((1, 0), 0, 2)
        second(2, 0)
        yield
        second_forward(0)
        yield
        wait((2, 0), 0, 4)
        second(3, 0)
        wait((2, 0), 1, 5)
        second(3, 1)
        yield
        for b in range(1, 4):
            second_forward(b)
            yield
        for b in range(4):
            for off, prt, idx in ((-1, 1, 7), (1, 0, 8), (2, 0, 10), (2, 1, 11)):
                wait((offs[b], off), prt, 6 * b + idx)
        yield
        for cp in done:
            cp.wait_send()
        yield

    def device(zz, yy):
        return (wrap4(zz) * 4 + wrap4(yy)) * 8 + j

    y_ways, z_ways = (device(z, y + 1), device(z, y - 1), device(z, y + 2)), (device(z + 1, y), device(z - 1, y), device(z + 2, y))

    def y_first(blk, prt):
        return ug.at[wrap4(z + blk[1]), wrap4(y + blk[0]), pl.ds(*prt)]

    def z_first(blk, prt):
        return ug.at[wrap4(z + blk[0]), wrap4(y + blk[1]), pl.ds(*prt)]

    def gather(hooks):
        flows = [[flow(GSEM * (2 * h + idx), *ways, ref, PARTS[h][idx]) for idx, (ways, ref) in enumerate((((y_ways, z_ways), y_first), ((z_ways, y_ways), z_first)))]
                 for h in range(2)]
        for mark in ORDER:
            if mark in hooks:
                hooks[mark]()
            else:
                for one in flows[int(mark)]:
                    next(one)

    def out_copy(slot, jj, dev):
        return remote(sig.at[rows_of(jj)], out_recv.at[slot], out_s.at[jj], out_r.at[slot], dev)

    def out_start():
        for dj in range(1, 8):
            jj, dev = in_row(dj)
            out_copy(j, jj, dev).start()
        out_recv[j] = sig[my_rows, :]

    def out_finish(step):
        for dj in range(1, 8):
            jj, dev = in_row(dj)
            out_copy(jj, jj, dev).wait_recv()
            out_copy(j, jj, dev).wait_send()
        cp_v.wait()
        alpha, inv = fin[pl.ds(COLS, 1), pl.ds(0, 1)], fin[pl.ds(COLS + 8, 1), pl.ds(0, 1)]
        for tile in range(5):
            lanes = pl.ds(LANES * tile, LANES)
            outv[:, lanes] = (dense_tile(lambda idx: out_recv[idx], tile) - alpha * outv[:, lanes]) * inv
        pltpu.make_async_copy(outv, vecs.at[step], loc.at[2]).start()

    def step_body(step, beta):
        cur = lax.rem(step, 3)
        prev = lax.rem(step + 2, 3)
        nxt = lax.rem(step + 1, 3)

        with jax.named_scope("pack"):
            strided = [vt[cur, pl.ds(r, ROWS, stride=PAIR), :] for r in range(PAIR)]
            for lt in range(5):
                half = [dense_tile(lambda idx, h=h: strided[8 * h + idx], lt) for h in range(2)]
                for h in range(2):
                    for tt in range(2):
                        ug[z, y, tile_of(lt, 2 * h + tt)] = half[h][PAIR * tt:PAIR * tt + PAIR].astype(BF16)
                ug[z, y, tile_of(lt, 4)] = jnp.concatenate([half[0][32:ROWS], half[1][32:ROWS]], axis=0).astype(BF16)

        def early():
            pl.when(step == 0)(left_forward)

        def late():
            pl.when(step == 0)(left_finish)

            @pl.when(step > 0)
            def _():
                out_finish(step)

        halves = iter(range(2))

        def left_half():
            h = next(halves)
            for pos in range(4 * h, 4 * h + 4):
                cols = []
                for r in (2 * pos, 2 * pos + 1):
                    rows = [take_piece(lambda t, tr=tr: ug[:, :, tile_of(t, tr)].reshape(256, LANES), r % 8) for tr in (2 * h, 2 * h + 1, 4)]
                    cols.append(jnp.concatenate(rows, axis=0))
                rhs = jnp.concatenate(cols, axis=1)
                for mc in range(2):
                    rows = pl.ds(BOND * mc, BOND)
                    res = jnp.dot(lh[h, rows, :], rhs, preferred_element_type=F32).astype(BF16)
                    for rr in range(2):
                        xs[2 * pos + rr, rows, :] = res[:, LANES * rr:LANES * rr + LANES]

        def named(name, call):
            def run():
                with jax.named_scope(name):
                    call()
            return run

        with jax.named_scope("gather"):
            gather({"P": early, "Q": named("late", late), "L": named("left", left_half)})

        def some_rows(ap, carry):
            for pr in range(4):
                for h in range(2):
                    starts = [pl.multiple_of((ap * 8 + 2 * pr + aa) * 32 + PAIR * h, PAIR) for aa in range(2)]
                    rhs = jnp.concatenate([xs[:, pl.ds(start, PAIR), :].reshape(256, LANES) for start in starts], axis=1)
                    res = jnp.dot(wbig[h], rhs, preferred_element_type=F32).astype(BF16)
                    for aa in range(2):
                        rows = pl.ds(pl.multiple_of((ap * 8 + 2 * pr + aa) * PAIR, PAIR), PAIR)
                        for k in range(PAIR):
                            ys[rows, pl.ds((PAIR * h + k) * LANES, LANES)] = res[PAIR * k:PAIR * k + PAIR, LANES * aa:LANES * aa + LANES]
            return carry

        xo, xu, xd = wrap4(x + 2), wrap4(x + 1), wrap4(x - 1)

        def sigma(cols):
            for half in range(2):
                res = lax.dot_general(rt[pl.ds(320 * half, 320), :], ys[cols, :], (((1,), (1,)), ((), ())), preferred_element_type=F32)
                for idx in range(4):
                    part[2 * half + idx // 2, idx % 2, :, cols] = res[idx * COLS:idx * COLS + COLS]

        class Chunk:
            def __init__(self, num, start, width):
                cols = self.cols = pl.ds(start, width)
                self.rows = start // LANES, (start + width) // LANES
                self.swap = remote(part.at[:, 1 - core, :, cols], rd.at[:, :, cols], d_s.at[num], d_r.at[num], partner)
                plan = ((xo, lo, ra, lo, x_up), (xo, hi, rb, lo, x_dn), (xu, hi, fl, hi, x_up), (xd, lo, fr, lo, x_dn), (xu, lo, fl, lo, x_up), (xd, hi, fr, hi, x_dn))
                self.copies = [remote(ssum.at[chip, rows, cols], dst.at[to, cols], ring_s.at[6 * num + idx], ring_r.at[6 * num + idx], dev)
                               for idx, (chip, rows, dst, to, dev) in enumerate(plan)]

            def make_y(self):
                lax.fori_loop(*self.rows, some_rows, 0)

            def make(self):
                sigma(self.cols)
                self.swap.start()

            def add(self):
                self.swap.wait()
                for chip in range(4):
                    ssum[chip, :, self.cols] = part[chip, core, :, self.cols] + rd[chip, :, self.cols]
                for cp in self.copies[:4]:
                    cp.start()

            def pass_on(self):
                self.copies[0].wait_recv()
                ssum[xu, lo, self.cols] = ssum[xu, lo, self.cols] + ra[:, self.cols]
                self.copies[4].start()
                self.copies[1].wait_recv()
                ssum[xd, hi, self.cols] = ssum[xd, hi, self.cols] + rb[:, self.cols]
                self.copies[5].start()

            def finish(self):
                for cp in self.copies[2:]:
                    cp.wait_recv()
                fin[pl.ds(0, COLS), self.cols] = ssum[x, :, self.cols] + fl[:, self.cols] + fr[:, self.cols]
                for cp in self.copies:
                    cp.wait_send()

        one, two, three = (Chunk(*spec) for spec in ((0, 0, 256), (1, 256, 256), (2, 512, LANES)))
        with jax.named_scope("w0"):
            one.make_y()
        with jax.named_scope("r0"):
            one.make()
        with jax.named_scope("w1"):
            two.make_y()
        with jax.named_scope("add0"):
            one.add()
        with jax.named_scope("r1"):
            two.make()
        with jax.named_scope("w2"):
            three.make_y()
        with jax.named_scope("add1"):
            two.add()
        with jax.named_scope("r2"):
            three.make()
        with jax.named_scope("pass0"):
            one.pass_on()
        with jax.named_scope("add2"):
            three.add()
        with jax.named_scope("pass1"):
            two.pass_on()
            three.pass_on()
        with jax.named_scope("xfin"):
            v_cur = vt[cur]
            n_loc = total(v_cur * v_cur)
            c_loc = total(v_cur * vt[prev])
            one.finish()
            two.finish()
            three.finish()
        with jax.named_scope("turn"):
            for b in range(5):
                rows = pl.ds(LANES * b, LANES)
                sig[rows, :] = jnp.where(row_lane < COLS, fin[:, rows].T, 0.0)

        with jax.named_scope("vec1"):
            t_val = sig[...] - beta * vt[prev]
            s_loc = total(t_val * vt[cur])
            sig[...] = t_val
            w_val = t_val - ratio(s_loc, n_loc) * vt[cur]
            e_loc = total(w_val * w_val)
        with jax.named_scope("allred"):
            def last_start():
                pl.when(step == NUM_STEPS - 1)(out_start)

            n, s, e, c = all_reduce([n_loc, s_loc, e_loc, c_loc], last_start)
            pl.when(step < NUM_STEPS - 1)(out_start)
        with jax.named_scope("vec2"):
            alpha = (s + beta * c) / VEC
            diff = alpha - ratio(s, n)
            beta_new = jnp.sqrt((e + diff * n * diff) / VEC)
            inv = 1.0 / beta_new
            vt[nxt] = (sig[...] - alpha * vt[cur]) * inv
            fin[pl.ds(COLS, 1), :] = jnp.broadcast_to(alpha, (1, BOND))
            fin[pl.ds(COLS + 8, 1), :] = jnp.broadcast_to(inv, (1, BOND))
            alphas[step] = alpha[0, 0]
            betas[step] = beta_new[0, 0]
        return beta_new

    lax.fori_loop(0, NUM_STEPS, step_body, jnp.zeros((1, 1), F32))
    out_finish(NUM_STEPS)
    cp_v.wait()


def run_kernel(psi, left, pair, order, right):
    vmem, anys, smem = (pl.BlockSpec(memory_space=space) for space in (pltpu.VMEM, pl.ANY, pltpu.SMEM))
    dma = pltpu.SemaphoreType.DMA
    vm = pltpu.VMEM
    block = (COLS, BOND)
    scratch = [
        vm((4, 2, 160, BOND), BF16), vm((2, 1280, 768), BF16), vm((2, 256, 256), BF16), vm((TERMS, LANES, BOND), BF16), vm((BOND, 4096), BF16),
        vm((4, 4, 25, PAIR, LANES), BF16), vm((PAIR, 1280, LANES), BF16), vm((BOND, 4096), BF16), vm((4, 2) + block, F32),
        vm((4,) + block, F32), vm((4,) + block, F32), vm((ROWS, BOND), F32), vm((ROWS, BOND), F32), vm(block, F32), vm(block, F32),
        vm((LANES, BOND), F32), vm((BOND, LANES), F32), vm((3, BOND, LANES), F32), vm((8, COLS, LANES), F32), vm((8, COLS, LANES), F32), vm(block, F32),
        vm((LANES, 2, LANES), F32),
    ] + [dma((num,)) for num in (8, 8, 8, 8, 8, 8, 4 * GSEM, 4 * GSEM, 3, 3, 18, 18)] + [dma, dma, dma((3,))]
    scal = jax.ShapeDtypeStruct((NUM_STEPS,), F32)
    return pl.pallas_call(
        kernel,
        out_shape=(jax.ShapeDtypeStruct((NUM_STEPS + 1,) + block, F32), scal, scal),
        in_specs=[vmem, anys, vmem, vmem, anys],
        out_specs=(anys, smem, smem),
        scratch_shapes=scratch,
        compiler_params=pltpu.CompilerParams(collective_id=0, has_side_effects=True, vmem_limit_bytes=67043328),
        name="lanczos",
    )(psi, left, pair, order, right)


def solution(mesh):
    def local_run(wave_rows, left_rows, op_pair, right_env):
        psi = wave_rows.reshape(COLS, BOND)
        left = jnp.transpose(left_rows, (1, 0, 2)).reshape(160, BOND)
        vecs, alphas, betas = run_kernel(psi, left, op_pair.reshape(512, PAIR), left_order(), right_env)
        return vecs.reshape(7, 5, 4, 4, BOND), alphas, betas

    rows = "rows"
    return jax.shard_map(local_run, mesh=mesh, in_specs=(P(rows), P(None, rows), P(), P()), out_specs=(P(None, rows), P(), P()), check_vma=False)
```

```python
import itertools

import jax
import jax.numpy as jnp
import numpy as np
from jax import lax
from jax.experimental import pallas as pl
from jax.experimental.pallas import tpu as pltpu
from jax.sharding import PartitionSpec as P

NUM_STEPS = 6
MESH = pl.DeviceIdType.MESH
F32 = jnp.float32
BF16 = jnp.bfloat16

ROWS, COLS = 40, 80
BOND, PAIR, TERMS = 640, 16, 32
LANES = 128
GC, RING, WIDE = 8, 4, 256
VEC = BOND * BOND * PAIR
PARTS = ((((0, 4), (4, 3)), ((7, 4), (11, 4))), (((15, 2), (17, 3)), ((20, 3), (23, 2))))
ORDER = "001000P1111001Q10011010L1L01"
GSEM = 30
FARTHEST = sorted(itertools.product(range(4), range(4), range(4), range(2)), key=lambda off: -sum(min(d, 4 - d) for d in off))[:-1]


def left_order():
    col = np.arange(1024)
    group, tail = (col % WIDE) // PAIR, col >= 512
    src = np.where(tail, ROWS * group + 32 + col % GC, ROWS * group + PAIR * (col // WIDE) + col % PAIR)
    used = ~tail | ((col // GC) % 2 == (col >= 768))
    return jnp.asarray((np.arange(BOND)[:, None] == src) & used, BF16)


def remote(src, dst, send, recv, dev):
    return pltpu.make_async_remote_copy(src_ref=src, dst_ref=dst, send_sem=send, recv_sem=recv, device_id=(dev,), device_id_type=MESH)


def tile_of(lane_tile, row_tile):
    return 15 + 2 * lane_tile + row_tile - 2 if row_tile in (2, 3) else 3 * lane_tile + min(row_tile, 2)


def lane_roll(val, shift):
    shift = shift % LANES
    return val if shift == 0 else pltpu.roll(val, shift, axis=val.ndim - 1)


def lane_iota(val):
    return lax.broadcasted_iota(jnp.int32, val.shape, val.ndim - 1)


def take_piece(tiles, idx):
    tile, off = divmod(COLS * idx, LANES)
    out = lane_roll(tiles(tile), -off)
    lane = lane_iota(out)
    if off + COLS > LANES:
        out = jnp.where(lane < LANES - off, out, lane_roll(tiles(tile + 1), -off))
    return jnp.where(lane < COLS, out, jnp.zeros_like(out))


def merge_three(one, two, three=None):
    if three is None:
        return one, two
    inner = lane_iota(one) < COLS
    return jnp.where(inner, one, lane_roll(three, COLS)), jnp.where(inner, two, lane_roll(three, COLS - 48))


def split_three(left, right):
    lane, zero = lane_iota(left), jnp.zeros_like(left)
    three = jnp.where(lane < 48, lane_roll(left, -COLS), jnp.where(lane < COLS, lane_roll(right, 48 - COLS), zero))
    return jnp.where(lane < COLS, left, zero), jnp.where(lane < COLS, right, zero), three


def dense_tile(pieces, tile):
    out = None
    for idx in range(GC):
        shift = COLS * idx - LANES * tile
        if shift <= -COLS or shift >= LANES:
            continue
        moved = lane_roll(pieces(idx), shift)
        out = moved if out is None else jnp.where(lane_iota(moved) >= shift, moved, out)
    return out


def kernel(psi, left, pair, order, right, vecs, alphas, betas, lall, lh, wbig, rtmp, rt, ug, xs, ys, part, rd, ssum, ra, rb, fl, fr, fin,
           sig, vt, piece_buf, out_recv, outv, stat, psi_s, psi_r, l_s, l_r, out_s, out_r, g_s, g_r, d_s, d_r,
           ring_s, ring_r, a_s, a_r, loc, ready):
    me = lax.axis_index("rows")
    core = lax.rem(me, 2)
    x = lax.rem(me // 2, RING)
    y = lax.rem(me // GC, RING)
    z = me // 32
    i = me // GC
    t_me = lax.rem(me, GC)
    label = lax.rem(me + x + y + z, 2)
    j = x * 2 + label
    lo, hi = pl.ds(0, ROWS), pl.ds(ROWS, ROWS)

    def wrap4(val):
        return lax.rem(val + RING, RING)

    def in_row(d):
        tt = lax.rem(t_me + d, GC)
        return tt, tt - lax.rem(tt, 2) + lax.rem(tt + tt // 2 + y + z, 2), i * GC + tt

    def rows_of(jj):
        return pl.ds(pl.multiple_of(jj * COLS, COLS), COLS)

    barrier = pltpu.get_barrier_semaphore()

    def col_dev(di):
        ii = lax.rem(i + di, PAIR)
        return ii * GC + x * 2 + lax.rem(label + x + ii + ii // RING, 2)

    for d in range(1, GC):
        pl.semaphore_signal(barrier, inc=1, device_id=(in_row(d)[2],), device_id_type=MESH)
    for di in range(1, PAIR):
        pl.semaphore_signal(barrier, inc=1, device_id=(col_dev(di),), device_id_type=MESH)
    pl.semaphore_wait(barrier, 22)
    for di in range(1, PAIR):
        pl.semaphore_signal(ready, inc=1, device_id=(col_dev(di),), device_id_type=MESH)

    partner = me + 1 - 2 * core
    places = ([wrap4(z + d) * 32 for d in range(RING)], [wrap4(y + d) * GC for d in range(RING)], [wrap4(x + d) * 2 for d in range(RING)], (core, 1 - core))
    x_up, x_dn = i * GC + wrap4(x + 1) * 2 + 1 - core, i * GC + wrap4(x - 1) * 2 + 1 - core
    left_up, left_dn, left_far = (i * GC + wrap4(x + d) * 2 + core for d in (1, -1, 2))
    my_rows = rows_of(t_me)

    def fetch_right(first, last, row, width):
        def body(m, carry):
            src = right.at[3 * m + first, pl.ds(pl.multiple_of(j * COLS + row, PAIR), width), :]
            pltpu.make_async_copy(src, rtmp.at[pl.ds(pl.multiple_of(WIDE * m + last, PAIR), width), :], loc.at[0]).start()
            return carry
        return body

    lax.fori_loop(0, 11, fetch_right(0, 0, 0, COLS), 0)
    lax.fori_loop(0, 11, fetch_right(1, LANES, 0, COLS), 0)
    lax.fori_loop(0, 10, fetch_right(2, COLS, 0, 48), 0)
    lax.fori_loop(0, 10, fetch_right(2, LANES + COLS, 48, 32), 0)
    cp_l = pltpu.make_async_copy(left, lall.at[x, core], loc.at[1])
    cp_l.start()

    row_lane = lax.broadcasted_iota(jnp.int32, (1, LANES), 1)

    def total(val):
        return jnp.sum(jnp.sum(val, axis=0, keepdims=True), axis=1, keepdims=True)

    def ratio(num, den):
        good = den > 0
        return jnp.where(good, num / jnp.where(good, den, 1.0), 0.0)

    def all_reduce(stats, hook):
        row = jnp.zeros((1, LANES), F32)
        for idx, val in enumerate(stats):
            row = jnp.where(row_lane == idx, val, row)
        stat[me, pl.ds(0, 1), :] = row
        stat[me, pl.ds(1, 1), :] = jnp.broadcast_to(ratio(stats[1], stats[0]), (1, LANES))

        for off in FARTHEST:
            dev = sum(spot[step] for spot, step in zip(places, off))
            remote(stat.at[me], stat.at[me], a_s, a_r, dev).start()
        hook()
        most = stat.at[pl.ds(0, LANES - 1)]
        with jax.named_scope("arwait"):
            remote(most, most, a_s, a_r, partner).wait()
        rows = stat[:, pl.ds(0, 1), :]
        sums = jnp.sum(rows, axis=0)
        n, s, e, c = (jnp.sum(jnp.where(row_lane == idx, sums, 0.0), axis=1, keepdims=True) for idx in range(RING))
        diff = stat[:, pl.ds(1, 1), :] - ratio(s, n)[None]
        moved = jnp.sum(diff * rows * diff, axis=0)
        return n, s, e + jnp.sum(jnp.where(row_lane == 0, moved, 0.0), axis=1, keepdims=True), c

    def l_copy(src, rows, idx, dev):
        ref = lall.at[src[0], src[1], rows]
        return remote(ref, ref, l_s.at[idx], l_r.at[idx], dev)

    every = pl.ds(0, 160)

    def psi_pieces():
        for jj in range(GC):
            piece_buf[jj] = take_piece(lambda t: psi[:, LANES * t:LANES * t + LANES], jj)
        vt[0, my_rows, :] = piece_buf[j]
        spread = jnp.where(lax.broadcasted_iota(jnp.int32, (PAIR, WIDE), 1) // PAIR == lax.broadcasted_iota(jnp.int32, (PAIR, WIDE), 0), 1.0, 0.0).astype(BF16)
        same = lax.broadcasted_iota(jnp.int32, (WIDE, WIDE), 1) % PAIR == lax.broadcasted_iota(jnp.int32, (WIDE, WIDE), 0) // PAIR
        for h in range(2):
            wide = jnp.dot(pair[pl.ds(WIDE * h, WIDE), :], spread, preferred_element_type=F32)
            wbig[h] = jnp.where(same, wide, 0.0).astype(BF16)
        vt[2] = jnp.zeros((BOND, LANES), F32)
        fin[...] = jnp.zeros((LANES, BOND), F32)

    def psi_sends():
        for d in range(1, GC):
            tt, jj, dev = in_row(d)
            remote(piece_buf.at[jj], vt.at[0, my_rows], psi_s.at[tt], psi_r.at[t_me], dev).start()
        cp_l.wait()
        l_copy((x, core), every, 0, left_up).start()
        l_copy((x, core), every, 1, left_dn).start()
        l_copy((x, core), every, 2, left_far).start()
        l_copy((x, core), every, RING, partner).start()

    def turn_right():
        some = rtmp.at[pl.ds(0, TERMS * COLS), :]
        pltpu.make_async_copy(some, some, loc.at[0]).wait()
        for m in range(11):
            rtmp[pl.ds(WIDE * m + 240, PAIR), :] = jnp.zeros((PAIR, BOND), BF16)
        for start in (COLS, LANES + COLS):
            rtmp[pl.ds(2560 + start, 48), :] = jnp.zeros((48, BOND), BF16)

        def body(k, carry):
            cols = pl.ds(pl.multiple_of(k * LANES, LANES), LANES)
            for b in range(5):
                rt[pl.ds(LANES * b, LANES), cols] = rtmp[cols, pl.ds(LANES * b, LANES)].T
            return carry

        lax.fori_loop(0, 22, body, 0)

    lower, upper, far = (wrap4(x - 1), core), (wrap4(x + 1), core), (wrap4(x + 2), core)

    def left_forward():
        for idx, (block, way) in enumerate(((lower, left_up), (upper, left_dn), (far, left_far))):
            l_copy(block, every, idx, way).wait_recv()
            l_copy(block, every, 5 + idx, partner).start()

    def start_up():
        with jax.named_scope("psi"):
            psi_sends()
        with jax.named_scope("turnr"):
            turn_right()

    psi_pieces()
    psi_val = psi[...]
    pl.semaphore_wait(ready, PAIR - 1)
    zero = jnp.zeros((1, 1), F32)
    n_psi = all_reduce([total(psi_val * psi_val), zero], start_up)[0]
    inv_norm = 1.0 / jnp.sqrt(n_psi / VEC)

    for d in range(1, GC):
        tt, jj, dev = in_row(d)
        cp = remote(piece_buf.at[jj], vt.at[0, rows_of(tt)], psi_s.at[tt], psi_r.at[tt], dev)
        cp.wait_recv()
        cp.wait_send()
    vt[0] = vt[0] * inv_norm
    outv[...] = psi_val * inv_norm
    cp_v = pltpu.make_async_copy(outv, vecs.at[0], loc.at[2])
    cp_v.start()

    def left_finish():
        for idx, dx in ((RING, 0), (5, 3), (6, 1), (7, 2)):
            l_copy((wrap4(x + dx), 1 - core), every, idx, partner).wait_recv()
        for idx in (0, 1, 2, RING, 5, 6, 7):
            l_copy((x, core), every, idx, partner).wait_send()
        def body(t, carry):
            rows = pl.ds(pl.multiple_of(t * 160, 160), 160)
            res = jnp.dot(lall[t // 2, t % 2], order[...], preferred_element_type=F32).astype(BF16)
            for h in range(2):
                lh[h, rows, :] = jnp.concatenate([res[:, :512], res[:, 512 + WIDE * h:768 + WIDE * h]], axis=1)
            return carry

        lax.fori_loop(0, GC, body, 0)

    def flow(base, firsts, seconds, ref, parts):
        done = []
        offs = (0, -1, 1, 2)

        def send(blk, prt, idx, dev):
            here = ref(blk, parts[prt])
            cp = remote(here, here, g_s.at[base + idx], g_r.at[base + idx], dev)
            cp.start()
            done.append(cp)

        def wait(blk, prt, idx):
            here = ref(blk, parts[prt])
            remote(here, here, g_s.at[base + idx], g_r.at[base + idx], partner).wait_recv()

        def second(b, prt):
            for way in ((0, 1) if prt == 0 else (1, 0)):
                send((offs[b], 0), prt, 6 * b + 6 + 2 * way + prt, seconds[way])

        def second_forward(b):
            wait((offs[b], -1), 0, 6 * b + 6)
            send((offs[b], -1), 0, 6 * b + 10, seconds[0])
            wait((offs[b], 1), 1, 6 * b + 9)
            send((offs[b], 1), 1, 6 * b + 11, seconds[1])

        for prt, way in ((0, 0), (1, 1), (1, 0), (0, 1)):
            send((0, 0), prt, 2 * way + prt, firsts[way])
        for prt in range(2):
            send((0, 0), prt, RING + prt, firsts[2])
        yield
        second(0, 0)
        second(0, 1)
        yield
        wait((-1, 0), 0, 0)
        second(1, 0)
        yield
        wait((1, 0), 1, 3)
        second(2, 1)
        yield
        wait((-1, 0), 1, 1)
        second(1, 1)
        wait((1, 0), 0, 2)
        second(2, 0)
        yield
        second_forward(0)
        yield
        wait((2, 0), 0, RING)
        second(3, 0)
        wait((2, 0), 1, 5)
        second(3, 1)
        yield
        for b in range(1, RING):
            second_forward(b)
            yield
        for b in range(RING):
            for off, prt, idx in ((-1, 1, 7), (1, 0, GC), (2, 0, 10), (2, 1, 11)):
                wait((offs[b], off), prt, 6 * b + idx)
        yield
        for cp in done:
            cp.wait_send()
        yield

    def device(dz, dy):
        return (wrap4(z + dz) * RING + wrap4(y + dy)) * GC + x * 2 + (1 - core if (dz + dy) % 2 else core)

    y_ways, z_ways = [device(0, d) for d in (1, -1, 2)], [device(d, 0) for d in (1, -1, 2)]

    def y_first(blk, prt):
        return ug.at[wrap4(z + blk[1]), wrap4(y + blk[0]), pl.ds(*prt)]

    def z_first(blk, prt):
        return ug.at[wrap4(z + blk[0]), wrap4(y + blk[1]), pl.ds(*prt)]

    def gather(hooks):
        flows = [[flow(GSEM * (2 * h + idx), *ways, ref, PARTS[h][idx]) for idx, (ways, ref) in enumerate((((y_ways, z_ways), y_first), ((z_ways, y_ways), z_first)))]
                 for h in range(2)]
        for mark in ORDER:
            if mark in hooks:
                hooks[mark]()
            else:
                for one in flows[int(mark)]:
                    next(one)

    def out_copy(slot, tt, dev):
        return remote(sig.at[rows_of(tt)], out_recv.at[slot], out_s.at[tt], out_r.at[slot], dev)

    def out_start():
        for d in range(1, GC):
            tt, jj, dev = in_row(d)
            out_copy(j, tt, dev).start()
        out_recv[j] = sig[my_rows, :]

    def out_finish(step):
        for d in range(1, GC):
            tt, jj, dev = in_row(d)
            out_copy(jj, tt, dev).wait_recv()
            out_copy(j, tt, dev).wait_send()
        cp_v.wait()
        alpha, inv = fin[pl.ds(COLS, 1), pl.ds(0, 1)], fin[pl.ds(COLS + GC, 1), pl.ds(0, 1)]
        for tile in range(5):
            lanes = pl.ds(LANES * tile, LANES)
            outv[:, lanes] = (dense_tile(lambda idx: out_recv[idx], tile) - alpha * outv[:, lanes]) * inv
        pltpu.make_async_copy(outv, vecs.at[step], loc.at[2]).start()

    def step_body(step, beta):
        cur = lax.rem(step, 3)
        prev = lax.rem(step + 2, 3)
        nxt = lax.rem(step + 1, 3)

        with jax.named_scope("pack"):
            strided = [vt[cur, pl.ds(r, ROWS, stride=PAIR), :] for r in range(PAIR)]
            for lt in range(5):
                half = [dense_tile(lambda idx, h=h: strided[GC * h + idx], lt) for h in range(2)]
                for h in range(2):
                    for tt in range(2):
                        ug[z, y, tile_of(lt, 2 * h + tt)] = half[h][PAIR * tt:PAIR * tt + PAIR].astype(BF16)
                ug[z, y, tile_of(lt, RING)] = jnp.concatenate([half[0][32:ROWS], half[1][32:ROWS]], axis=0).astype(BF16)

        def early():
            pl.when(step == 0)(left_forward)

        def late():
            pl.when(step == 0)(left_finish)

            @pl.when(step > 0)
            def _():
                out_finish(step)

        halves = iter(range(2))

        def left_half():
            h = next(halves)
            for group in range(3):
                first = 3 * group
                got = []
                for r in range(first, min(first + 3, GC)):
                    rows = [take_piece(lambda t, tr=tr: ug[:, :, tile_of(t, tr)].reshape(WIDE, LANES), r) for tr in (2 * h, 2 * h + 1, RING)]
                    got.append(jnp.concatenate(rows, axis=0))
                rhs = jnp.concatenate(merge_three(*got), axis=1)
                for mc in range(2):
                    rows = pl.ds(BOND * mc, BOND)
                    res = jnp.dot(lh[h, rows, :], rhs, preferred_element_type=F32).astype(BF16)
                    for rr, val in enumerate(split_three(res[:, :LANES], res[:, LANES:])[:len(got)]):
                        xs[h * GC + first + rr, rows, :] = val

        def named(name, call):
            def run():
                with jax.named_scope(name):
                    call()
            return run

        with jax.named_scope("gather"):
            gather({"P": early, "Q": named("late", late), "L": named("left", left_half)})

        def some_rows(ap, carry):
            for pr in range(RING):
                spots = [ap * GC + 2 * pr + aa for aa in range(2)]
                both = []
                for h in range(2):
                    rhs = jnp.concatenate([xs[:, pl.ds(pl.multiple_of(spot * 32 + PAIR * h, PAIR), PAIR), :].reshape(WIDE, LANES) for spot in spots], axis=1)
                    both.append(jnp.dot(wbig[h], rhs, preferred_element_type=F32).astype(BF16))
                for aa, spot in enumerate(spots):
                    rows = pl.ds(pl.multiple_of(spot * PAIR, PAIR), PAIR)
                    terms = [res[PAIR * k:PAIR * k + PAIR, LANES * aa:LANES * aa + LANES] for res in both for k in range(PAIR)]
                    for m in range(11):
                        for side, val in enumerate(merge_three(*terms[3 * m:3 * m + 3])):
                            ys[rows, pl.ds(WIDE * m + LANES * side, LANES)] = val
            return carry

        xo, xu, xd = wrap4(x + 2), wrap4(x + 1), wrap4(x - 1)

        def sigma(cols):
            for half in range(2):
                res = lax.dot_general(rt[pl.ds(320 * half, 320), :], ys[cols, :], (((1,), (1,)), ((), ())), preferred_element_type=F32)
                for idx in range(RING):
                    part[2 * half + idx // 2, idx % 2, :, cols] = res[idx * COLS:idx * COLS + COLS]

        class Chunk:
            def __init__(self, num, start, width):
                cols = self.cols = pl.ds(start, width)
                self.rows = start // LANES, (start + width) // LANES
                self.swap = remote(part.at[:, 1 - label, :, cols], rd.at[:, :, cols], d_s.at[num], d_r.at[num], partner)
                plan = ((xo, lo, ra, lo, x_up), (xo, hi, rb, lo, x_dn), (xu, hi, fl, hi, x_up), (xd, lo, fr, lo, x_dn), (xu, lo, fl, lo, x_up), (xd, hi, fr, hi, x_dn))
                self.copies = [remote(ssum.at[chip, rows, cols], dst.at[to, cols], ring_s.at[6 * num + idx], ring_r.at[6 * num + idx], dev)
                               for idx, (chip, rows, dst, to, dev) in enumerate(plan)]

            def make_y(self):
                lax.fori_loop(*self.rows, some_rows, 0)

            def make(self):
                sigma(self.cols)
                self.swap.start()

            def add(self):
                self.swap.wait()
                for chip in range(RING):
                    ssum[chip, :, self.cols] = part[chip, label, :, self.cols] + rd[chip, :, self.cols]
                for cp in self.copies[:RING]:
                    cp.start()

            def pass_on(self):
                self.copies[0].wait_recv()
                ssum[xu, lo, self.cols] = ssum[xu, lo, self.cols] + ra[:, self.cols]
                self.copies[RING].start()
                self.copies[1].wait_recv()
                ssum[xd, hi, self.cols] = ssum[xd, hi, self.cols] + rb[:, self.cols]
                self.copies[5].start()

            def finish(self):
                for cp in self.copies[2:]:
                    cp.wait_recv()
                fin[pl.ds(0, COLS), self.cols] = ssum[x, :, self.cols] + fl[:, self.cols] + fr[:, self.cols]
                for cp in self.copies:
                    cp.wait_send()

        one, two, three = (Chunk(*spec) for spec in ((0, 0, WIDE), (1, WIDE, WIDE), (2, 512, LANES)))
        with jax.named_scope("w0"):
            one.make_y()
        with jax.named_scope("r0"):
            one.make()
        with jax.named_scope("w1"):
            two.make_y()
        with jax.named_scope("add0"):
            one.add()
        with jax.named_scope("r1"):
            two.make()
        with jax.named_scope("w2"):
            three.make_y()
        with jax.named_scope("add1"):
            two.add()
        with jax.named_scope("r2"):
            three.make()
        with jax.named_scope("pass0"):
            one.pass_on()
        with jax.named_scope("add2"):
            three.add()
        with jax.named_scope("pass1"):
            two.pass_on()
            three.pass_on()
        with jax.named_scope("xfin"):
            v_cur = vt[cur]
            n_loc = total(v_cur * v_cur)
            c_loc = total(v_cur * vt[prev])
            one.finish()
            two.finish()
            three.finish()
        with jax.named_scope("turn"):
            for b in range(5):
                rows = pl.ds(LANES * b, LANES)
                sig[rows, :] = jnp.where(row_lane < COLS, fin[:, rows].T, 0.0)

        with jax.named_scope("vec1"):
            t_val = sig[...] - beta * vt[prev]
            s_loc = total(t_val * vt[cur])
            sig[...] = t_val
            w_val = t_val - ratio(s_loc, n_loc) * vt[cur]
            e_loc = total(w_val * w_val)
        with jax.named_scope("allred"):
            def last_start():
                pl.when(step == NUM_STEPS - 1)(out_start)

            n, s, e, c = all_reduce([n_loc, s_loc, e_loc, c_loc], last_start)
            pl.when(step < NUM_STEPS - 1)(out_start)
        with jax.named_scope("vec2"):
            alpha = (s + beta * c) / VEC
            diff = alpha - ratio(s, n)
            beta_new = jnp.sqrt((e + diff * n * diff) / VEC)
            inv = 1.0 / beta_new
            vt[nxt] = (sig[...] - alpha * vt[cur]) * inv
            fin[pl.ds(COLS, 1), :] = jnp.broadcast_to(alpha, (1, BOND))
            fin[pl.ds(COLS + GC, 1), :] = jnp.broadcast_to(inv, (1, BOND))
            alphas[step] = alpha[0, 0]
            betas[step] = beta_new[0, 0]
        return beta_new

    lax.fori_loop(0, NUM_STEPS, step_body, jnp.zeros((1, 1), F32))
    out_finish(NUM_STEPS)
    cp_v.wait()


def run_kernel(psi, left, pair, order, right):
    vmem, anys, smem = (pl.BlockSpec(memory_space=space) for space in (pltpu.VMEM, pl.ANY, pltpu.SMEM))
    dma = pltpu.SemaphoreType.DMA
    vm = pltpu.VMEM
    block = (COLS, BOND)
    scratch = [
        vm((RING, 2, 160, BOND), BF16), vm((2, 1280, 768), BF16), vm((2, WIDE, WIDE), BF16), vm((2816, BOND), BF16), vm((BOND, 2816), BF16),
        vm((RING, RING, 25, PAIR, LANES), BF16), vm((PAIR, 1280, LANES), BF16), vm((BOND, 2816), BF16), vm((RING, 2) + block, F32),
        vm((RING,) + block, F32), vm((RING,) + block, F32), vm((ROWS, BOND), F32), vm((ROWS, BOND), F32), vm(block, F32), vm(block, F32),
        vm((LANES, BOND), F32), vm((BOND, LANES), F32), vm((3, BOND, LANES), F32), vm((GC, COLS, LANES), F32), vm((GC, COLS, LANES), F32), vm(block, F32),
        vm((LANES, 2, LANES), F32),
    ] + [dma((num,)) for num in (GC, GC, GC, GC, GC, GC, RING * GSEM, RING * GSEM, 3, 3, 18, 18)] + [dma, dma, dma((3,)), pltpu.SemaphoreType.REGULAR]
    scal = jax.ShapeDtypeStruct((NUM_STEPS,), F32)
    return pl.pallas_call(
        kernel,
        out_shape=(jax.ShapeDtypeStruct((NUM_STEPS + 1,) + block, F32), scal, scal),
        in_specs=[vmem, anys, vmem, vmem, anys],
        out_specs=(anys, smem, smem),
        scratch_shapes=scratch,
        compiler_params=pltpu.CompilerParams(collective_id=0, has_side_effects=True, vmem_limit_bytes=67043328),
        name="lanczos",
    )(psi, left, pair, order, right)


def solution(mesh):
    def local_run(wave_rows, left_rows, op_pair, right_env):
        psi = wave_rows.reshape(COLS, BOND)
        left = jnp.transpose(left_rows, (1, 0, 2)).reshape(160, BOND)
        vecs, alphas, betas = run_kernel(psi, left, op_pair.reshape(512, PAIR), left_order(), right_env)
        return vecs.reshape(7, 5, RING, RING, BOND), alphas, betas

    rows = "rows"
    return jax.shard_map(local_run, mesh=mesh, in_specs=(P(rows), P(None, rows), P(), P()), out_specs=(P(None, rows), P(), P()), check_vma=False)
```

```python
import itertools

import jax
import jax.numpy as jnp
import numpy as np
from jax import lax
from jax.experimental import pallas as pl
from jax.experimental.pallas import tpu as pltpu
from jax.sharding import PartitionSpec as P

NUM_STEPS = 6
MESH = pl.DeviceIdType.MESH
F32 = jnp.float32
BF16 = jnp.bfloat16

ROWS, COLS = 40, 80
BOND, PAIR, TERMS = 640, 16, 32
LANES = 128
GC, RING, WIDE = 8, 4, 256
VEC = BOND * BOND * PAIR
PARTS = ((((0, 4), (4, 3)), ((7, 4), (11, 4))), (((15, 2), (17, 3)), ((20, 3), (23, 2))))
ORDER = "001000P1111001Q1001101R0L1L01"
GSEM = 30
FARTHEST = sorted(itertools.product(range(4), range(4), range(4), range(2)), key=lambda off: -sum(min(d, 4 - d) for d in off))[:-1]


def left_order():
    col = np.arange(1024)
    group, tail = (col % WIDE) // PAIR, col >= 512
    src = np.where(tail, ROWS * group + 32 + col % GC, ROWS * group + PAIR * (col // WIDE) + col % PAIR)
    used = ~tail | ((col // GC) % 2 == (col >= 768))
    return jnp.asarray((np.arange(BOND)[:, None] == src) & used, BF16)


def remote(src, dst, send, recv, dev):
    return pltpu.make_async_remote_copy(src_ref=src, dst_ref=dst, send_sem=send, recv_sem=recv, device_id=(dev,), device_id_type=MESH)


def tile_of(lane_tile, row_tile):
    return 15 + 2 * lane_tile + row_tile - 2 if row_tile in (2, 3) else 3 * lane_tile + min(row_tile, 2)


def lane_roll(val, shift):
    shift = shift % LANES
    return val if shift == 0 else pltpu.roll(val, shift, axis=val.ndim - 1)


def lane_iota(val):
    return lax.broadcasted_iota(jnp.int32, val.shape, val.ndim - 1)


def take_piece(tiles, idx):
    tile, off = divmod(COLS * idx, LANES)
    out = lane_roll(tiles(tile), -off)
    lane = lane_iota(out)
    if off + COLS > LANES:
        out = jnp.where(lane < LANES - off, out, lane_roll(tiles(tile + 1), -off))
    return jnp.where(lane < COLS, out, jnp.zeros_like(out))


def merge_three(one, two, three=None):
    if three is None:
        return one, two
    inner = lane_iota(one) < COLS
    return jnp.where(inner, one, lane_roll(three, COLS)), jnp.where(inner, two, lane_roll(three, COLS - 48))


def split_three(left, right):
    lane, zero = lane_iota(left), jnp.zeros_like(left)
    three = jnp.where(lane < 48, lane_roll(left, -COLS), jnp.where(lane < COLS, lane_roll(right, 48 - COLS), zero))
    return jnp.where(lane < COLS, left, zero), jnp.where(lane < COLS, right, zero), three


def dense_tile(pieces, tile):
    out = None
    for idx in range(GC):
        shift = COLS * idx - LANES * tile
        if shift <= -COLS or shift >= LANES:
            continue
        moved = lane_roll(pieces(idx), shift)
        out = moved if out is None else jnp.where(lane_iota(moved) >= shift, moved, out)
    return out


def kernel(psi, left, pair, order_hbm, right, vecs, alphas, betas, order, lall, lh, wbig, rtmp, rt, ug, xs, ys, part, rd, ssum, ra, rb, fl, fr, fin,
           sig, vt, piece_buf, out_recv, outv, stat, psi_s, psi_r, l_s, l_r, out_s, out_r, g_s, g_r, d_s, d_r,
           ring_s, ring_r, a_s, a_r, loc, ready):
    me = lax.axis_index("rows")
    core = lax.rem(me, 2)
    x = lax.rem(me // 2, RING)
    y = lax.rem(me // GC, RING)
    z = me // 32
    i = me // GC
    t_me = lax.rem(me, GC)
    label = lax.rem(me + x + y + z, 2)
    j = x * 2 + label
    lo, hi = pl.ds(0, ROWS), pl.ds(ROWS, ROWS)

    def wrap4(val):
        return lax.rem(val + RING, RING)

    def in_row(d):
        tt = lax.rem(t_me + d, GC)
        return tt, tt - lax.rem(tt, 2) + lax.rem(tt + tt // 2 + y + z, 2), i * GC + tt

    def rows_of(jj):
        return pl.ds(pl.multiple_of(jj * COLS, COLS), COLS)

    barrier = pltpu.get_barrier_semaphore()

    def col_dev(di):
        ii = lax.rem(i + di, PAIR)
        return ii * GC + x * 2 + lax.rem(label + x + ii + ii // RING, 2)

    for d in range(1, GC):
        pl.semaphore_signal(barrier, inc=1, device_id=(in_row(d)[2],), device_id_type=MESH)
    for di in range(1, PAIR):
        pl.semaphore_signal(barrier, inc=1, device_id=(col_dev(di),), device_id_type=MESH)
    pl.semaphore_wait(barrier, 22)
    for di in range(1, PAIR):
        pl.semaphore_signal(ready, inc=1, device_id=(col_dev(di),), device_id_type=MESH)

    partner = me + 1 - 2 * core
    places = ([wrap4(z + d) * 32 for d in range(RING)], [wrap4(y + d) * GC for d in range(RING)], [wrap4(x + d) * 2 for d in range(RING)], (core, 1 - core))
    x_up, x_dn = i * GC + wrap4(x + 1) * 2 + 1 - core, i * GC + wrap4(x - 1) * 2 + 1 - core
    left_up, left_dn = (i * GC + wrap4(x + d) * 2 + core for d in (1, -1))
    my_rows = rows_of(t_me)

    def fetch_right(first, last, row, width):
        def body(m, carry):
            src = right.at[3 * m + first, pl.ds(pl.multiple_of(j * COLS + row, PAIR), width), :]
            pltpu.make_async_copy(src, rtmp.at[pl.ds(pl.multiple_of(WIDE * m + last, PAIR), width), :], loc.at[0]).start()
            return carry
        return body

    lax.fori_loop(0, 11, fetch_right(0, 0, 0, COLS), 0)
    lax.fori_loop(0, 11, fetch_right(1, LANES, 0, COLS), 0)
    lax.fori_loop(0, 10, fetch_right(2, COLS, 0, 48), 0)
    lax.fori_loop(0, 10, fetch_right(2, LANES + COLS, 48, 32), 0)
    cp_l = pltpu.make_async_copy(left, lall.at[x, core], loc.at[1])
    cp_l.start()
    cp_order = pltpu.make_async_copy(order_hbm, order, loc.at[3])
    cp_order.start()

    row_lane = lax.broadcasted_iota(jnp.int32, (1, LANES), 1)

    def total(val):
        return jnp.sum(jnp.sum(val, axis=0, keepdims=True), axis=1, keepdims=True)

    def ratio(num, den):
        good = den > 0
        return jnp.where(good, num / jnp.where(good, den, 1.0), 0.0)

    def all_reduce(stats, hook):
        row = jnp.zeros((1, LANES), F32)
        for idx, val in enumerate(stats):
            row = jnp.where(row_lane == idx, val, row)
        stat[me, pl.ds(0, 1), :] = row
        stat[me, pl.ds(1, 1), :] = jnp.broadcast_to(ratio(stats[1], stats[0]), (1, LANES))

        for off in FARTHEST:
            dev = sum(spot[step] for spot, step in zip(places, off))
            remote(stat.at[me], stat.at[me], a_s, a_r, dev).start()
        hook()
        most = stat.at[pl.ds(0, LANES - 1)]
        with jax.named_scope("arwait"):
            remote(most, most, a_s, a_r, partner).wait()
        rows = stat[:, pl.ds(0, 1), :]
        sums = jnp.sum(rows, axis=0)
        n, s, e, c = (jnp.sum(jnp.where(row_lane == idx, sums, 0.0), axis=1, keepdims=True) for idx in range(RING))
        diff = stat[:, pl.ds(1, 1), :] - ratio(s, n)[None]
        moved = jnp.sum(diff * rows * diff, axis=0)
        return n, s, e + jnp.sum(jnp.where(row_lane == 0, moved, 0.0), axis=1, keepdims=True), c

    def l_copy(src, rows, idx, dev):
        ref = lall.at[src[0], src[1], rows]
        return remote(ref, ref, l_s.at[idx], l_r.at[idx], dev)

    every, low, high = pl.ds(0, 160), pl.ds(0, COLS), pl.ds(COLS, COLS)

    def psi_pieces():
        for jj in range(GC):
            piece_buf[jj] = take_piece(lambda t: psi[:, LANES * t:LANES * t + LANES], jj)
        vt[0, my_rows, :] = piece_buf[j]
        spread = jnp.where(lax.broadcasted_iota(jnp.int32, (PAIR, WIDE), 1) // PAIR == lax.broadcasted_iota(jnp.int32, (PAIR, WIDE), 0), 1.0, 0.0).astype(BF16)
        same = lax.broadcasted_iota(jnp.int32, (WIDE, WIDE), 1) % PAIR == lax.broadcasted_iota(jnp.int32, (WIDE, WIDE), 0) // PAIR
        for h in range(2):
            wide = jnp.dot(pair[pl.ds(WIDE * h, WIDE), :], spread, preferred_element_type=F32)
            wbig[h] = jnp.where(same, wide, 0.0).astype(BF16)
        vt[2] = jnp.zeros((BOND, LANES), F32)
        fin[...] = jnp.zeros((LANES, BOND), F32)

    def psi_sends():
        for d in range(1, GC):
            tt, jj, dev = in_row(d)
            remote(piece_buf.at[jj], vt.at[0, my_rows], psi_s.at[tt], psi_r.at[t_me], dev).start()
        cp_l.wait()
        l_copy((x, core), every, 0, left_up).start()
        l_copy((x, core), every, 1, left_dn).start()
        l_copy((x, core), every, RING, partner).start()

    def turn_right():
        some = rtmp.at[pl.ds(0, TERMS * COLS), :]
        pltpu.make_async_copy(some, some, loc.at[0]).wait()
        for m in range(11):
            rtmp[pl.ds(WIDE * m + 240, PAIR), :] = jnp.zeros((PAIR, BOND), BF16)
        for start in (COLS, LANES + COLS):
            rtmp[pl.ds(2560 + start, 48), :] = jnp.zeros((48, BOND), BF16)

        def body(k, carry):
            cols = pl.ds(pl.multiple_of(k * LANES, LANES), LANES)
            for b in range(5):
                rt[pl.ds(LANES * b, LANES), cols] = rtmp[cols, pl.ds(LANES * b, LANES)].T
            return carry

        lax.fori_loop(0, 22, body, 0)

    lower, upper, far = (wrap4(x - 1), core), (wrap4(x + 1), core), (wrap4(x + 2), core)

    def left_forward():
        for idx, (block, way, rows) in enumerate(((lower, left_up, low), (upper, left_dn, high))):
            l_copy(block, every, idx, way).wait_recv()
            l_copy(block, rows, idx + 2, way).start()
            l_copy(block, every, idx + 5, partner).start()

    def left_far():
        l_copy(far, low, 2, partner).wait_recv()
        l_copy(far, high, 3, partner).wait_recv()
        l_copy(far, every, 7, partner).start()

    def start_up():
        with jax.named_scope("psi"):
            psi_sends()
        with jax.named_scope("turnr"):
            turn_right()

    psi_pieces()
    psi_val = psi[...]
    pl.semaphore_wait(ready, PAIR - 1)
    zero = jnp.zeros((1, 1), F32)
    n_psi = all_reduce([total(psi_val * psi_val), zero], start_up)[0]
    inv_norm = 1.0 / jnp.sqrt(n_psi / VEC)

    for d in range(1, GC):
        tt, jj, dev = in_row(d)
        cp = remote(piece_buf.at[jj], vt.at[0, rows_of(tt)], psi_s.at[tt], psi_r.at[tt], dev)
        cp.wait_recv()
        cp.wait_send()
    vt[0] = vt[0] * inv_norm
    outv[...] = psi_val * inv_norm
    cp_v = pltpu.make_async_copy(outv, vecs.at[0], loc.at[2])
    cp_v.start()

    def left_finish():
        for idx, dx in ((RING, 0), (5, 3), (6, 1), (7, 2)):
            l_copy((wrap4(x + dx), 1 - core), every, idx, partner).wait_recv()
        for idx, rows in enumerate((every, every, low, high) + (every,) * RING):
            l_copy((x, core), rows, idx, partner).wait_send()

        cp_order.wait()

        def body(t, carry):
            rows = pl.ds(pl.multiple_of(t * 160, 160), 160)
            res = jnp.dot(lall[t // 2, t % 2], order[...], preferred_element_type=F32).astype(BF16)
            for h in range(2):
                lh[h, rows, :] = jnp.concatenate([res[:, :512], res[:, 512 + WIDE * h:768 + WIDE * h]], axis=1)
            return carry

        lax.fori_loop(0, GC, body, 0)

    def flow(base, firsts, seconds, ref, parts):
        done = []
        offs = (0, -1, 1, 2)

        def send(blk, prt, idx, dev):
            here = ref(blk, parts[prt])
            cp = remote(here, here, g_s.at[base + idx], g_r.at[base + idx], dev)
            cp.start()
            done.append(cp)

        def wait(blk, prt, idx):
            here = ref(blk, parts[prt])
            remote(here, here, g_s.at[base + idx], g_r.at[base + idx], partner).wait_recv()

        def second(b, prt):
            for way in ((0, 1) if prt == 0 else (1, 0)):
                send((offs[b], 0), prt, 6 * b + 6 + 2 * way + prt, seconds[way])

        def second_forward(b):
            wait((offs[b], -1), 0, 6 * b + 6)
            send((offs[b], -1), 0, 6 * b + 10, seconds[0])
            wait((offs[b], 1), 1, 6 * b + 9)
            send((offs[b], 1), 1, 6 * b + 11, seconds[1])

        for prt, way in ((0, 0), (1, 1), (1, 0), (0, 1)):
            send((0, 0), prt, 2 * way + prt, firsts[way])
        for prt in range(2):
            send((0, 0), prt, RING + prt, firsts[2])
        yield
        second(0, 0)
        second(0, 1)
        yield
        wait((-1, 0), 0, 0)
        second(1, 0)
        yield
        wait((1, 0), 1, 3)
        second(2, 1)
        yield
        wait((-1, 0), 1, 1)
        second(1, 1)
        wait((1, 0), 0, 2)
        second(2, 0)
        yield
        second_forward(0)
        yield
        wait((2, 0), 0, RING)
        second(3, 0)
        wait((2, 0), 1, 5)
        second(3, 1)
        yield
        for b in range(1, RING):
            second_forward(b)
            yield
        for b in range(RING):
            for off, prt, idx in ((-1, 1, 7), (1, 0, GC), (2, 0, 10), (2, 1, 11)):
                wait((offs[b], off), prt, 6 * b + idx)
        yield
        for cp in done:
            cp.wait_send()
        yield

    def device(dz, dy):
        return (wrap4(z + dz) * RING + wrap4(y + dy)) * GC + x * 2 + (1 - core if (dz + dy) % 2 else core)

    y_ways, z_ways = [device(0, d) for d in (1, -1, 2)], [device(d, 0) for d in (1, -1, 2)]

    def y_first(blk, prt):
        return ug.at[wrap4(z + blk[1]), wrap4(y + blk[0]), pl.ds(*prt)]

    def z_first(blk, prt):
        return ug.at[wrap4(z + blk[0]), wrap4(y + blk[1]), pl.ds(*prt)]

    def gather(hooks):
        flows = [[flow(GSEM * (2 * h + idx), *ways, ref, PARTS[h][idx]) for idx, (ways, ref) in enumerate((((y_ways, z_ways), y_first), ((z_ways, y_ways), z_first)))]
                 for h in range(2)]
        for mark in ORDER:
            if mark in hooks:
                hooks[mark]()
            else:
                for one in flows[int(mark)]:
                    next(one)

    def out_copy(slot, tt, dev):
        return remote(sig.at[rows_of(tt)], out_recv.at[slot], out_s.at[tt], out_r.at[slot], dev)

    def out_start():
        for d in range(1, GC):
            tt, jj, dev = in_row(d)
            out_copy(j, tt, dev).start()
        out_recv[j] = sig[my_rows, :]

    def out_finish(step):
        for d in range(1, GC):
            tt, jj, dev = in_row(d)
            out_copy(jj, tt, dev).wait_recv()
            out_copy(j, tt, dev).wait_send()
        cp_v.wait()
        alpha, inv = fin[pl.ds(COLS, 1), pl.ds(0, 1)], fin[pl.ds(COLS + GC, 1), pl.ds(0, 1)]
        for tile in range(5):
            lanes = pl.ds(LANES * tile, LANES)
            outv[:, lanes] = (dense_tile(lambda idx: out_recv[idx], tile) - alpha * outv[:, lanes]) * inv
        pltpu.make_async_copy(outv, vecs.at[step], loc.at[2]).start()

    def step_body(step, beta):
        cur = lax.rem(step, 3)
        prev = lax.rem(step + 2, 3)
        nxt = lax.rem(step + 1, 3)

        with jax.named_scope("pack"):
            strided = [vt[cur, pl.ds(r, ROWS, stride=PAIR), :] for r in range(PAIR)]
            for lt in range(5):
                half = [dense_tile(lambda idx, h=h: strided[GC * h + idx], lt) for h in range(2)]
                for h in range(2):
                    for tt in range(2):
                        ug[z, y, tile_of(lt, 2 * h + tt)] = half[h][PAIR * tt:PAIR * tt + PAIR].astype(BF16)
                ug[z, y, tile_of(lt, RING)] = jnp.concatenate([half[0][32:ROWS], half[1][32:ROWS]], axis=0).astype(BF16)

        def early():
            pl.when(step == 0)(left_forward)

        def middle():
            pl.when(step == 0)(left_far)

            @pl.when(step > 0)
            def _():
                out_finish(step)

        def late():
            pl.when(step == 0)(left_finish)

        halves = iter(range(2))

        def left_half():
            h = next(halves)
            for group in range(3):
                first = 3 * group
                got = []
                for r in range(first, min(first + 3, GC)):
                    rows = [take_piece(lambda t, tr=tr: ug[:, :, tile_of(t, tr)].reshape(WIDE, LANES), r) for tr in (2 * h, 2 * h + 1, RING)]
                    got.append(jnp.concatenate(rows, axis=0))
                rhs = jnp.concatenate(merge_three(*got), axis=1)
                for mc in range(2):
                    rows = pl.ds(BOND * mc, BOND)
                    res = jnp.dot(lh[h, rows, :], rhs, preferred_element_type=F32).astype(BF16)
                    for rr, val in enumerate(split_three(res[:, :LANES], res[:, LANES:])[:len(got)]):
                        xs[h * GC + first + rr, rows, :] = val

        def named(name, call):
            def run():
                with jax.named_scope(name):
                    call()
            return run

        with jax.named_scope("gather"):
            gather({"P": early, "Q": middle, "R": named("late", late), "L": named("left", left_half)})

        def some_rows(ap, carry):
            for pr in range(RING):
                spots = [ap * GC + 2 * pr + aa for aa in range(2)]
                both = []
                for h in range(2):
                    rhs = jnp.concatenate([xs[:, pl.ds(pl.multiple_of(spot * 32 + PAIR * h, PAIR), PAIR), :].reshape(WIDE, LANES) for spot in spots], axis=1)
                    both.append(jnp.dot(wbig[h], rhs, preferred_element_type=F32).astype(BF16))
                for aa, spot in enumerate(spots):
                    rows = pl.ds(pl.multiple_of(spot * PAIR, PAIR), PAIR)
                    terms = [res[PAIR * k:PAIR * k + PAIR, LANES * aa:LANES * aa + LANES] for res in both for k in range(PAIR)]
                    for m in range(11):
                        for side, val in enumerate(merge_three(*terms[3 * m:3 * m + 3])):
                            ys[rows, pl.ds(WIDE * m + LANES * side, LANES)] = val
            return carry

        xo, xu, xd = wrap4(x + 2), wrap4(x + 1), wrap4(x - 1)

        def sigma(cols):
            for half in range(2):
                res = lax.dot_general(rt[pl.ds(320 * half, 320), :], ys[cols, :], (((1,), (1,)), ((), ())), preferred_element_type=F32)
                for idx in range(RING):
                    part[2 * half + idx // 2, idx % 2, :, cols] = res[idx * COLS:idx * COLS + COLS]

        class Chunk:
            def __init__(self, num, start, width):
                cols = self.cols = pl.ds(start, width)
                self.rows = start // LANES, (start + width) // LANES
                self.swap = remote(part.at[:, 1 - label, :, cols], rd.at[:, :, cols], d_s.at[num], d_r.at[num], partner)
                plan = ((xo, lo, ra, lo, x_up), (xo, hi, rb, lo, x_dn), (xu, hi, fl, hi, x_up), (xd, lo, fr, lo, x_dn), (xu, lo, fl, lo, x_up), (xd, hi, fr, hi, x_dn))
                self.copies = [remote(ssum.at[chip, rows, cols], dst.at[to, cols], ring_s.at[6 * num + idx], ring_r.at[6 * num + idx], dev)
                               for idx, (chip, rows, dst, to, dev) in enumerate(plan)]

            def make_y(self):
                for group in range(*self.rows):
                    some_rows(group, 0)

            def make(self):
                sigma(self.cols)
                self.swap.start()

            def add(self):
                self.swap.wait()
                for chip in range(RING):
                    ssum[chip, :, self.cols] = part[chip, label, :, self.cols] + rd[chip, :, self.cols]
                for cp in self.copies[:RING]:
                    cp.start()

            def pass_on(self):
                self.copies[0].wait_recv()
                ssum[xu, lo, self.cols] = ssum[xu, lo, self.cols] + ra[:, self.cols]
                self.copies[RING].start()
                self.copies[1].wait_recv()
                ssum[xd, hi, self.cols] = ssum[xd, hi, self.cols] + rb[:, self.cols]
                self.copies[5].start()

            def finish(self):
                for cp in self.copies[2:]:
                    cp.wait_recv()
                fin[pl.ds(0, COLS), self.cols] = ssum[x, :, self.cols] + fl[:, self.cols] + fr[:, self.cols]
                for cp in self.copies:
                    cp.wait_send()

        one, two, three = (Chunk(*spec) for spec in ((0, 0, WIDE), (1, WIDE, WIDE), (2, 512, LANES)))
        with jax.named_scope("w0"):
            one.make_y()
        with jax.named_scope("r0"):
            one.make()
        with jax.named_scope("w1"):
            two.make_y()
        with jax.named_scope("add0"):
            one.add()
        with jax.named_scope("r1"):
            two.make()
        with jax.named_scope("w2"):
            three.make_y()
        with jax.named_scope("add1"):
            two.add()
        with jax.named_scope("r2"):
            three.make()
        with jax.named_scope("pass0"):
            one.pass_on()
        with jax.named_scope("add2"):
            three.add()
        with jax.named_scope("pass1"):
            two.pass_on()
            three.pass_on()
        with jax.named_scope("xfin"):
            v_cur = vt[cur]
            n_loc = total(v_cur * v_cur)
            c_loc = total(v_cur * vt[prev])
            one.finish()
            two.finish()
            three.finish()
        with jax.named_scope("turn"):
            for b in range(5):
                rows = pl.ds(LANES * b, LANES)
                sig[rows, :] = jnp.where(row_lane < COLS, fin[:, rows].T, 0.0)

        with jax.named_scope("vec1"):
            t_val = sig[...] - beta * vt[prev]
            s_loc = total(t_val * vt[cur])
            sig[...] = t_val
            w_val = t_val - ratio(s_loc, n_loc) * vt[cur]
            e_loc = total(w_val * w_val)
        with jax.named_scope("allred"):
            def last_start():
                pl.when(step == NUM_STEPS - 1)(out_start)

            n, s, e, c = all_reduce([n_loc, s_loc, e_loc, c_loc], last_start)
            pl.when(step < NUM_STEPS - 1)(out_start)
        with jax.named_scope("vec2"):
            alpha = (s + beta * c) / VEC
            diff = alpha - ratio(s, n)
            beta_new = jnp.sqrt((e + diff * n * diff) / VEC)
            inv = 1.0 / beta_new
            vt[nxt] = (sig[...] - alpha * vt[cur]) * inv
            fin[pl.ds(COLS, 1), :] = jnp.broadcast_to(alpha, (1, BOND))
            fin[pl.ds(COLS + GC, 1), :] = jnp.broadcast_to(inv, (1, BOND))
            alphas[step] = alpha[0, 0]
            betas[step] = beta_new[0, 0]
        return beta_new

    lax.fori_loop(0, NUM_STEPS, step_body, jnp.zeros((1, 1), F32))
    out_finish(NUM_STEPS)
    cp_v.wait()


def run_kernel(psi, left, pair, order, right):
    vmem, anys, smem = (pl.BlockSpec(memory_space=space) for space in (pltpu.VMEM, pl.ANY, pltpu.SMEM))
    dma = pltpu.SemaphoreType.DMA
    vm = pltpu.VMEM
    block = (COLS, BOND)
    scratch = [
        vm((BOND, 1024), BF16),
        vm((RING, 2, 160, BOND), BF16), vm((2, 1280, 768), BF16), vm((2, WIDE, WIDE), BF16), vm((2816, BOND), BF16), vm((BOND, 2816), BF16),
        vm((RING, RING, 25, PAIR, LANES), BF16), vm((PAIR, 1280, LANES), BF16), vm((BOND, 2816), BF16), vm((RING, 2) + block, F32),
        vm((RING,) + block, F32), vm((RING,) + block, F32), vm((ROWS, BOND), F32), vm((ROWS, BOND), F32), vm(block, F32), vm(block, F32),
        vm((LANES, BOND), F32), vm((BOND, LANES), F32), vm((3, BOND, LANES), F32), vm((GC, COLS, LANES), F32), vm((GC, COLS, LANES), F32), vm(block, F32),
        vm((LANES, 2, LANES), F32),
    ] + [dma((num,)) for num in (GC, GC, GC, GC, GC, GC, RING * GSEM, RING * GSEM, 3, 3, 18, 18)] + [dma, dma, dma((RING,)), pltpu.SemaphoreType.REGULAR]
    scal = jax.ShapeDtypeStruct((NUM_STEPS,), F32)
    return pl.pallas_call(
        kernel,
        out_shape=(jax.ShapeDtypeStruct((NUM_STEPS + 1,) + block, F32), scal, scal),
        in_specs=[vmem, anys, vmem, anys, anys],
        out_specs=(anys, smem, smem),
        scratch_shapes=scratch,
        compiler_params=pltpu.CompilerParams(collective_id=0, has_side_effects=True, vmem_limit_bytes=67043328),
        name="lanczos",
    )(psi, left, pair, order, right)


def solution(mesh):
    def local_run(wave_rows, left_rows, op_pair, right_env):
        psi = wave_rows.reshape(COLS, BOND)
        left = jnp.transpose(left_rows, (1, 0, 2)).reshape(160, BOND)
        vecs, alphas, betas = run_kernel(psi, left, op_pair.reshape(512, PAIR), left_order(), right_env)
        return vecs.reshape(7, 5, RING, RING, BOND), alphas, betas

    rows = "rows"
    return jax.shard_map(local_run, mesh=mesh, in_specs=(P(rows), P(None, rows), P(), P()), out_specs=(P(None, rows), P(), P()), check_vma=False)
```

```python
import itertools

import jax
import jax.numpy as jnp
import numpy as np
from jax import lax
from jax.experimental import pallas as pl
from jax.experimental.pallas import tpu as pltpu
from jax.sharding import PartitionSpec as P

NUM_STEPS = 6
MESH = pl.DeviceIdType.MESH
F32 = jnp.float32
BF16 = jnp.bfloat16

ROWS, COLS = 40, 80
BOND, PAIR, TERMS = 640, 16, 32
LANES = 128
GC, RING, WIDE = 8, 4, 256
VEC = BOND * BOND * PAIR
PARTS = ((((0, 4), (4, 3)), ((7, 4), (11, 4))), (((15, 2), (17, 3)), ((20, 3), (23, 2))))
ORDER = "0011000P111001Q1001101R0L1L01"
GSEM = 30
FARTHEST = sorted(itertools.product(range(4), range(4), range(4), range(2)), key=lambda off: -sum(min(d, 4 - d) for d in off))[:-1]


def left_order():
    col = np.arange(1024)
    group, tail = (col % WIDE) // PAIR, col >= 512
    src = np.where(tail, ROWS * group + 32 + col % GC, ROWS * group + PAIR * (col // WIDE) + col % PAIR)
    used = ~tail | ((col // GC) % 2 == (col >= 768))
    return jnp.asarray((np.arange(BOND)[:, None] == src) & used, BF16)


def remote(src, dst, send, recv, dev):
    return pltpu.make_async_remote_copy(src_ref=src, dst_ref=dst, send_sem=send, recv_sem=recv, device_id=(dev,), device_id_type=MESH)


def tile_of(lane_tile, row_tile):
    return 15 + 2 * lane_tile + row_tile - 2 if row_tile in (2, 3) else 3 * lane_tile + min(row_tile, 2)


def lane_roll(val, shift):
    shift = shift % LANES
    return val if shift == 0 else pltpu.roll(val, shift, axis=val.ndim - 1)


def lane_iota(val):
    return lax.broadcasted_iota(jnp.int32, val.shape, val.ndim - 1)


def take_piece(tiles, idx):
    tile, off = divmod(COLS * idx, LANES)
    out = lane_roll(tiles(tile), -off)
    lane = lane_iota(out)
    if off + COLS > LANES:
        out = jnp.where(lane < LANES - off, out, lane_roll(tiles(tile + 1), -off))
    return jnp.where(lane < COLS, out, jnp.zeros_like(out))


def merge_three(one, two, three=None):
    if three is None:
        return one, two
    inner = lane_iota(one) < COLS
    return jnp.where(inner, one, lane_roll(three, COLS)), jnp.where(inner, two, lane_roll(three, COLS - 48))


def split_three(left, right):
    lane, zero = lane_iota(left), jnp.zeros_like(left)
    three = jnp.where(lane < 48, lane_roll(left, -COLS), jnp.where(lane < COLS, lane_roll(right, 48 - COLS), zero))
    return jnp.where(lane < COLS, left, zero), jnp.where(lane < COLS, right, zero), three


def dense_tile(pieces, tile):
    out = None
    for idx in range(GC):
        shift = COLS * idx - LANES * tile
        if shift <= -COLS or shift >= LANES:
            continue
        moved = lane_roll(pieces(idx), shift)
        out = moved if out is None else jnp.where(lane_iota(moved) >= shift, moved, out)
    return out


def kernel(psi, left, pair, order_hbm, right, vecs, alphas, betas, order, lall, lh, wbig, rtmp, rt, ug, xs, ys, part, rd, ssum, ra, rb, fl, fr, fin,
           sig, vt, piece_buf, out_recv, outv, stat, psi_s, psi_r, l_s, l_r, out_s, out_r, g_s, g_r, d_s, d_r,
           ring_s, ring_r, a_s, a_r, loc, ready):
    me = lax.axis_index("rows")
    core = lax.rem(me, 2)
    x = lax.rem(me // 2, RING)
    y = lax.rem(me // GC, RING)
    z = me // 32
    i = me // GC
    t_me = lax.rem(me, GC)
    label = lax.rem(me + x + y + z, 2)
    j = x * 2 + label
    lo, hi = pl.ds(0, ROWS), pl.ds(ROWS, ROWS)

    def wrap4(val):
        return lax.rem(val + RING, RING)

    def in_row(d):
        tt = lax.rem(t_me + d, GC)
        return tt, tt - lax.rem(tt, 2) + lax.rem(tt + tt // 2 + y + z, 2), i * GC + tt

    def rows_of(jj):
        return pl.ds(pl.multiple_of(jj * COLS, COLS), COLS)

    barrier = pltpu.get_barrier_semaphore()

    def col_dev(di):
        ii = lax.rem(i + di, PAIR)
        return ii * GC + x * 2 + lax.rem(label + x + ii + ii // RING, 2)

    for d in range(1, GC):
        pl.semaphore_signal(barrier, inc=1, device_id=(in_row(d)[2],), device_id_type=MESH)
    for di in range(1, PAIR):
        pl.semaphore_signal(barrier, inc=1, device_id=(col_dev(di),), device_id_type=MESH)
    pl.semaphore_wait(barrier, 22)
    for di in range(1, PAIR):
        pl.semaphore_signal(ready, inc=1, device_id=(col_dev(di),), device_id_type=MESH)

    partner = me + 1 - 2 * core
    places = ([wrap4(z + d) * 32 for d in range(RING)], [wrap4(y + d) * GC for d in range(RING)], [wrap4(x + d) * 2 for d in range(RING)], (core, 1 - core))
    x_up, x_dn = i * GC + wrap4(x + 1) * 2 + 1 - core, i * GC + wrap4(x - 1) * 2 + 1 - core
    left_up, left_dn = (i * GC + wrap4(x + d) * 2 + core for d in (1, -1))
    my_rows = rows_of(t_me)

    def fetch_right(first, last, row, width):
        def body(m, carry):
            src = right.at[3 * m + first, pl.ds(pl.multiple_of(j * COLS + row, PAIR), width), :]
            pltpu.make_async_copy(src, rtmp.at[pl.ds(pl.multiple_of(WIDE * m + last, PAIR), width), :], loc.at[0]).start()
            return carry
        return body

    lax.fori_loop(0, 11, fetch_right(0, 0, 0, COLS), 0)
    lax.fori_loop(0, 11, fetch_right(1, LANES, 0, COLS), 0)
    lax.fori_loop(0, 10, fetch_right(2, COLS, 0, 48), 0)
    lax.fori_loop(0, 10, fetch_right(2, LANES + COLS, 48, 32), 0)
    cp_l = pltpu.make_async_copy(left, lall.at[x, core], loc.at[1])
    cp_l.start()
    cp_order = pltpu.make_async_copy(order_hbm, order, loc.at[3])
    cp_order.start()

    row_lane = lax.broadcasted_iota(jnp.int32, (1, LANES), 1)

    def total(val):
        return jnp.sum(jnp.sum(val, axis=0, keepdims=True), axis=1, keepdims=True)

    def ratio(num, den):
        good = den > 0
        return jnp.where(good, num / jnp.where(good, den, 1.0), 0.0)

    def all_reduce(stats, hook):
        row = jnp.zeros((1, LANES), F32)
        for idx, val in enumerate(stats):
            row = jnp.where(row_lane == idx, val, row)
        stat[me, pl.ds(0, 1), :] = row
        stat[me, pl.ds(1, 1), :] = jnp.broadcast_to(ratio(stats[1], stats[0]), (1, LANES))

        for off in FARTHEST:
            dev = sum(spot[step] for spot, step in zip(places, off))
            remote(stat.at[me], stat.at[me], a_s, a_r, dev).start()
        hook()
        most = stat.at[pl.ds(0, LANES - 1)]
        with jax.named_scope("arwait"):
            remote(most, most, a_s, a_r, partner).wait()
        rows = stat[:, pl.ds(0, 1), :]
        sums = jnp.sum(rows, axis=0)
        n, s, e, c = (jnp.sum(jnp.where(row_lane == idx, sums, 0.0), axis=1, keepdims=True) for idx in range(RING))
        diff = stat[:, pl.ds(1, 1), :] - ratio(s, n)[None]
        moved = jnp.sum(diff * rows * diff, axis=0)
        return n, s, e + jnp.sum(jnp.where(row_lane == 0, moved, 0.0), axis=1, keepdims=True), c

    def l_copy(src, rows, idx, dev):
        ref = lall.at[src[0], src[1], rows]
        return remote(ref, ref, l_s.at[idx], l_r.at[idx], dev)

    every, low, high = pl.ds(0, 160), pl.ds(0, COLS), pl.ds(COLS, COLS)

    def psi_pieces():
        for jj in range(GC):
            piece_buf[jj] = take_piece(lambda t: psi[:, LANES * t:LANES * t + LANES], jj)
        vt[0, my_rows, :] = piece_buf[j]
        spread = jnp.where(lax.broadcasted_iota(jnp.int32, (PAIR, WIDE), 1) // PAIR == lax.broadcasted_iota(jnp.int32, (PAIR, WIDE), 0), 1.0, 0.0).astype(BF16)
        same = lax.broadcasted_iota(jnp.int32, (WIDE, WIDE), 1) % PAIR == lax.broadcasted_iota(jnp.int32, (WIDE, WIDE), 0) // PAIR
        for h in range(2):
            wide = jnp.dot(pair[pl.ds(WIDE * h, WIDE), :], spread, preferred_element_type=F32)
            wbig[h] = jnp.where(same, wide, 0.0).astype(BF16)
        vt[2] = jnp.zeros((BOND, LANES), F32)
        fin[...] = jnp.zeros((LANES, BOND), F32)

    def psi_sends():
        for d in range(1, GC):
            tt, jj, dev = in_row(d)
            remote(piece_buf.at[jj], vt.at[0, my_rows], psi_s.at[tt], psi_r.at[t_me], dev).start()
        cp_l.wait()
        l_copy((x, core), every, 0, left_up).start()
        l_copy((x, core), every, 1, left_dn).start()
        l_copy((x, core), every, RING, partner).start()

    def turn_right():
        some = rtmp.at[pl.ds(0, TERMS * COLS), :]
        pltpu.make_async_copy(some, some, loc.at[0]).wait()
        for m in range(11):
            rtmp[pl.ds(WIDE * m + 240, PAIR), :] = jnp.zeros((PAIR, BOND), BF16)
        for start in (COLS, LANES + COLS):
            rtmp[pl.ds(2560 + start, 48), :] = jnp.zeros((48, BOND), BF16)

        def body(k, carry):
            cols = pl.ds(pl.multiple_of(k * LANES, LANES), LANES)
            for b in range(5):
                rt[pl.ds(LANES * b, LANES), cols] = rtmp[cols, pl.ds(LANES * b, LANES)].T
            return carry

        lax.fori_loop(0, 22, body, 0)

    lower, upper, far = (wrap4(x - 1), core), (wrap4(x + 1), core), (wrap4(x + 2), core)

    def left_forward():
        for idx, (block, way, rows) in enumerate(((lower, left_up, low), (upper, left_dn, high))):
            l_copy(block, every, idx, way).wait_recv()
            l_copy(block, rows, idx + 2, way).start()
            l_copy(block, every, idx + 5, partner).start()

    def left_far():
        l_copy(far, low, 2, partner).wait_recv()
        l_copy(far, high, 3, partner).wait_recv()
        l_copy(far, every, 7, partner).start()

    def start_up():
        with jax.named_scope("psi"):
            psi_sends()
        with jax.named_scope("turnr"):
            turn_right()

    psi_pieces()
    psi_val = psi[...]
    pl.semaphore_wait(ready, PAIR - 1)
    zero = jnp.zeros((1, 1), F32)
    n_psi = all_reduce([total(psi_val * psi_val), zero], start_up)[0]
    inv_norm = 1.0 / jnp.sqrt(n_psi / VEC)

    for d in range(1, GC):
        tt, jj, dev = in_row(d)
        cp = remote(piece_buf.at[jj], vt.at[0, rows_of(tt)], psi_s.at[tt], psi_r.at[tt], dev)
        cp.wait_recv()
        cp.wait_send()
    vt[0] = vt[0] * inv_norm
    outv[...] = psi_val * inv_norm
    cp_v = pltpu.make_async_copy(outv, vecs.at[0], loc.at[2])
    cp_v.start()

    def left_finish():
        for idx, dx in ((RING, 0), (5, 3), (6, 1), (7, 2)):
            l_copy((wrap4(x + dx), 1 - core), every, idx, partner).wait_recv()
        for idx, rows in enumerate((every, every, low, high) + (every,) * RING):
            l_copy((x, core), rows, idx, partner).wait_send()

        cp_order.wait()

        def body(t, carry):
            rows = pl.ds(pl.multiple_of(t * 160, 160), 160)
            res = jnp.dot(lall[t // 2, t % 2], order[...], preferred_element_type=F32).astype(BF16)
            for h in range(2):
                lh[h, rows, :] = jnp.concatenate([res[:, :512], res[:, 512 + WIDE * h:768 + WIDE * h]], axis=1)
            return carry

        lax.fori_loop(0, GC, body, 0)

    def flow(base, firsts, seconds, ref, parts):
        done = []
        offs = (0, -1, 1, 2)

        def send(blk, prt, idx, dev):
            here = ref(blk, parts[prt])
            cp = remote(here, here, g_s.at[base + idx], g_r.at[base + idx], dev)
            cp.start()
            done.append(cp)

        def wait(blk, prt, idx):
            here = ref(blk, parts[prt])
            remote(here, here, g_s.at[base + idx], g_r.at[base + idx], partner).wait_recv()

        def second(b, prt):
            for way in ((0, 1) if prt == 0 else (1, 0)):
                send((offs[b], 0), prt, 6 * b + 6 + 2 * way + prt, seconds[way])

        def second_forward(b):
            wait((offs[b], -1), 0, 6 * b + 6)
            send((offs[b], -1), 0, 6 * b + 10, seconds[0])
            wait((offs[b], 1), 1, 6 * b + 9)
            send((offs[b], 1), 1, 6 * b + 11, seconds[1])

        for prt, way in ((0, 0), (1, 1), (1, 0), (0, 1)):
            send((0, 0), prt, 2 * way + prt, firsts[way])
        for prt in range(2):
            send((0, 0), prt, RING + prt, firsts[2])
        yield
        second(0, 0)
        second(0, 1)
        yield
        wait((-1, 0), 0, 0)
        second(1, 0)
        yield
        wait((1, 0), 1, 3)
        second(2, 1)
        yield
        wait((-1, 0), 1, 1)
        second(1, 1)
        wait((1, 0), 0, 2)
        second(2, 0)
        yield
        wait((2, 0), 0, RING)
        second(3, 0)
        wait((2, 0), 1, 5)
        second(3, 1)
        yield
        second_forward(0)
        yield
        for b in range(1, RING):
            second_forward(b)
            yield
        for b in range(RING):
            for off, prt, idx in ((-1, 1, 7), (1, 0, GC), (2, 0, 10), (2, 1, 11)):
                wait((offs[b], off), prt, 6 * b + idx)
        yield
        for cp in done:
            cp.wait_send()
        yield

    def device(dz, dy):
        return (wrap4(z + dz) * RING + wrap4(y + dy)) * GC + x * 2 + (1 - core if (dz + dy) % 2 else core)

    y_ways, z_ways = [device(0, d) for d in (1, -1, 2)], [device(d, 0) for d in (1, -1, 2)]

    def y_first(blk, prt):
        return ug.at[wrap4(z + blk[1]), wrap4(y + blk[0]), pl.ds(*prt)]

    def z_first(blk, prt):
        return ug.at[wrap4(z + blk[0]), wrap4(y + blk[1]), pl.ds(*prt)]

    def gather(hooks):
        flows = [[flow(GSEM * (2 * h + idx), *ways, ref, PARTS[h][idx]) for idx, (ways, ref) in enumerate((((y_ways, z_ways), y_first), ((z_ways, y_ways), z_first)))]
                 for h in range(2)]
        for mark in ORDER:
            if mark in hooks:
                hooks[mark]()
            else:
                for one in flows[int(mark)]:
                    next(one)

    def out_copy(slot, tt, dev):
        return remote(sig.at[rows_of(tt)], out_recv.at[slot], out_s.at[tt], out_r.at[slot], dev)

    def out_start():
        for d in range(1, GC):
            tt, jj, dev = in_row(d)
            out_copy(j, tt, dev).start()
        out_recv[j] = sig[my_rows, :]

    def out_finish(step):
        for d in range(1, GC):
            tt, jj, dev = in_row(d)
            out_copy(jj, tt, dev).wait_recv()
            out_copy(j, tt, dev).wait_send()
        cp_v.wait()
        alpha, inv = fin[pl.ds(COLS, 1), pl.ds(0, 1)], fin[pl.ds(COLS + GC, 1), pl.ds(0, 1)]
        for tile in range(5):
            lanes = pl.ds(LANES * tile, LANES)
            outv[:, lanes] = (dense_tile(lambda idx: out_recv[idx], tile) - alpha * outv[:, lanes]) * inv
        pltpu.make_async_copy(outv, vecs.at[step], loc.at[2]).start()

    def step_body(step, beta):
        cur = lax.rem(step, 3)
        prev = lax.rem(step + 2, 3)
        nxt = lax.rem(step + 1, 3)

        with jax.named_scope("pack"):
            strided = [vt[cur, pl.ds(r, ROWS, stride=PAIR), :] for r in range(PAIR)]
            for lt in range(5):
                half = [dense_tile(lambda idx, h=h: strided[GC * h + idx], lt) for h in range(2)]
                for h in range(2):
                    for tt in range(2):
                        ug[z, y, tile_of(lt, 2 * h + tt)] = half[h][PAIR * tt:PAIR * tt + PAIR].astype(BF16)
                ug[z, y, tile_of(lt, RING)] = jnp.concatenate([half[0][32:ROWS], half[1][32:ROWS]], axis=0).astype(BF16)

        def early():
            pl.when(step == 0)(left_forward)

        def middle():
            pl.when(step == 0)(left_far)

            @pl.when(step > 0)
            def _():
                out_finish(step)

        def late():
            pl.when(step == 0)(left_finish)

        halves = iter(range(2))

        def left_half():
            h = next(halves)
            for group in range(3):
                first = 3 * group
                got = []
                for r in range(first, min(first + 3, GC)):
                    rows = [take_piece(lambda t, tr=tr: ug[:, :, tile_of(t, tr)].reshape(WIDE, LANES), r) for tr in (2 * h, 2 * h + 1, RING)]
                    got.append(jnp.concatenate(rows, axis=0))
                rhs = jnp.concatenate(merge_three(*got), axis=1)
                for mc in range(2):
                    rows = pl.ds(BOND * mc, BOND)
                    res = jnp.dot(lh[h, rows, :], rhs, preferred_element_type=F32).astype(BF16)
                    for rr, val in enumerate(split_three(res[:, :LANES], res[:, LANES:])[:len(got)]):
                        xs[h * GC + first + rr, rows, :] = val

        def named(name, call):
            def run():
                with jax.named_scope(name):
                    call()
            return run

        with jax.named_scope("gather"):
            gather({"P": early, "Q": middle, "R": named("late", late), "L": named("left", left_half)})

        def some_rows(ap, carry):
            for pr in range(RING):
                spots = [ap * GC + 2 * pr + aa for aa in range(2)]
                both = []
                for h in range(2):
                    rhs = jnp.concatenate([xs[:, pl.ds(pl.multiple_of(spot * 32 + PAIR * h, PAIR), PAIR), :].reshape(WIDE, LANES) for spot in spots], axis=1)
                    both.append(jnp.dot(wbig[h], rhs, preferred_element_type=F32).astype(BF16))
                for aa, spot in enumerate(spots):
                    rows = pl.ds(pl.multiple_of(spot * PAIR, PAIR), PAIR)
                    terms = [res[PAIR * k:PAIR * k + PAIR, LANES * aa:LANES * aa + LANES] for res in both for k in range(PAIR)]
                    for m in range(11):
                        for side, val in enumerate(merge_three(*terms[3 * m:3 * m + 3])):
                            ys[rows, pl.ds(WIDE * m + LANES * side, LANES)] = val
            return carry

        xo, xu, xd = wrap4(x + 2), wrap4(x + 1), wrap4(x - 1)

        def sigma(cols):
            for half in range(2):
                res = lax.dot_general(rt[pl.ds(320 * half, 320), :], ys[cols, :], (((1,), (1,)), ((), ())), preferred_element_type=F32)
                for idx in range(RING):
                    part[2 * half + idx // 2, idx % 2, :, cols] = res[idx * COLS:idx * COLS + COLS]

        class Chunk:
            def __init__(self, num, start, width):
                cols = self.cols = pl.ds(start, width)
                self.rows = start // LANES, (start + width) // LANES
                self.swap = remote(part.at[:, 1 - label, :, cols], rd.at[:, :, cols], d_s.at[num], d_r.at[num], partner)
                plan = ((xo, lo, ra, lo, x_up), (xo, hi, rb, lo, x_dn), (xu, hi, fl, hi, x_up), (xd, lo, fr, lo, x_dn), (xu, lo, fl, lo, x_up), (xd, hi, fr, hi, x_dn))
                self.copies = [remote(ssum.at[chip, rows, cols], dst.at[to, cols], ring_s.at[6 * num + idx], ring_r.at[6 * num + idx], dev)
                               for idx, (chip, rows, dst, to, dev) in enumerate(plan)]

            def make_y(self):
                for group in range(*self.rows):
                    some_rows(group, 0)

            def make(self):
                sigma(self.cols)
                self.swap.start()

            def add(self):
                self.swap.wait()
                for chip in range(RING):
                    ssum[chip, :, self.cols] = part[chip, label, :, self.cols] + rd[chip, :, self.cols]
                for cp in self.copies[:RING]:
                    cp.start()

            def pass_on(self):
                self.copies[0].wait_recv()
                ssum[xu, lo, self.cols] = ssum[xu, lo, self.cols] + ra[:, self.cols]
                self.copies[RING].start()
                self.copies[1].wait_recv()
                ssum[xd, hi, self.cols] = ssum[xd, hi, self.cols] + rb[:, self.cols]
                self.copies[5].start()

            def finish(self):
                for cp in self.copies[2:]:
                    cp.wait_recv()
                fin[pl.ds(0, COLS), self.cols] = ssum[x, :, self.cols] + fl[:, self.cols] + fr[:, self.cols]
                for cp in self.copies:
                    cp.wait_send()

        one, two, three = (Chunk(*spec) for spec in ((0, 0, WIDE), (1, WIDE, WIDE), (2, 512, LANES)))
        with jax.named_scope("w0"):
            one.make_y()
        with jax.named_scope("r0"):
            one.make()
        with jax.named_scope("w1"):
            two.make_y()
        with jax.named_scope("add0"):
            one.add()
        with jax.named_scope("r1"):
            two.make()
        with jax.named_scope("w2"):
            three.make_y()
        with jax.named_scope("add1"):
            two.add()
        with jax.named_scope("r2"):
            three.make()
        with jax.named_scope("pass0"):
            one.pass_on()
        with jax.named_scope("add2"):
            three.add()
        with jax.named_scope("pass1"):
            two.pass_on()
            three.pass_on()
        with jax.named_scope("xfin"):
            v_cur = vt[cur]
            n_loc = total(v_cur * v_cur)
            c_loc = total(v_cur * vt[prev])
            one.finish()
            two.finish()
            three.finish()
        with jax.named_scope("turn"):
            for b in range(5):
                rows = pl.ds(LANES * b, LANES)
                sig[rows, :] = jnp.where(row_lane < COLS, fin[:, rows].T, 0.0)

        with jax.named_scope("vec1"):
            t_val = sig[...] - beta * vt[prev]
            s_loc = total(t_val * vt[cur])
            sig[...] = t_val
            w_val = t_val - ratio(s_loc, n_loc) * vt[cur]
            e_loc = total(w_val * w_val)
        with jax.named_scope("allred"):
            def last_start():
                pl.when(step == NUM_STEPS - 1)(out_start)

            n, s, e, c = all_reduce([n_loc, s_loc, e_loc, c_loc], last_start)
            pl.when(step < NUM_STEPS - 1)(out_start)
        with jax.named_scope("vec2"):
            alpha = (s + beta * c) / VEC
            diff = alpha - ratio(s, n)
            beta_new = jnp.sqrt((e + diff * n * diff) / VEC)
            inv = 1.0 / beta_new
            vt[nxt] = (sig[...] - alpha * vt[cur]) * inv
            fin[pl.ds(COLS, 1), :] = jnp.broadcast_to(alpha, (1, BOND))
            fin[pl.ds(COLS + GC, 1), :] = jnp.broadcast_to(inv, (1, BOND))
            alphas[step] = alpha[0, 0]
            betas[step] = beta_new[0, 0]
        return beta_new

    lax.fori_loop(0, NUM_STEPS, step_body, jnp.zeros((1, 1), F32))
    out_finish(NUM_STEPS)
    cp_v.wait()


def run_kernel(psi, left, pair, order, right):
    vmem, anys, smem = (pl.BlockSpec(memory_space=space) for space in (pltpu.VMEM, pl.ANY, pltpu.SMEM))
    dma = pltpu.SemaphoreType.DMA
    vm = pltpu.VMEM
    block = (COLS, BOND)
    scratch = [
        vm((BOND, 1024), BF16),
        vm((RING, 2, 160, BOND), BF16), vm((2, 1280, 768), BF16), vm((2, WIDE, WIDE), BF16), vm((2816, BOND), BF16), vm((BOND, 2816), BF16),
        vm((RING, RING, 25, PAIR, LANES), BF16), vm((PAIR, 1280, LANES), BF16), vm((BOND, 2816), BF16), vm((RING, 2) + block, F32),
        vm((RING,) + block, F32), vm((RING,) + block, F32), vm((ROWS, BOND), F32), vm((ROWS, BOND), F32), vm(block, F32), vm(block, F32),
        vm((LANES, BOND), F32), vm((BOND, LANES), F32), vm((3, BOND, LANES), F32), vm((GC, COLS, LANES), F32), vm((GC, COLS, LANES), F32), vm(block, F32),
        vm((LANES, 2, LANES), F32),
    ] + [dma((num,)) for num in (GC, GC, GC, GC, GC, GC, RING * GSEM, RING * GSEM, 3, 3, 18, 18)] + [dma, dma, dma((RING,)), pltpu.SemaphoreType.REGULAR]
    scal = jax.ShapeDtypeStruct((NUM_STEPS,), F32)
    return pl.pallas_call(
        kernel,
        out_shape=(jax.ShapeDtypeStruct((NUM_STEPS + 1,) + block, F32), scal, scal),
        in_specs=[vmem, anys, vmem, anys, anys],
        out_specs=(anys, smem, smem),
        scratch_shapes=scratch,
        compiler_params=pltpu.CompilerParams(collective_id=0, has_side_effects=True, vmem_limit_bytes=67043328),
        name="lanczos",
    )(psi, left, pair, order, right)


def solution(mesh):
    def local_run(wave_rows, left_rows, op_pair, right_env):
        psi = wave_rows.reshape(COLS, BOND)
        left = jnp.transpose(left_rows, (1, 0, 2)).reshape(160, BOND)
        vecs, alphas, betas = run_kernel(psi, left, op_pair.reshape(512, PAIR), left_order(), right_env)
        return vecs.reshape(7, 5, RING, RING, BOND), alphas, betas

    rows = "rows"
    return jax.shard_map(local_run, mesh=mesh, in_specs=(P(rows), P(None, rows), P(), P()), out_specs=(P(None, rows), P(), P()), check_vma=False)
```

```python
import itertools

import jax
import jax.numpy as jnp
import numpy as np
from jax import lax
from jax.experimental import pallas as pl
from jax.experimental.pallas import tpu as pltpu
from jax.sharding import PartitionSpec as P

NUM_STEPS = 6
MESH = pl.DeviceIdType.MESH
F32 = jnp.float32
BF16 = jnp.bfloat16

ROWS, COLS = 40, 80
BOND, PAIR, TERMS = 640, 16, 32
LANES = 128
GC, RING, WIDE = 8, 4, 256
VEC = BOND * BOND * PAIR
PARTS = ((((0, 4), (4, 3)), ((7, 4), (11, 4))), (((15, 2), (17, 3)), ((20, 3), (23, 2))))
ORDER = "0011000P111001Q1001101R0L1L01"
GSEM = 30
FARTHEST = sorted(itertools.product(range(4), range(4), range(4), range(2)), key=lambda off: -sum(min(d, 4 - d) for d in off))[:-1]


def left_order():
    col = np.arange(1024)
    group, tail = (col % WIDE) // PAIR, col >= 512
    src = np.where(tail, ROWS * group + 32 + col % GC, ROWS * group + PAIR * (col // WIDE) + col % PAIR)
    used = ~tail | ((col // GC) % 2 == (col >= 768))
    return jnp.asarray((np.arange(BOND)[:, None] == src) & used, BF16)


def remote(src, dst, send, recv, dev):
    return pltpu.make_async_remote_copy(src_ref=src, dst_ref=dst, send_sem=send, recv_sem=recv, device_id=(dev,), device_id_type=MESH)


def tile_of(lane_tile, row_tile):
    return 15 + 2 * lane_tile + row_tile - 2 if row_tile in (2, 3) else 3 * lane_tile + min(row_tile, 2)


def lane_roll(val, shift):
    shift = shift % LANES
    return val if shift == 0 else pltpu.roll(val, shift, axis=val.ndim - 1)


def lane_iota(val):
    return lax.broadcasted_iota(jnp.int32, val.shape, val.ndim - 1)


def take_piece(tiles, idx):
    tile, off = divmod(COLS * idx, LANES)
    out = lane_roll(tiles(tile), -off)
    lane = lane_iota(out)
    if off + COLS > LANES:
        out = jnp.where(lane < LANES - off, out, lane_roll(tiles(tile + 1), -off))
    return jnp.where(lane < COLS, out, jnp.zeros_like(out))


def merge_three(one, two, three=None):
    if three is None:
        return one, two
    inner = lane_iota(one) < COLS
    return jnp.where(inner, one, lane_roll(three, COLS)), jnp.where(inner, two, lane_roll(three, COLS - 48))


def split_three(left, right):
    lane, zero = lane_iota(left), jnp.zeros_like(left)
    three = jnp.where(lane < 48, lane_roll(left, -COLS), jnp.where(lane < COLS, lane_roll(right, 48 - COLS), zero))
    return jnp.where(lane < COLS, left, zero), jnp.where(lane < COLS, right, zero), three


def dense_tile(pieces, tile):
    out = None
    for idx in range(GC):
        shift = COLS * idx - LANES * tile
        if shift <= -COLS or shift >= LANES:
            continue
        moved = lane_roll(pieces(idx), shift)
        out = moved if out is None else jnp.where(lane_iota(moved) >= shift, moved, out)
    return out


def kernel(psi, left, pair, order_hbm, right, vecs, alphas, betas, order, lall, lh, wbig, rtmp, rt, ug, xs, ys, part, rd, ssum, ra, rb, fl, fr, fin,
           sig, vt, piece_buf, out_recv, outv, stat, psi_s, psi_r, l_s, l_r, out_s, out_r, g_s, g_r, d_s, d_r,
           ring_s, ring_r, a_s, a_r, loc, ready):
    me = lax.axis_index("rows")
    core = lax.rem(me, 2)
    x = lax.rem(me // 2, RING)
    y = lax.rem(me // GC, RING)
    z = me // 32
    i = me // GC
    t_me = lax.rem(me, GC)
    label = lax.rem(me + x + y + z, 2)
    j = x * 2 + label
    lo, hi = pl.ds(0, ROWS), pl.ds(ROWS, ROWS)

    def wrap4(val):
        return lax.rem(val + RING, RING)

    def in_row(d):
        tt = lax.rem(t_me + d, GC)
        return tt, tt - lax.rem(tt, 2) + lax.rem(tt + tt // 2 + y + z, 2), i * GC + tt

    def rows_of(jj):
        return pl.ds(pl.multiple_of(jj * COLS, COLS), COLS)

    barrier = pltpu.get_barrier_semaphore()

    def col_dev(di):
        ii = lax.rem(i + di, PAIR)
        return ii * GC + x * 2 + lax.rem(label + x + ii + ii // RING, 2)

    for d in range(1, GC):
        pl.semaphore_signal(barrier, inc=1, device_id=(in_row(d)[2],), device_id_type=MESH)
    for di in range(1, PAIR):
        pl.semaphore_signal(barrier, inc=1, device_id=(col_dev(di),), device_id_type=MESH)
    pl.semaphore_wait(barrier, 22)
    for di in range(1, PAIR):
        pl.semaphore_signal(ready, inc=1, device_id=(col_dev(di),), device_id_type=MESH)

    partner = me + 1 - 2 * core
    places = ([wrap4(z + d) * 32 for d in range(RING)], [wrap4(y + d) * GC for d in range(RING)], [wrap4(x + d) * 2 for d in range(RING)], (core, 1 - core))
    x_up, x_dn = i * GC + wrap4(x + 1) * 2 + 1 - core, i * GC + wrap4(x - 1) * 2 + 1 - core
    left_up, left_dn = (i * GC + wrap4(x + d) * 2 + core for d in (1, -1))
    my_rows = rows_of(t_me)

    def fetch_right(first, last, row, width):
        def body(m, carry):
            src = right.at[3 * m + first, pl.ds(pl.multiple_of(j * COLS + row, PAIR), width), :]
            pltpu.make_async_copy(src, rtmp.at[pl.ds(pl.multiple_of(WIDE * m + last, PAIR), width), :], loc.at[0]).start()
            return carry
        return body

    lax.fori_loop(0, 11, fetch_right(0, 0, 0, COLS), 0)
    lax.fori_loop(0, 11, fetch_right(1, LANES, 0, COLS), 0)
    lax.fori_loop(0, 10, fetch_right(2, COLS, 0, 48), 0)
    lax.fori_loop(0, 10, fetch_right(2, LANES + COLS, 48, 32), 0)
    cp_l = pltpu.make_async_copy(left, lall.at[x, core], loc.at[1])
    cp_l.start()
    cp_order = pltpu.make_async_copy(order_hbm, order, loc.at[3])
    cp_order.start()

    row_lane = lax.broadcasted_iota(jnp.int32, (1, LANES), 1)

    def total(val):
        return jnp.sum(jnp.sum(val, axis=0, keepdims=True), axis=1, keepdims=True)

    def ratio(num, den):
        good = den > 0
        return jnp.where(good, num / jnp.where(good, den, 1.0), 0.0)

    def all_reduce(stats, hook):
        row = jnp.zeros((1, LANES), F32)
        for idx, val in enumerate(stats):
            row = jnp.where(row_lane == idx, val, row)
        stat[me, pl.ds(0, 1), :] = row
        stat[me, pl.ds(1, 1), :] = jnp.broadcast_to(ratio(stats[1], stats[0]), (1, LANES))

        for off in FARTHEST:
            dev = sum(spot[step] for spot, step in zip(places, off))
            remote(stat.at[me], stat.at[me], a_s, a_r, dev).start()
        hook()
        most = stat.at[pl.ds(0, LANES - 1)]
        with jax.named_scope("arwait"):
            remote(most, most, a_s, a_r, partner).wait()
        rows = stat[:, pl.ds(0, 1), :]
        sums = jnp.sum(rows, axis=0)
        n, s, e, c = (jnp.sum(jnp.where(row_lane == idx, sums, 0.0), axis=1, keepdims=True) for idx in range(RING))
        diff = stat[:, pl.ds(1, 1), :] - ratio(s, n)[None]
        moved = jnp.sum(diff * rows * diff, axis=0)
        return n, s, e + jnp.sum(jnp.where(row_lane == 0, moved, 0.0), axis=1, keepdims=True), c

    def l_copy(src, rows, idx, dev):
        ref = lall.at[src[0], src[1], rows]
        return remote(ref, ref, l_s.at[idx], l_r.at[idx], dev)

    every, low, high = pl.ds(0, 160), pl.ds(0, COLS), pl.ds(COLS, COLS)

    def psi_pieces():
        for jj in range(GC):
            piece_buf[jj] = take_piece(lambda t: psi[:, LANES * t:LANES * t + LANES], jj)
        vt[0, my_rows, :] = piece_buf[j]
        spread = jnp.where(lax.broadcasted_iota(jnp.int32, (PAIR, WIDE), 1) // PAIR == lax.broadcasted_iota(jnp.int32, (PAIR, WIDE), 0), 1.0, 0.0).astype(BF16)
        same = lax.broadcasted_iota(jnp.int32, (WIDE, WIDE), 1) % PAIR == lax.broadcasted_iota(jnp.int32, (WIDE, WIDE), 0) // PAIR
        for h in range(2):
            wide = jnp.dot(pair[pl.ds(WIDE * h, WIDE), :], spread, preferred_element_type=F32)
            wbig[h] = jnp.where(same, wide, 0.0).astype(BF16)
        vt[2] = jnp.zeros((BOND, LANES), F32)
        fin[...] = jnp.zeros((LANES, BOND), F32)

    def psi_sends():
        for d in range(1, GC):
            tt, jj, dev = in_row(d)
            remote(piece_buf.at[jj], vt.at[0, my_rows], psi_s.at[tt], psi_r.at[t_me], dev).start()
        cp_l.wait()
        l_copy((x, core), every, 0, left_up).start()
        l_copy((x, core), every, 1, left_dn).start()
        l_copy((x, core), every, RING, partner).start()

    def turn_right():
        some = rtmp.at[pl.ds(0, TERMS * COLS), :]
        pltpu.make_async_copy(some, some, loc.at[0]).wait()
        for m in range(11):
            rtmp[pl.ds(WIDE * m + 240, PAIR), :] = jnp.zeros((PAIR, BOND), BF16)
        for start in (COLS, LANES + COLS):
            rtmp[pl.ds(2560 + start, 48), :] = jnp.zeros((48, BOND), BF16)

        def body(k, carry):
            cols = pl.ds(pl.multiple_of(k * LANES, LANES), LANES)
            for b in range(5):
                rt[pl.ds(LANES * b, LANES), cols] = rtmp[cols, pl.ds(LANES * b, LANES)].T
            return carry

        lax.fori_loop(0, 22, body, 0)

    lower, upper, far = (wrap4(x - 1), core), (wrap4(x + 1), core), (wrap4(x + 2), core)

    def left_forward():
        for idx, (block, way, rows) in enumerate(((lower, left_up, low), (upper, left_dn, high))):
            l_copy(block, every, idx, way).wait_recv()
            l_copy(block, rows, idx + 2, way).start()
            l_copy(block, every, idx + 5, partner).start()

    def left_far():
        l_copy(far, low, 2, partner).wait_recv()
        l_copy(far, high, 3, partner).wait_recv()
        l_copy(far, every, 7, partner).start()

    def start_up():
        with jax.named_scope("psi"):
            psi_sends()
        with jax.named_scope("turnr"):
            turn_right()

    psi_pieces()
    psi_val = psi[...]
    pl.semaphore_wait(ready, PAIR - 1)
    zero = jnp.zeros((1, 1), F32)
    n_psi = all_reduce([total(psi_val * psi_val), zero], start_up)[0]
    inv_norm = 1.0 / jnp.sqrt(n_psi / VEC)

    for d in range(1, GC):
        tt, jj, dev = in_row(d)
        cp = remote(piece_buf.at[jj], vt.at[0, rows_of(tt)], psi_s.at[tt], psi_r.at[tt], dev)
        cp.wait_recv()
        cp.wait_send()
    vt[0] = vt[0] * inv_norm
    outv[...] = psi_val * inv_norm
    cp_v = pltpu.make_async_copy(outv, vecs.at[0], loc.at[2])
    cp_v.start()

    def left_finish():
        for idx, dx in ((RING, 0), (5, 3), (6, 1), (7, 2)):
            l_copy((wrap4(x + dx), 1 - core), every, idx, partner).wait_recv()
        for idx, rows in enumerate((every, every, low, high) + (every,) * RING):
            l_copy((x, core), rows, idx, partner).wait_send()

        cp_order.wait()

        def body(t, carry):
            rows = pl.ds(pl.multiple_of(t * 160, 160), 160)
            res = jnp.dot(lall[t // 2, t % 2], order[...], preferred_element_type=F32).astype(BF16)
            for h in range(2):
                lh[h, rows, :] = jnp.concatenate([res[:, :512], res[:, 512 + WIDE * h:768 + WIDE * h]], axis=1)
            return carry

        lax.fori_loop(0, GC, body, 0)

    def flow(base, firsts, seconds, ref, parts):
        done = []
        offs = (0, -1, 1, 2)

        def send(blk, prt, idx, dev):
            here = ref(blk, parts[prt])
            cp = remote(here, here, g_s.at[base + idx], g_r.at[base + idx], dev)
            cp.start()
            done.append(cp)

        def wait(blk, prt, idx):
            here = ref(blk, parts[prt])
            remote(here, here, g_s.at[base + idx], g_r.at[base + idx], partner).wait_recv()

        def second(b, prt):
            for way in ((0, 1) if prt == 0 else (1, 0)):
                send((offs[b], 0), prt, 6 * b + 6 + 2 * way + prt, seconds[way])

        def second_forward(b):
            wait((offs[b], -1), 0, 6 * b + 6)
            send((offs[b], -1), 0, 6 * b + 10, seconds[0])
            wait((offs[b], 1), 1, 6 * b + 9)
            send((offs[b], 1), 1, 6 * b + 11, seconds[1])

        for prt, way in ((0, 0), (1, 1), (1, 0), (0, 1)):
            send((0, 0), prt, 2 * way + prt, firsts[way])
        for prt in range(2):
            send((0, 0), prt, RING + prt, firsts[2])
        yield
        second(0, 0)
        second(0, 1)
        yield
        wait((-1, 0), 0, 0)
        second(1, 0)
        yield
        wait((1, 0), 1, 3)
        second(2, 1)
        yield
        wait((-1, 0), 1, 1)
        second(1, 1)
        wait((1, 0), 0, 2)
        second(2, 0)
        yield
        wait((2, 0), 0, RING)
        second(3, 0)
        wait((2, 0), 1, 5)
        second(3, 1)
        yield
        second_forward(0)
        yield
        for b in range(1, RING):
            second_forward(b)
            yield
        for b in range(RING):
            for off, prt, idx in ((-1, 1, 7), (1, 0, GC), (2, 0, 10), (2, 1, 11)):
                wait((offs[b], off), prt, 6 * b + idx)
        yield
        for cp in done:
            cp.wait_send()
        yield

    def device(dz, dy):
        return (wrap4(z + dz) * RING + wrap4(y + dy)) * GC + x * 2 + (1 - core if (dz + dy) % 2 else core)

    y_ways, z_ways = [device(0, d) for d in (1, -1, 2)], [device(d, 0) for d in (1, -1, 2)]

    def y_first(blk, prt):
        return ug.at[wrap4(z + blk[1]), wrap4(y + blk[0]), pl.ds(*prt)]

    def z_first(blk, prt):
        return ug.at[wrap4(z + blk[0]), wrap4(y + blk[1]), pl.ds(*prt)]

    def gather(hooks):
        flows = [[flow(GSEM * (2 * h + idx), *ways, ref, PARTS[h][idx]) for idx, (ways, ref) in enumerate((((y_ways, z_ways), y_first), ((z_ways, y_ways), z_first)))]
                 for h in range(2)]
        for mark in ORDER:
            if mark in hooks:
                hooks[mark]()
            else:
                for one in flows[int(mark)]:
                    next(one)

    def out_copy(slot, tt, dev):
        return remote(sig.at[rows_of(tt)], out_recv.at[slot], out_s.at[tt], out_r.at[slot], dev)

    def out_start():
        for d in range(1, GC):
            tt, jj, dev = in_row(d)
            out_copy(j, tt, dev).start()
        out_recv[j] = sig[my_rows, :]

    def out_finish(step):
        for d in range(1, GC):
            tt, jj, dev = in_row(d)
            out_copy(jj, tt, dev).wait_recv()
            out_copy(j, tt, dev).wait_send()
        cp_v.wait()
        alpha, inv = fin[pl.ds(COLS, 1), pl.ds(0, 1)], fin[pl.ds(COLS + GC, 1), pl.ds(0, 1)]
        for tile in range(5):
            lanes = pl.ds(LANES * tile, LANES)
            outv[:, lanes] = (dense_tile(lambda idx: out_recv[idx], tile) - alpha * outv[:, lanes]) * inv
        pltpu.make_async_copy(outv, vecs.at[step], loc.at[2]).start()

    def step_body(step, beta):
        cur = lax.rem(step, 3)
        prev = lax.rem(step + 2, 3)
        nxt = lax.rem(step + 1, 3)

        with jax.named_scope("pack"):
            strided = [vt[cur, pl.ds(r, ROWS, stride=PAIR), :] for r in range(PAIR)]
            for lt in range(5):
                half = [dense_tile(lambda idx, h=h: strided[GC * h + idx], lt) for h in range(2)]
                for h in range(2):
                    for tt in range(2):
                        ug[z, y, tile_of(lt, 2 * h + tt)] = half[h][PAIR * tt:PAIR * tt + PAIR].astype(BF16)
                ug[z, y, tile_of(lt, RING)] = jnp.concatenate([half[0][32:ROWS], half[1][32:ROWS]], axis=0).astype(BF16)

        def early():
            pl.when(step == 0)(left_forward)

        def middle():
            pl.when(step == 0)(left_far)

            @pl.when(step > 0)
            def _():
                out_finish(step)

        def late():
            pl.when(step == 0)(left_finish)

        halves = iter(range(2))

        def left_half():
            h = next(halves)
            for group in range(3):
                first = 3 * group
                got = []
                for r in range(first, min(first + 3, GC)):
                    rows = [take_piece(lambda t, tr=tr: ug[:, :, tile_of(t, tr)].reshape(WIDE, LANES), r) for tr in (2 * h, 2 * h + 1, RING)]
                    got.append(jnp.concatenate(rows, axis=0))
                rhs = jnp.concatenate(merge_three(*got), axis=1)
                for mc in range(2):
                    rows = pl.ds(BOND * mc, BOND)
                    res = jnp.dot(lh[h, rows, :], rhs, preferred_element_type=F32).astype(BF16)
                    for rr, val in enumerate(split_three(res[:, :LANES], res[:, LANES:])[:len(got)]):
                        xs[h * GC + first + rr, rows, :] = val

        def named(name, call):
            def run():
                with jax.named_scope(name):
                    call()
            return run

        with jax.named_scope("gather"):
            gather({"P": early, "Q": middle, "R": named("late", late), "L": named("left", left_half)})

        def some_rows(ap, carry):
            for pr in range(RING):
                spots = [ap * GC + 2 * pr + aa for aa in range(2)]
                both = []
                for h in range(2):
                    rhs = jnp.concatenate([xs[:, pl.ds(pl.multiple_of(spot * 32 + PAIR * h, PAIR), PAIR), :].reshape(WIDE, LANES) for spot in spots], axis=1)
                    both.append(jnp.dot(wbig[h], rhs, preferred_element_type=F32).astype(BF16))
                for aa, spot in enumerate(spots):
                    rows = pl.ds(pl.multiple_of(spot * PAIR, PAIR), PAIR)
                    terms = [res[PAIR * k:PAIR * k + PAIR, LANES * aa:LANES * aa + LANES] for res in both for k in range(PAIR)]
                    for m in range(11):
                        for side, val in enumerate(merge_three(*terms[3 * m:3 * m + 3])):
                            ys[rows, pl.ds(WIDE * m + LANES * side, LANES)] = val
            return carry

        xo, xu, xd = wrap4(x + 2), wrap4(x + 1), wrap4(x - 1)

        def sigma(cols):
            for half in range(2):
                res = lax.dot_general(rt[pl.ds(320 * half, 320), :], ys[cols, :], (((1,), (1,)), ((), ())), preferred_element_type=F32)
                for idx in range(RING):
                    part[2 * half + idx // 2, idx % 2, :, cols] = res[idx * COLS:idx * COLS + COLS]

        class Chunk:
            def __init__(self, num, start, width):
                cols = self.cols = pl.ds(start, width)
                self.rows = start // LANES, (start + width) // LANES
                self.swap = remote(part.at[:, 1 - label, :, cols], rd.at[:, :, cols], d_s.at[num], d_r.at[num], partner)
                plan = ((xo, lo, ra, lo, x_up), (xo, hi, rb, lo, x_dn), (xu, hi, fl, hi, x_up), (xd, lo, fr, lo, x_dn), (xu, lo, fl, lo, x_up), (xd, hi, fr, hi, x_dn))
                self.copies = [remote(ssum.at[chip, rows, cols], dst.at[to, cols], ring_s.at[6 * num + idx], ring_r.at[6 * num + idx], dev)
                               for idx, (chip, rows, dst, to, dev) in enumerate(plan)]

            def make_y(self):
                for group in range(*self.rows):
                    some_rows(group, 0)

            def make(self):
                sigma(self.cols)
                self.swap.start()

            def add(self):
                self.swap.wait()
                for chip in range(RING):
                    ssum[chip, :, self.cols] = part[chip, label, :, self.cols] + rd[chip, :, self.cols]
                for cp in self.copies[:RING]:
                    cp.start()

            def pass_on(self):
                self.copies[0].wait_recv()
                ssum[xu, lo, self.cols] = ssum[xu, lo, self.cols] + ra[:, self.cols]
                self.copies[RING].start()
                self.copies[1].wait_recv()
                ssum[xd, hi, self.cols] = ssum[xd, hi, self.cols] + rb[:, self.cols]
                self.copies[5].start()

            def finish(self):
                for cp in self.copies[2:]:
                    cp.wait_recv()
                fin[pl.ds(0, COLS), self.cols] = ssum[x, :, self.cols] + fl[:, self.cols] + fr[:, self.cols]
                for cp in self.copies:
                    cp.wait_send()

        one, two, three = (Chunk(*spec) for spec in ((0, 0, LANES), (1, LANES, WIDE), (2, 3 * LANES, WIDE)))
        with jax.named_scope("w0"):
            one.make_y()
        with jax.named_scope("r0"):
            one.make()
        with jax.named_scope("w1"):
            two.make_y()
        with jax.named_scope("add0"):
            one.add()
        with jax.named_scope("r1"):
            two.make()
        with jax.named_scope("w2"):
            three.make_y()
        with jax.named_scope("add1"):
            two.add()
        with jax.named_scope("r2"):
            three.make()
        with jax.named_scope("pass0"):
            one.pass_on()
        with jax.named_scope("add2"):
            three.add()
        with jax.named_scope("pass1"):
            two.pass_on()
            three.pass_on()
        with jax.named_scope("xfin"):
            v_cur = vt[cur]
            n_loc = total(v_cur * v_cur)
            c_loc = total(v_cur * vt[prev])
            one.finish()
            two.finish()
            three.finish()
        with jax.named_scope("turn"):
            for b in range(5):
                rows = pl.ds(LANES * b, LANES)
                sig[rows, :] = jnp.where(row_lane < COLS, fin[:, rows].T, 0.0)

        with jax.named_scope("vec1"):
            t_val = sig[...] - beta * vt[prev]
            s_loc = total(t_val * vt[cur])
            sig[...] = t_val
            w_val = t_val - ratio(s_loc, n_loc) * vt[cur]
            e_loc = total(w_val * w_val)
        with jax.named_scope("allred"):
            def last_start():
                pl.when(step == NUM_STEPS - 1)(out_start)

            n, s, e, c = all_reduce([n_loc, s_loc, e_loc, c_loc], last_start)
            pl.when(step < NUM_STEPS - 1)(out_start)
        with jax.named_scope("vec2"):
            alpha = (s + beta * c) / VEC
            diff = alpha - ratio(s, n)
            beta_new = jnp.sqrt((e + diff * n * diff) / VEC)
            inv = 1.0 / beta_new
            vt[nxt] = (sig[...] - alpha * vt[cur]) * inv
            fin[pl.ds(COLS, 1), :] = jnp.broadcast_to(alpha, (1, BOND))
            fin[pl.ds(COLS + GC, 1), :] = jnp.broadcast_to(inv, (1, BOND))
            alphas[step] = alpha[0, 0]
            betas[step] = beta_new[0, 0]
        return beta_new

    lax.fori_loop(0, NUM_STEPS, step_body, jnp.zeros((1, 1), F32))
    out_finish(NUM_STEPS)
    cp_v.wait()


def run_kernel(psi, left, pair, order, right):
    vmem, anys, smem = (pl.BlockSpec(memory_space=space) for space in (pltpu.VMEM, pl.ANY, pltpu.SMEM))
    dma = pltpu.SemaphoreType.DMA
    vm = pltpu.VMEM
    block = (COLS, BOND)
    scratch = [
        vm((BOND, 1024), BF16),
        vm((RING, 2, 160, BOND), BF16), vm((2, 1280, 768), BF16), vm((2, WIDE, WIDE), BF16), vm((2816, BOND), BF16), vm((BOND, 2816), BF16),
        vm((RING, RING, 25, PAIR, LANES), BF16), vm((PAIR, 1280, LANES), BF16), vm((BOND, 2816), BF16), vm((RING, 2) + block, F32),
        vm((RING,) + block, F32), vm((RING,) + block, F32), vm((ROWS, BOND), F32), vm((ROWS, BOND), F32), vm(block, F32), vm(block, F32),
        vm((LANES, BOND), F32), vm((BOND, LANES), F32), vm((3, BOND, LANES), F32), vm((GC, COLS, LANES), F32), vm((GC, COLS, LANES), F32), vm(block, F32),
        vm((LANES, 2, LANES), F32),
    ] + [dma((num,)) for num in (GC, GC, GC, GC, GC, GC, RING * GSEM, RING * GSEM, 3, 3, 18, 18)] + [dma, dma, dma((RING,)), pltpu.SemaphoreType.REGULAR]
    scal = jax.ShapeDtypeStruct((NUM_STEPS,), F32)
    return pl.pallas_call(
        kernel,
        out_shape=(jax.ShapeDtypeStruct((NUM_STEPS + 1,) + block, F32), scal, scal),
        in_specs=[vmem, anys, vmem, anys, anys],
        out_specs=(anys, smem, smem),
        scratch_shapes=scratch,
        compiler_params=pltpu.CompilerParams(collective_id=0, has_side_effects=True, vmem_limit_bytes=67043328),
        name="lanczos",
    )(psi, left, pair, order, right)


def solution(mesh):
    def local_run(wave_rows, left_rows, op_pair, right_env):
        psi = wave_rows.reshape(COLS, BOND)
        left = jnp.transpose(left_rows, (1, 0, 2)).reshape(160, BOND)
        vecs, alphas, betas = run_kernel(psi, left, op_pair.reshape(512, PAIR), left_order(), right_env)
        return vecs.reshape(7, 5, RING, RING, BOND), alphas, betas

    rows = "rows"
    return jax.shard_map(local_run, mesh=mesh, in_specs=(P(rows), P(None, rows), P(), P()), out_specs=(P(None, rows), P(), P()), check_vma=False)
```
